32 devices in a mesh: dp: 4 (over z), row: 4 (over y, x), col: 2 (over core).
Axes of the slice: x: 2, y: 2, z: 4, core: 2. Of those that a mesh axis runs over, the one named last changes fastest.
Arguments:
- tokens: bfloat16 [4096, 1600], P(('dp', 'row'), 'col'), may hold values from -6 to 6
- segment_ids: int32 [4, 1024], P('dp'), may hold values from 0 to 3, as said below
- first_gain: float32 [1600], replicated, may hold values from 0.1 to 1.9
- first_shift: float32 [1600], replicated, may hold values from -3 to 3
- triple_weight: bfloat16 [1600, 4800], P('col', 'row'), may hold values from -1 to 1
- query_bias: float32 [1600], replicated, may hold values from -3 to 3
- value_bias: float32 [1600], replicated, may hold values from -3 to 3
- proj_weight: bfloat16 [1600, 1600], P('row', 'col'), may hold values from -0.4375 to 0.4375
- proj_bias: float32 [1600], replicated, may hold values from -3 to 3
- second_gain: float32 [1600], replicated, may hold values from 0.1 to 1.9
- second_shift: float32 [1600], replicated, may hold values from -3 to 3
- expand_weight: bfloat16 [1600, 6400], P('col', 'row'), may hold values from -0.15625 to 0.15625
- expand_bias: float32 [6400], replicated, may hold values from -3 to 3
- shrink_weight: bfloat16 [6400, 1600], P('row', 'col'), may hold values from -0.078125 to 0.078125
- shrink_bias: float32 [1600], replicated, may hold values from -3 to 3
- cotangent: bfloat16 [4096, 1600], P(('dp', 'row'), 'col'), may hold values from -6 to 6
Outputs:
- block_out: bfloat16 [4096, 1600], P(('dp', 'row'), 'col')
- input_grad: float32 [4096, 1600], P(('dp', 'row'), 'col')
- first_gain_grad: float32 [1600], replicated
- first_shift_grad: float32 [1600], replicated
- triple_grad: float32 [2, 800, 4800], P('col', 'dp', 'row')
- query_bias_grad: float32 [1600], replicated
- value_bias_grad: float32 [1600], replicated
- proj_grad: float32 [4, 400, 1600], P('row', 'dp', 'col')
- proj_bias_grad: float32 [1600], replicated
- second_gain_grad: float32 [1600], replicated
- second_shift_grad: float32 [1600], replicated
- expand_grad: float32 [2, 800, 6400], P('col', 'dp', 'row')
- expand_bias_grad: float32 [6400], replicated
- shrink_grad: float32 [4, 1600, 1600], P('row', 'dp', 'col')
- shrink_bias_grad: float32 [1600], replicated
The draws below stay inside these ranges and needn't reach their ends.
Inputs may be any that keep to these rules, and one draw needn't show every extreme that they name: `segment_ids`: each row lists the sequences of one data group in order: it starts at 0 and rises by one where a new sequence starts. A row holds 1 to 4 sequences; in every draw some row holds exactly 4 and another holds a single sequence of 1024 tokens.
All inputs are finite; a program needn't handle non-finite values.
Results may differ from the reference program's by a relative error of at most 0.014.
Values may be sent and summed in bfloat16 or wider, within the bound.
A program may use at most 192 MiB of HBM per device.

```python
import math
import jax
import jax.numpy as jnp
from jax import lax

HEADS = 25
HEAD_DIM = 64
D = 1600
FF = 6400
TOK_GRP = 1024
SEGMAX = 4
TOKENS = 4096
N_DP = 4
N_ROW = 4
N_COL = 2


def draw_triple_weight(key, part):
    width = HEADS * HEAD_DIM
    base_key = jax.random.fold_in(key, 0)
    base = jax.random.normal(base_key, (width, 3 * width), jnp.float32) * width ** (-0.5)
    return jnp.clip(base, -1.0, 1.0).astype(jnp.bfloat16)


def draw_segment_ids(key, part):
    count_key, busy_key, whole_key, cut_key = jax.random.split(key, 4)
    counts = jax.random.randint(count_key, (N_DP,), 1, SEGMAX + 1)
    busy = jax.random.randint(busy_key, (), 0, N_DP)
    single = (busy + 1 + jax.random.randint(whole_key, (), 0, N_DP - 1)) % N_DP
    indices = jnp.arange(N_DP)
    counts = jnp.where(indices == busy, SEGMAX, counts)
    counts = jnp.where(indices == single, 1, counts)

    def one_row(row_key, count):
        ranks = jax.random.permutation(row_key, TOK_GRP - 1)
        cuts = (ranks < count - 1).astype(jnp.int32)
        return jnp.concatenate([jnp.zeros((1,), jnp.int32), jnp.cumsum(cuts).astype(jnp.int32)])
    row_keys = jax.random.split(cut_key, N_DP)
    return jax.vmap(one_row)(row_keys, counts)


def block_scale(rng, extent, shards, least, largest):
    factor_of, own = 1.0, jax.random.fold_in(rng, 6)
    for dim, shards_of in shards:
        draws = jnp.exp(jax.random.uniform(jax.random.fold_in(own, dim), (shards_of,), jnp.float32, least / len(shards), largest / len(shards)))
        factor_of = factor_of * jnp.repeat(draws, extent[dim] // shards_of).reshape([-1 if axis == dim else 1 for axis in range(len(extent))])
    return factor_of


def gaussian(own_key, shape, scale, limit, cuts=(), kind=jnp.bfloat16):
    drawn = scale * jax.random.normal(own_key, shape, jnp.float32)
    if cuts:
        drawn = drawn * block_scale(own_key, shape, cuts, -0.22, 0.18)
    return jnp.clip(drawn, -limit, limit).astype(kind)


def setup_inputs(seed: int = 0) -> dict:
    key_of = jax.random.split(jax.random.key(seed), 17)
    return {
        "tokens": gaussian(key_of[0], (TOKENS, D), 1.0, 6.0, ((0, 16), (1, 2))),
        "segment_ids": draw_segment_ids(jax.random.fold_in(key_of[16], 71), 0),
        "first_gain": jnp.clip(1.0 + 0.18 * jax.random.normal(key_of[2], (D,), jnp.float32), 0.1, 1.9),
        "first_shift": gaussian(key_of[3], (D,), 0.5, 3.0, (), jnp.float32),
        "triple_weight": draw_triple_weight(jax.random.fold_in(key_of[16], 71), 0),
        "query_bias": gaussian(key_of[5], (D,), 0.5, 3.0, (), jnp.float32),
        "value_bias": gaussian(key_of[6], (D,), 0.5, 3.0, (), jnp.float32),
        "proj_weight": gaussian(key_of[7], (D, D), (D // 8) ** -0.5, 0.4375, ((0, 4), (1, 2))),
        "proj_bias": gaussian(key_of[8], (D,), 0.5, 3.0, (), jnp.float32),
        "second_gain": jnp.clip(1.0 + 0.18 * jax.random.normal(key_of[9], (D,), jnp.float32), 0.1, 1.9),
        "second_shift": gaussian(key_of[10], (D,), 0.5, 3.0, (), jnp.float32),
        "expand_weight": gaussian(key_of[11], (D, FF), D ** -0.5, 0.15625, ((0, 2), (1, 4))),
        "expand_bias": gaussian(key_of[12], (FF,), 0.5, 3.0, (), jnp.float32),
        "shrink_weight": gaussian(key_of[13], (FF, D), FF ** -0.5, 0.078125, ((0, 4), (1, 2))),
        "shrink_bias": gaussian(key_of[14], (D,), 0.5, 3.0, (), jnp.float32),
        "cotangent": gaussian(key_of[15], (TOKENS, D), 1.0, 6.0, ((0, 16), (1, 2))),
    }


EPS = 1e-05
NEG = -1e+30

def gelu_tanh(values):
    return 0.5 * values * (1.0 + jnp.tanh(0.7978845608028654 * (values + 0.044715 * values * values * values)))

def norm_forward(matrix, gain, shift):
    width = matrix.shape[-1]
    average = lax.optimization_barrier(jnp.sum(matrix, axis=-1, keepdims=True)) / width
    square = lax.optimization_barrier(jnp.sum(matrix * matrix, axis=-1, keepdims=True)) / width
    rstd = lax.rsqrt(square - average * average + EPS)
    normed_hat = (matrix - average) * rstd
    return (normed_hat * gain + shift, normed_hat, rstd)

def norm_backward(grad_in, normed_hat, rstd, gain):
    width = grad_in.shape[-1]
    scaled = grad_in * gain
    total = lax.optimization_barrier(jnp.sum(scaled, axis=-1, keepdims=True))
    mixed = lax.optimization_barrier(jnp.sum(scaled * normed_hat, axis=-1, keepdims=True))
    return rstd * (scaled - total / width - normed_hat * mixed / width)

def head_split(matrix):
    rows = matrix.shape[0]
    group_size = math.gcd(HEADS, 5)
    return matrix.reshape(rows, HEADS // group_size, group_size, HEAD_DIM).transpose(1, 0, 2, 3)

def head_join(blocks):
    rows = blocks.shape[1]
    return blocks.transpose(1, 0, 2, 3).reshape(rows, HEADS * HEAD_DIM)

def attention_forward(query_part, key_part, value_part, allowed):
    scaling = HEAD_DIM ** (-0.5)

    def one_group(blocks):
        query_block, key_block, value_block = blocks
        scores = jnp.einsum('qhd,khd->hqk', query_block.astype(jnp.float32), key_block.astype(jnp.float32)) * scaling
        scores = jnp.where(allowed[None], scores, NEG)
        highest = lax.optimization_barrier(jnp.max(scores, axis=-1))
        log_total = highest + jnp.log(lax.optimization_barrier(jnp.sum(jnp.exp(scores - highest[..., None]), axis=-1)))
        weights = jnp.exp(scores - log_total[..., None]).astype(jnp.bfloat16)
        combined = jnp.einsum('hqk,khd->qhd', weights.astype(jnp.float32), value_block.astype(jnp.float32)).astype(jnp.bfloat16)
        return (combined, log_total)
    combined, log_total = lax.map(one_group, (head_split(query_part), head_split(key_part), head_split(value_part)))
    return (head_join(combined), log_total)

def attention_backward(query_part, key_part, value_part, attended, attended_grad, log_total, allowed):
    scaling = HEAD_DIM ** (-0.5)

    def one_group(blocks):
        query_block, key_block, value_block, out_block, grad_block, lse_block = blocks
        query_wide = query_block.astype(jnp.float32)
        key_wide = key_block.astype(jnp.float32)
        grad_wide = grad_block.astype(jnp.float32)
        scores = jnp.einsum('qhd,khd->hqk', query_wide, key_wide) * scaling
        scores = jnp.where(allowed[None], scores, NEG)
        weights = jnp.exp(scores - lse_block[..., None])
        weights_half = weights.astype(jnp.bfloat16)
        value_grad = jnp.einsum('hqk,qhd->khd', weights_half.astype(jnp.float32), grad_wide)
        weight_grad = jnp.einsum('qhd,khd->hqk', grad_wide, value_block.astype(jnp.float32))
        delta = lax.optimization_barrier(jnp.sum(grad_wide * out_block.astype(jnp.float32), axis=-1)).transpose(1, 0)
        mix_half = (weights * (weight_grad - delta[..., None])).astype(jnp.bfloat16)
        mix_wide = mix_half.astype(jnp.float32)
        query_grad = jnp.einsum('hqk,khd->qhd', mix_wide, key_wide) * scaling
        key_grad = jnp.einsum('hqk,qhd->khd', mix_wide, query_wide) * scaling
        return (query_grad, key_grad, value_grad)
    query_grad, key_grad, value_grad = lax.map(one_group, (head_split(query_part), head_split(key_part), head_split(value_part), head_split(attended), head_split(attended_grad), log_total))
    return (head_join(query_grad), head_join(key_grad), head_join(value_grad))

def group_pass(tokens, segments, cotangent, params):
    first_gain, first_shift, triple_weight, query_bias, value_bias, proj_weight, proj_bias, second_gain, second_shift, expand_weight, expand_bias, shrink_weight, shrink_bias = params
    width = HEADS * HEAD_DIM
    rows = tokens.shape[0]
    tokens_wide = tokens.astype(jnp.float32)
    first_normed, first_hat, first_rstd = norm_forward(tokens_wide, first_gain, first_shift)
    first_half = first_normed.astype(jnp.bfloat16)
    full_bias = jnp.concatenate([query_bias, jnp.zeros((width,), jnp.float32), value_bias])
    triple = (jnp.dot(first_half, triple_weight, preferred_element_type=jnp.float32) + full_bias).astype(jnp.bfloat16)
    query_part = triple[:, :width]
    key_part = triple[:, width:2 * width]
    value_part = triple[:, 2 * width:]
    places = jnp.arange(rows, dtype=jnp.int32)
    allowed = (segments[:, None] == segments[None, :]) & (places[None, :] <= places[:, None])
    attended, log_total = attention_forward(query_part, key_part, value_part, allowed)
    middle = tokens_wide + jnp.dot(attended, proj_weight, preferred_element_type=jnp.float32) + proj_bias
    second_normed, second_hat, second_rstd = norm_forward(middle, second_gain, second_shift)
    second_half = second_normed.astype(jnp.bfloat16)
    before_act = jnp.dot(second_half, expand_weight, preferred_element_type=jnp.float32) + expand_bias
    activated = gelu_tanh(before_act).astype(jnp.bfloat16)
    block_out = (middle + jnp.dot(activated, shrink_weight, preferred_element_type=jnp.float32) + shrink_bias).astype(jnp.bfloat16)
    cot_wide = cotangent.astype(jnp.float32)
    shrink_grad = jnp.dot(activated.T, cotangent, preferred_element_type=jnp.float32)
    shrink_bias_grad = lax.optimization_barrier(jnp.sum(cot_wide, axis=0))
    act_grad = jnp.dot(cotangent, shrink_weight.T, preferred_element_type=jnp.float32)
    gelu_back = jax.vjp(gelu_tanh, before_act)[1]
    before_grad = gelu_back(act_grad)[0]
    expand_bias_grad = lax.optimization_barrier(jnp.sum(before_grad, axis=0))
    hidden_grad = before_grad.astype(jnp.bfloat16)
    expand_grad = jnp.dot(second_half.T, hidden_grad, preferred_element_type=jnp.float32)
    second_normed_grad = jnp.dot(hidden_grad, expand_weight.T, preferred_element_type=jnp.float32)
    middle_grad = cot_wide + norm_backward(second_normed_grad, second_hat, second_rstd, second_gain)
    second_gain_grad = lax.optimization_barrier(jnp.sum(second_normed_grad * second_hat, axis=0))
    second_shift_grad = lax.optimization_barrier(jnp.sum(second_normed_grad, axis=0))
    middle_half = middle_grad.astype(jnp.bfloat16)
    proj_grad = jnp.dot(attended.T, middle_half, preferred_element_type=jnp.float32)
    proj_bias_grad = lax.optimization_barrier(jnp.sum(middle_grad, axis=0))
    attended_grad = jnp.dot(middle_half, proj_weight.T, preferred_element_type=jnp.float32).astype(jnp.bfloat16)
    query_grad, key_grad, value_grad = attention_backward(query_part, key_part, value_part, attended, attended_grad, log_total, allowed)
    query_bias_grad = lax.optimization_barrier(jnp.sum(query_grad, axis=0))
    value_bias_grad = lax.optimization_barrier(jnp.sum(value_grad, axis=0))
    triple_half = jnp.concatenate([query_grad, key_grad, value_grad], axis=1).astype(jnp.bfloat16)
    triple_grad = jnp.dot(first_half.T, triple_half, preferred_element_type=jnp.float32)
    first_normed_grad = jnp.dot(triple_half, triple_weight.T, preferred_element_type=jnp.float32)
    input_grad = middle_grad + norm_backward(first_normed_grad, first_hat, first_rstd, first_gain)
    first_gain_grad = lax.optimization_barrier(jnp.sum(first_normed_grad * first_hat, axis=0))
    first_shift_grad = lax.optimization_barrier(jnp.sum(first_normed_grad, axis=0))
    grads = (first_gain_grad, first_shift_grad, triple_grad, query_bias_grad, value_bias_grad, proj_grad, proj_bias_grad, second_gain_grad, second_shift_grad, expand_grad, expand_bias_grad, shrink_grad, shrink_bias_grad)
    return (block_out, input_grad, grads)

def reference(tokens, segment_ids, first_gain, first_shift, triple_weight, query_bias, value_bias, proj_weight, proj_bias, second_gain, second_shift, expand_weight, expand_bias, shrink_weight, shrink_bias, cotangent):
    width = HEADS * HEAD_DIM
    params = (first_gain, first_shift, triple_weight, query_bias, value_bias, proj_weight, proj_bias, second_gain, second_shift, expand_weight, expand_bias, shrink_weight, shrink_bias)
    token_groups = tokens.reshape(N_DP, TOK_GRP, width)
    cot_groups = cotangent.reshape(N_DP, TOK_GRP, width)
    start = tuple((jnp.zeros(param.shape, jnp.float32) for param in params))

    def one_step(carry, blocks):
        group_tokens, group_segments, group_cot = blocks
        block_out, input_grad, grads = group_pass(group_tokens, group_segments, group_cot, params)
        return (tuple((first_term + second_term for first_term, second_term in zip(carry, grads))), (block_out, input_grad))
    totals, (outs_grouped, grads_grouped) = lax.scan(one_step, start, (token_groups, segment_ids, cot_groups))
    first_gain_grad, first_shift_grad, triple_grad, query_bias_grad, value_bias_grad, proj_grad, proj_bias_grad, second_gain_grad, second_shift_grad, expand_grad, expand_bias_grad, shrink_grad, shrink_bias_grad = totals
    return (outs_grouped.reshape(N_DP * TOK_GRP, width), grads_grouped.reshape(N_DP * TOK_GRP, width), first_gain_grad, first_shift_grad, triple_grad.reshape(N_COL, width // N_COL, 3 * width), query_bias_grad, value_bias_grad, proj_grad.reshape(N_ROW, width // N_ROW, width), proj_bias_grad, second_gain_grad, second_shift_grad, expand_grad.reshape(N_COL, width // N_COL, FF), expand_bias_grad, shrink_grad.reshape(N_ROW, FF // N_ROW, width), shrink_bias_grad)
```

```python
import functools

import jax
import jax.numpy as jnp
from jax import lax
from jax.experimental import pallas as pl
from jax.experimental.pallas import tpu as pltpu
from jax.sharding import PartitionSpec as P

HEADS = 25
HEAD_DIM = 64
EPS = 1e-05
NEG = -1e30
GRAIN = 16
AXES = ("dp", "row", "col")
MESH = pl.DeviceIdType.MESH
F32 = jnp.float32
BF16 = jnp.bfloat16
VMEM_BYTES = 60 * 1024 * 1024

NN = (((1,), (0,)), ((), ()))
NT = (((1,), (1,)), ((), ()))
TN = (((0,), (0,)), ((), ()))


def dot(left, right, dims):
    return lax.dot_general(left, right, dims, preferred_element_type=F32)


class Place:
    def __init__(self):
        self.d = lax.axis_index("dp")
        self.r = lax.axis_index("row")
        self.c = lax.axis_index("col")
        one = self.r + 1 - 2 * lax.rem(self.r, 2)
        two = lax.rem(self.r + 2, 4)
        self.a = 1 + self.c
        self.b = 2 - self.c
        self.ra = (1 - self.c) * one + self.c * two
        self.rb = self.c * one + (1 - self.c) * two
        self.r3 = 3 - self.r

    def dev(self, row, col=None):
        return (self.d, row, self.c if col is None else col)

    def mate(self):
        return (self.d, self.r, 1 - self.c)

    def barrier(self, devices):
        semaphore = pltpu.get_barrier_semaphore()
        for device in devices:
            pl.semaphore_signal(semaphore, inc=1, device_id=device, device_id_type=MESH)
        pl.semaphore_wait(semaphore, len(devices))

    def group(self):
        flat = 2 * self.r + self.c
        found = []
        for step in range(1, 8):
            other = lax.rem(flat + step, 8)
            found.append((self.d, other // 2, lax.rem(other, 2)))
        return found

    def square(self):
        return [self.mate(), self.dev(self.ra), self.dev(self.rb)]


def rcopy(src, dst, send, recv, device):
    return pltpu.make_async_remote_copy(
        src_ref=src, dst_ref=dst, send_sem=send, recv_sem=recv, device_id=device,
        device_id_type=MESH,
    )


def lanes(index, size):
    return pl.ds(pl.multiple_of(index * size, size), size)


def call(kernel, out_shapes, out_specs, in_specs, scratch, cid, flops=0, bytes_accessed=0):
    return pl.pallas_call(
        kernel,
        out_shape=out_shapes,
        in_specs=in_specs,
        out_specs=out_specs,
        scratch_shapes=scratch,
        compiler_params=pltpu.CompilerParams(
            collective_id=cid, has_side_effects=True, vmem_limit_bytes=VMEM_BYTES
        ),
    )


VM = pl.BlockSpec(memory_space=pltpu.VMEM)
ANY = pl.BlockSpec(memory_space=pl.ANY)
DMA = pltpu.SemaphoreType.DMA


def gather_scratch(rows, cols):
    return [pltpu.VMEM((2, 4, rows, cols), BF16), DMA((7,)), DMA((2, 4)), DMA((4,))]


def run_gather(place, x_ref, all_ref, got, send, recv, out_sem, work):
    mate = place.mate()
    to_mate = rcopy(x_ref, got.at[1, 0], send.at[0], recv.at[1, 0], mate)
    to_a = rcopy(x_ref, got.at[0, place.a], send.at[1], recv.at[0, place.a], place.dev(place.ra))
    to_b = rcopy(x_ref, got.at[0, place.b], send.at[2], recv.at[0, place.b], place.dev(place.rb))
    to_a.start()
    to_b.start()
    to_mate.start()
    got[0, 0] = x_ref[...]
    own_out = pltpu.make_async_copy(x_ref, all_ref.at[place.r], out_sem.at[0])
    own_out.start()

    def forward(slot, number):
        copy = rcopy(got.at[0, slot], got.at[1, slot], send.at[number], recv.at[1, slot], mate)
        copy.start()
        return copy

    def keep(slot, row, number):
        copy = pltpu.make_async_copy(got.at[0, slot], all_ref.at[row], out_sem.at[number])
        copy.start()
        return copy

    to_mate.wait_recv()
    work(0, place.r)
    to_a.wait_recv()
    relay = rcopy(
        got.at[0, place.a], got.at[0, 3], send.at[3], recv.at[0, 3], place.dev(place.rb)
    )
    relay.start()
    fwd_a = forward(place.a, 4)
    keep_a = keep(place.a, place.ra, 1)
    to_b.wait_recv()
    fwd_b = forward(place.b, 5)
    keep_b = keep(place.b, place.rb, 2)
    fwd_b.wait_recv()
    work(place.b, place.rb)
    fwd_a.wait_recv()
    work(place.a, place.ra)
    relay.wait_recv()
    fwd_3 = forward(3, 6)
    keep_3 = keep(3, place.r3, 3)
    fwd_3.wait_recv()
    work(3, place.r3)
    for copy in (to_mate, to_a, to_b, relay, fwd_a, fwd_b, fwd_3):
        copy.wait_send()
    for copy in (own_out, keep_a, keep_b, keep_3):
        copy.wait()


def gather_linear(x, w_own, w_oth, dims, transposed, out_dtype, cid):
    rows, cols = x.shape
    feats = w_own.shape[0] if dims == NT else w_own.shape[1]
    shape = (feats, 4 * rows) if transposed else (4, rows, feats)

    def kernel(x_ref, wo_ref, wn_ref, all_ref, y_ref, got, send, recv, out_sem):
        place = Place()
        place.barrier(place.square())

        def work(slot, row):
            if transposed:
                total = dot(wo_ref[...], got[0, slot], NT) + dot(wn_ref[...], got[1, slot], NT)
                y_ref[:, lanes(row, rows)] = total.astype(out_dtype)
            else:
                total = dot(got[0, slot], wo_ref[...], dims) + dot(got[1, slot], wn_ref[...], dims)
                y_ref[row] = total.astype(out_dtype)

        run_gather(place, x_ref, all_ref, got, send, recv, out_sem, work)

    return call(
        kernel,
        (jax.ShapeDtypeStruct((4, rows, cols), BF16), jax.ShapeDtypeStruct(shape, out_dtype)),
        (ANY, VM), [VM, VM, VM], gather_scratch(rows, cols), cid,
    )(x, w_own, w_oth)


def gather_triple(x, w_own, w_oth, bias, width, triple_width, cid):
    rows, cols = x.shape
    feats = w_own.shape[0]
    grains = feats // GRAIN
    shift = triple_width - feats
    per = 3 * HEAD_DIM

    def kernel(x_ref, wo_ref, wn_ref, b_ref, all_ref, h_ref, got, tt, send, recv, out_sem, gs, gr):
        place = Place()
        place.barrier(place.group())
        me = 2 * place.r + place.c

        def target(j):
            feature = triple_width * place.r + shift * place.c + GRAIN * j
            part = feature // width
            inner = feature - part * width
            head = inner // HEAD_DIM
            owner = jnp.minimum(head // 3, 7)
            row = (head - 3 * owner) * per + part * HEAD_DIM + (inner - head * HEAD_DIM)
            return owner, pl.ds(pl.multiple_of(row, GRAIN), GRAIN)

        def work(slot, row):
            total = dot(wo_ref[...], got[0, slot], NT) + dot(wn_ref[...], got[1, slot], NT)
            tt[:, lanes(row, rows)] = (total + b_ref[...]).astype(BF16)

            def send_grain(j, carry):
                owner, place_rows = target(j)
                src = tt.at[pl.ds(pl.multiple_of(GRAIN * j, GRAIN), GRAIN), lanes(row, rows)]
                dst = h_ref.at[place_rows, lanes(row, rows)]

                @pl.when(owner == me)
                def _():
                    pltpu.make_async_copy(src, dst, gr).start()

                @pl.when(owner != me)
                def _():
                    rcopy(src, dst, gs, gr, (place.d, owner // 2, lax.rem(owner, 2))).start()

                return carry

            lax.fori_loop(place.c, grains, send_grain, 0)

        run_gather(place, x_ref, all_ref, got, send, recv, out_sem, work)

        def sent(j, count):
            return count + jnp.where(target(j)[0] == me, 0, 1)

        def drain(j, carry):
            @pl.when(target(j)[0] != me)
            def _():
                src = tt.at[pl.ds(0, GRAIN)]
                pltpu.make_async_copy(src, src, gs).wait()

            return carry

        lax.fori_loop(place.c, grains, drain, 0)

        @pl.when(me == 7)
        def _():
            pltpu.make_async_copy(h_ref, h_ref, gr).wait()

        @pl.when(me != 7)
        def _():
            part = h_ref.at[pl.ds(0, 3 * per)]
            pltpu.make_async_copy(part, part, gr).wait()

    scratch = gather_scratch(rows, cols)
    scratch.insert(1, pltpu.VMEM((feats, 4 * rows), BF16))
    return call(
        kernel,
        (
            jax.ShapeDtypeStruct((4, rows, cols), BF16),
            jax.ShapeDtypeStruct((4 * per, 4 * rows), BF16),
        ),
        (ANY, ANY), [VM] * 4, scratch + [DMA, DMA], cid,
    )(x, w_own, w_oth, bias)


def gather_hidden(x, w_own, w_oth, bias, act_grad, cid):
    rows, cols = x.shape
    feats = w_own.shape[1]

    def kernel(
        x_ref, wo_ref, wn_ref, b_ref, g_ref, all_ref, act_ref, hid_ref, sum_ref,
        got, act, hid, send, recv, out_sem, swap_send, swap_recv, swap_out,
    ):
        place = Place()
        place.barrier(place.square())
        mate = place.mate()
        sum_ref[...] = jnp.zeros_like(sum_ref)
        pending = []

        def work(slot, row):
            number = len(pending)
            p = dot(got[0, slot], wo_ref[...], NN) + dot(got[1, slot], wn_ref[...], NN) + b_ref[...]
            square = p * p
            t = jnp.tanh(0.7978845608028654 * (p + 0.044715 * (square * p)))
            act[number] = (0.5 * p * (1.0 + t)).astype(BF16)
            slope = 0.5 * (1.0 + t) + 0.5 * p * (1.0 - t * t) * (
                0.7978845608028654 * (1.0 + 3.0 * 0.044715 * square)
            )
            grad = g_ref[row] * slope
            hid[number] = grad.astype(BF16)
            sum_ref[...] += jnp.sum(grad, axis=0, keepdims=True)
            copies = []
            for k, (buf, out) in enumerate(((act, act_ref), (hid, hid_ref))):
                there = out.at[place.c, row]
                out_copy = pltpu.make_async_copy(buf.at[number], there, swap_out.at[k, number])
                swap = rcopy(
                    buf.at[number], there, swap_send.at[k, number], swap_recv.at[k, number], mate
                )
                out_copy.start()
                swap.start()
                copies += [out_copy, swap]
            pending.append(copies)

        run_gather(place, x_ref, all_ref, got, send, recv, out_sem, work)
        for copies in pending:
            for copy in copies:
                copy.wait()

    full = jax.ShapeDtypeStruct((2, 4, rows, feats), BF16)
    return call(
        kernel,
        (
            jax.ShapeDtypeStruct((4, rows, cols), BF16), full, full,
            jax.ShapeDtypeStruct((1, feats), F32),
        ),
        (ANY, ANY, ANY, VM), [VM] * 5,
        [gather_scratch(rows, cols)[0], pltpu.VMEM((4, rows, feats), BF16),
         pltpu.VMEM((4, rows, feats), BF16)] + gather_scratch(rows, cols)[1:]
        + [DMA((2, 4)), DMA((2, 4)), DMA((2, 4))],
        cid,
    )(x, w_own, w_oth, bias, act_grad)


def scatter_scratch(rows, cols):
    return [
        pltpu.VMEM((3, rows, cols), BF16), pltpu.VMEM((3, rows, cols), BF16), DMA((3,)), DMA((3,))
    ]


def run_scatter(place, block, out_ref, outbox, inbox, send, recv):
    dev_a, dev_b = place.dev(place.ra), place.dev(place.rb)
    outbox[0] = block(place.r3).astype(BF16)
    first = rcopy(outbox.at[0], inbox.at[0], send.at[0], recv.at[0], dev_a)
    first.start()
    outbox[1] = block(place.ra).astype(BF16)
    second = rcopy(outbox.at[1], inbox.at[1], send.at[1], recv.at[1], dev_a)
    second.start()
    passed = block(place.rb)
    first.wait_recv()
    outbox[2] = (passed + inbox[0].astype(F32)).astype(BF16)
    third = rcopy(outbox.at[2], inbox.at[2], send.at[2], recv.at[2], dev_b)
    third.start()
    own = block(place.r)
    second.wait_recv()
    own = own + inbox[1].astype(F32)
    third.wait_recv()
    out_ref[...] = own + inbox[2].astype(F32)
    for copy in (first, second, third):
        copy.wait_send()


def pair_scatter(left, w_own, w_oth, dims, cid):
    rows = left.shape[2]
    cols = w_own.shape[0] if dims == NT else w_own.shape[1]

    def kernel(l_ref, wo_ref, wn_ref, out_ref, outbox, inbox, send, recv):
        place = Place()
        place.barrier([place.dev(place.ra), place.dev(place.rb)])

        def block(row):
            return dot(l_ref[place.c, row], wo_ref[...], dims) + dot(
                l_ref[1 - place.c, row], wn_ref[...], dims
            )

        run_scatter(place, block, out_ref, outbox, inbox, send, recv)

    return call(
        kernel, jax.ShapeDtypeStruct((rows, cols), F32), VM, [VM] * 3,
        scatter_scratch(rows, cols), cid,
    )(left, w_own, w_oth)


def attended_scatter(heads, weight, cid):
    feats, cols = weight.shape
    tokens = heads.shape[1]
    rows = tokens // 4

    def kernel(h_ref, w_ref, all_ref, out_ref, full, outbox, inbox, send, recv, gs, gr, keep):
        place = Place()
        place.barrier(place.group())
        me = 2 * place.r + place.c
        count = jnp.where(me == 7, 4, 3) * (HEAD_DIM // GRAIN)

        def send_grain(j, carry):
            feature = 3 * HEAD_DIM * me + GRAIN * j
            owner = feature // feats
            src = h_ref.at[pl.ds(pl.multiple_of(GRAIN * j, GRAIN), GRAIN)]
            dst = full.at[pl.ds(pl.multiple_of(feature - owner * feats, GRAIN), GRAIN)]
            rcopy(src, dst, gs, gr, (place.d, owner, 1 - place.c)).start()

            @pl.when(owner == place.r)
            def _():
                pltpu.make_async_copy(src, dst, gr).start()

            @pl.when(owner != place.r)
            def _():
                rcopy(src, dst, gs, gr, (place.d, owner, place.c)).start()

            return carry

        lax.fori_loop(0, count, send_grain, 0)

        def drain(j, carry):
            feature = 3 * HEAD_DIM * me + GRAIN * j
            src = h_ref.at[pl.ds(0, GRAIN)]
            pltpu.make_async_copy(src, src, gs).wait()

            @pl.when(feature // feats != place.r)
            def _():
                pltpu.make_async_copy(src, src, gs).wait()

            return carry

        lax.fori_loop(0, count, drain, 0)
        pltpu.make_async_copy(full, full, gr).wait()
        kept = pltpu.make_async_copy(full, all_ref, keep)
        kept.start()

        def block(row):
            return dot(full[:, lanes(row, rows)], w_ref[...], TN)

        run_scatter(place, block, out_ref, outbox, inbox, send, recv)
        kept.wait()

    return call(
        kernel,
        (jax.ShapeDtypeStruct((feats, tokens), BF16), jax.ShapeDtypeStruct((rows, cols), F32)),
        (ANY, VM), [VM, VM],
        [pltpu.VMEM((feats, tokens), BF16)] + scatter_scratch(rows, cols) + [DMA, DMA, DMA], cid,
    )(heads, weight)


def triple_scatter(heads, weight, width, cid):
    feats, cols = weight.shape
    tokens = heads.shape[1]
    rows = tokens // 4
    per = 3 * HEAD_DIM
    low = (feats // GRAIN + 1) // 2 * GRAIN

    def kernel(h_ref, w_ref, all_ref, out_ref, full, outbox, inbox, send, recv, gs, gr, ms, mr, keep):
        place = Place()
        place.barrier(place.group())
        me = 2 * place.r + place.c
        count = jnp.where(me == 7, 4, 3) * (per // GRAIN)

        def target(j):
            row = GRAIN * j
            head = row // per
            rest = row - head * per
            part = rest // HEAD_DIM
            feature = part * width + (3 * me + head) * HEAD_DIM + rest - part * HEAD_DIM
            owner = feature // feats
            inner = feature - owner * feats
            return 2 * owner + inner // low, inner

        def send_grain(j, carry):
            owner, inner = target(j)
            src = h_ref.at[pl.ds(pl.multiple_of(GRAIN * j, GRAIN), GRAIN)]
            dst = full.at[pl.ds(pl.multiple_of(inner, GRAIN), GRAIN)]

            @pl.when(owner == me)
            def _():
                pltpu.make_async_copy(src, dst, gr).start()

            @pl.when(owner != me)
            def _():
                rcopy(src, dst, gs, gr, (place.d, owner // 2, lax.rem(owner, 2))).start()

            return carry

        lax.fori_loop(0, count, send_grain, 0)

        def drain(j, carry):
            @pl.when(target(j)[0] != me)
            def _():
                src = h_ref.at[pl.ds(0, GRAIN)]
                pltpu.make_async_copy(src, src, gs).wait()

            return carry

        lax.fori_loop(0, count, drain, 0)
        lower, upper = full.at[pl.ds(0, low)], full.at[pl.ds(low, feats - low)]

        def swap(mine, theirs):
            pltpu.make_async_copy(mine, mine, gr).wait()
            copy = rcopy(mine, mine, ms, mr, place.mate())
            copy.start()
            copy.wait_send()
            pltpu.make_async_copy(theirs, theirs, mr).wait()

        @pl.when(place.c == 0)
        def _():
            swap(lower, upper)

        @pl.when(place.c == 1)
        def _():
            swap(upper, lower)

        kept = pltpu.make_async_copy(full, all_ref, keep)
        kept.start()

        def block(row):
            return dot(full[:, lanes(row, rows)], w_ref[...], TN)

        run_scatter(place, block, out_ref, outbox, inbox, send, recv)
        kept.wait()

    return call(
        kernel,
        (jax.ShapeDtypeStruct((feats, tokens), BF16), jax.ShapeDtypeStruct((rows, cols), F32)),
        (ANY, VM), [VM, VM],
        [pltpu.VMEM((feats, tokens), BF16)] + scatter_scratch(rows, cols)
        + [DMA, DMA, DMA, DMA, DMA], cid,
    )(heads, weight)


def attention_bias(seg_col, seg_row, bias_ref):
    tokens = seg_row.shape[1]
    key = lax.broadcasted_iota(jnp.int32, (tokens, tokens), 0)
    query = lax.broadcasted_iota(jnp.int32, (tokens, tokens), 1)
    allowed = (seg_col[...] == seg_row[...]) & (key <= query)
    bias_ref[...] = jnp.where(allowed, 0.0, NEG)


def holds(head):
    return (head < 3) | ((lax.axis_index("row") == 3) & (lax.axis_index("col") == 1))


def attention_forward(triple, seg_col, seg_row):
    per = 3 * HEAD_DIM
    tokens = triple.shape[1]
    span = tokens // 4

    def kernel(sc_ref, sr_ref, t_ref, o_ref, l_ref, bias_ref):
        @pl.when(pl.program_id(0) == 0)
        def _():
            attention_bias(sc_ref, sr_ref, bias_ref)

        @pl.when(holds(pl.program_id(0)))
        def _():
            for j in range(4):
                reach, here = (j + 1) * span, slice(j * span, (j + 1) * span)
                query = t_ref[0:HEAD_DIM, here] * BF16(HEAD_DIM ** (-0.5))
                score = dot(t_ref[HEAD_DIM : 2 * HEAD_DIM, 0:reach], query, TN)
                score = score + bias_ref[0:reach, here]
                top = jnp.max(score, axis=0, keepdims=True)
                weight = jnp.exp(score - top)
                total = jnp.sum(weight, axis=0, keepdims=True)
                mixed = dot(t_ref[2 * HEAD_DIM : per, 0:reach], weight.astype(BF16), NN)
                o_ref[:, here] = (mixed / total).astype(BF16)
                l_ref[0, :, here] = top + jnp.log(total)

    return pl.pallas_call(
        kernel,
        grid=(4,),
        out_shape=(
            jax.ShapeDtypeStruct((4 * HEAD_DIM, tokens), BF16),
            jax.ShapeDtypeStruct((4, 1, tokens), F32),
        ),
        in_specs=[
            pl.BlockSpec((tokens, 1), lambda h: (0, 0)),
            pl.BlockSpec((1, tokens), lambda h: (0, 0)),
            pl.BlockSpec((per, tokens), lambda h: (h, 0)),
        ],
        out_specs=(
            pl.BlockSpec((HEAD_DIM, tokens), lambda h: (h, 0)),
            pl.BlockSpec((1, 1, tokens), lambda h: (h, 0, 0)),
        ),
        scratch_shapes=[pltpu.VMEM((tokens, tokens), F32)],
        compiler_params=pltpu.CompilerParams(vmem_limit_bytes=VMEM_BYTES),
    )(seg_col, seg_row, triple)


def attention_backward(triple, seg_col, seg_row, attended, attended_grad, lse):
    per = 3 * HEAD_DIM
    tokens = triple.shape[1]
    span = tokens // 4

    def kernel(sc_ref, sr_ref, t_ref, o_ref, g_ref, l_ref, d_ref, bias_ref, kg_ref, vg_ref):
        @pl.when(pl.program_id(0) == 0)
        def _():
            attention_bias(sc_ref, sr_ref, bias_ref)

        @pl.when(holds(pl.program_id(0)))
        def _():
            kg_ref[...] = jnp.zeros_like(kg_ref)
            vg_ref[...] = jnp.zeros_like(vg_ref)
            for j in range(4):
                reach, here = (j + 1) * span, slice(j * span, (j + 1) * span)
                query = t_ref[0:HEAD_DIM, here] * BF16(HEAD_DIM ** (-0.5))
                key = t_ref[HEAD_DIM : 2 * HEAD_DIM, 0:reach]
                grad = g_ref[:, here]
                delta = jnp.sum(
                    grad.astype(F32) * o_ref[:, here].astype(F32), axis=0, keepdims=True
                )
                score = dot(key, query, TN) + bias_ref[0:reach, here]
                prob = jnp.exp(score - l_ref[0, :, here])
                vg_ref[:, 0:reach] += dot(grad, prob.astype(BF16), NT)
                back = dot(t_ref[2 * HEAD_DIM : per, 0:reach], grad, TN)
                mix = (prob * (back - delta)).astype(BF16)
                d_ref[0:HEAD_DIM, here] = (dot(key, mix, NN) * HEAD_DIM ** (-0.5)).astype(BF16)
                kg_ref[:, 0:reach] += dot(query, mix, NT)
            d_ref[HEAD_DIM : 2 * HEAD_DIM, :] = kg_ref[...].astype(BF16)
            d_ref[2 * HEAD_DIM : per, :] = vg_ref[...].astype(BF16)

    return pl.pallas_call(
        kernel,
        grid=(4,),
        out_shape=jax.ShapeDtypeStruct((4 * per, tokens), BF16),
        in_specs=[
            pl.BlockSpec((tokens, 1), lambda h: (0, 0)),
            pl.BlockSpec((1, tokens), lambda h: (0, 0)),
            pl.BlockSpec((per, tokens), lambda h: (h, 0)),
            pl.BlockSpec((HEAD_DIM, tokens), lambda h: (h, 0)),
            pl.BlockSpec((HEAD_DIM, tokens), lambda h: (h, 0)),
            pl.BlockSpec((1, 1, tokens), lambda h: (h, 0, 0)),
        ],
        out_specs=pl.BlockSpec((per, tokens), lambda h: (h, 0)),
        scratch_shapes=[
            pltpu.VMEM((tokens, tokens), F32),
            pltpu.VMEM((HEAD_DIM, tokens), F32),
            pltpu.VMEM((HEAD_DIM, tokens), F32),
        ],
        compiler_params=pltpu.CompilerParams(vmem_limit_bytes=VMEM_BYTES),
    )(seg_col, seg_row, triple, attended, attended_grad, lse)


def sum_all(pieces, sizes, cid):
    count = pieces.shape[0]
    rows, cols = sizes

    def kernel(x_ref, out_ref, inbox, piece, sems):
        me = (lax.axis_index("dp") * rows + lax.axis_index("row")) * cols + lax.axis_index("col")

        def dev(step):
            flat = lax.rem(me + step, count)
            return flat, (flat // (rows * cols), lax.rem(flat // cols, rows), lax.rem(flat, cols))

        semaphore = pltpu.get_barrier_semaphore()

        def greet(step, carry):
            pl.semaphore_signal(semaphore, inc=1, device_id=dev(step)[1], device_id_type=MESH)
            return carry

        lax.fori_loop(1, count, greet, 0)
        pl.semaphore_wait(semaphore, count - 1)

        def spread(step, carry):
            flat, device = dev(step)
            rcopy(x_ref.at[flat], inbox.at[me], sems.at[0], sems.at[1], device).start()
            return carry

        lax.fori_loop(1, count, spread, 0)
        inbox[me] = x_ref[me]
        rest = inbox.at[pl.ds(0, count - 1)]
        pltpu.make_async_copy(rest, rest, sems.at[1]).wait()
        pltpu.make_async_copy(rest, rest, sems.at[0]).wait()
        piece[...] = jnp.sum(inbox[...], axis=0)

        def share(step, carry):
            rcopy(piece, out_ref.at[me], sems.at[2], sems.at[3], dev(step)[1]).start()
            return carry

        lax.fori_loop(1, count, share, 0)
        out_ref[me] = piece[...]
        rest = out_ref.at[pl.ds(0, count - 1)]
        pltpu.make_async_copy(rest, rest, sems.at[3]).wait()
        pltpu.make_async_copy(rest, rest, sems.at[2]).wait()

    return call(
        kernel, jax.ShapeDtypeStruct(pieces.shape, F32), VM, [VM],
        [pltpu.VMEM(pieces.shape, F32), pltpu.VMEM(pieces.shape[1:], F32), DMA((4,))], cid,
    )(pieces)


def feature_totals(first_term, second_term):
    return lax.psum(
        (jnp.sum(first_term, axis=1, keepdims=True), jnp.sum(second_term, axis=1, keepdims=True)),
        "col",
    )


def norm_local(matrix, gain, shift):
    width = HEADS * HEAD_DIM
    total, square = feature_totals(matrix, matrix * matrix)
    average = total / width
    rstd = lax.rsqrt(square / width - average * average + EPS)
    normed_hat = (matrix - average) * rstd
    return (normed_hat * gain + shift, normed_hat, rstd)


def norm_back(grad_in, normed_hat, rstd, gain):
    width = HEADS * HEAD_DIM
    scaled = grad_in * gain
    total, mixed = feature_totals(scaled, scaled * normed_hat)
    return rstd * (scaled - total / width - normed_hat * mixed / width)


def swap(block):
    return lax.ppermute(block, "col", [(0, 1), (1, 0)])


def shards(
    tokens, segment_ids, first_gain, first_shift, triple_weight, query_bias, value_bias,
    proj_weight, proj_bias, second_gain, second_shift, expand_weight, expand_bias,
    shrink_weight, shrink_bias, cotangent, *, axis_sizes,
):
    width = HEADS * HEAD_DIM
    dp_count, row_count, col_count = axis_sizes
    row, col = lax.axis_index("row"), lax.axis_index("col")
    rows, col_width = tokens.shape
    triple_width = triple_weight.shape[1]
    proj_rows = proj_weight.shape[0]
    hidden = expand_weight.shape[1] // 2

    def col_slice(vector):
        return lax.dynamic_slice_in_dim(vector, col * col_width, col_width)

    def halves(matrix, size, axis):
        step = matrix.shape[axis] - size
        return (
            lax.dynamic_slice_in_dim(matrix, col * step, size, axis),
            lax.dynamic_slice_in_dim(matrix, (1 - col) * step, size, axis),
        )

    triple_t = triple_weight.T
    core_feats = (triple_width // GRAIN + 1) // 2 * GRAIN
    triple_own, triple_theirs = halves(triple_t, core_feats, 0)
    triple_oth = swap(triple_theirs)
    expand_own, expand_theirs = halves(expand_weight, hidden, 1)
    expand_oth = swap(expand_theirs)
    shrink_own, shrink_theirs = halves(shrink_weight, hidden, 0)
    shrink_oth = swap(shrink_theirs)
    head_rows = 3 * HEAD_DIM
    lag = (row_count - 1) * (proj_rows - 2 * head_rows)
    before = lax.ppermute(
        proj_weight[proj_rows - lag :], "row", [(i, i + 1) for i in range(row_count - 1)]
    )
    padded = jnp.concatenate(
        [before, proj_weight, jnp.zeros((2 * HEAD_DIM, col_width), BF16)], axis=0
    )
    start = lag - (proj_rows - 2 * head_rows) * row
    proj_own = lax.dynamic_slice_in_dim(padded, start + head_rows * col, 4 * HEAD_DIM, 0)
    proj_theirs = lax.dynamic_slice_in_dim(
        padded, start + head_rows * (1 - col), 4 * HEAD_DIM, 0
    )
    proj_oth = swap(proj_theirs)
    full_bias = jnp.concatenate([query_bias, jnp.zeros((width,), F32), value_bias])
    core_bias = lax.dynamic_slice_in_dim(
        full_bias, row * triple_width + col * (triple_width - core_feats), core_feats
    )[:, None]
    core_expand_bias = lax.dynamic_slice_in_dim(
        expand_bias, (row * 2 + col) * hidden, hidden
    )[None, :]
    seg_row = segment_ids
    seg_col = segment_ids.reshape(-1, 1)

    tokens_wide = tokens.astype(F32)
    first_normed, first_hat, first_rstd = norm_local(
        tokens_wide, col_slice(first_gain), col_slice(first_shift)
    )
    first_all, triple = gather_triple(
        first_normed.astype(BF16), triple_own, triple_oth, core_bias, width, triple_width, 0
    )
    cot_all, act_grad = gather_linear(cotangent, shrink_own, shrink_oth, NT, False, F32, 1)
    attended, lse = attention_forward(triple, seg_col, seg_row)
    attended_all, proj_out = attended_scatter(attended, proj_weight, 2)
    middle = tokens_wide + proj_out + col_slice(proj_bias)
    second_normed, second_hat, second_rstd = norm_local(
        middle, col_slice(second_gain), col_slice(second_shift)
    )
    second_all, act_all, hid_all, expand_bias_part = gather_hidden(
        second_normed.astype(BF16), expand_own, expand_oth, core_expand_bias, act_grad, 3
    )

    second_normed_grad = pair_scatter(hid_all, expand_own, expand_theirs, NT, 4)
    cot_wide = cotangent.astype(F32)
    middle_grad = cot_wide + norm_back(
        second_normed_grad, second_hat, second_rstd, col_slice(second_gain)
    )
    middle_all, attended_grad = gather_linear(
        middle_grad.astype(BF16), proj_own, proj_oth, NT, True, BF16, 5
    )
    triple_head_grad = attention_backward(
        triple, seg_col, seg_row, attended, attended_grad, lse
    )
    triple_all, first_normed_grad = triple_scatter(triple_head_grad, triple_t, width, 6)
    input_grad = middle_grad + norm_back(
        first_normed_grad, first_hat, first_rstd, col_slice(first_gain)
    )
    shrink_out = pair_scatter(act_all, shrink_own, shrink_theirs, NN, 7)
    block_out = (middle + shrink_out + col_slice(shrink_bias)).astype(BF16)

    def owned(grad, axis):
        return lax.psum_scatter(
            grad.astype(BF16), "dp", scatter_dimension=axis, tiled=True
        ).astype(F32)

    def flat(blocks):
        return blocks.reshape(-1, blocks.shape[-1])

    cot_flat, second_flat = flat(cot_all), flat(second_all)
    act_flat = act_all.reshape(2, -1, hidden)
    hid_flat = hid_all.reshape(2, -1, hidden)
    shrink_grad = jnp.einsum("ctf,td->cfd", act_flat, cot_flat, preferred_element_type=F32)
    shrink_owned = owned(shrink_grad.reshape(2 * hidden, col_width), 0)
    expand_grad = jnp.concatenate(
        [
            jnp.einsum("td,tf->df", second_flat, hid_flat[c], preferred_element_type=F32)
            for c in range(2)
        ],
        axis=1,
    )
    expand_owned = owned(expand_grad, 0)
    proj_grad = jnp.einsum("kt,td->kd", attended_all, flat(middle_all), preferred_element_type=F32)
    proj_owned = owned(proj_grad, 0)
    triple_grad = jnp.einsum(
        "td,kt->dk", flat(first_all), triple_all, preferred_element_type=F32
    )
    triple_owned = owned(triple_grad, 0)

    by_col = jnp.stack(
        [
            jnp.sum(first_normed_grad * first_hat, axis=0),
            jnp.sum(first_normed_grad, axis=0),
            jnp.sum(middle_grad, axis=0),
            jnp.sum(second_normed_grad * second_hat, axis=0),
            jnp.sum(second_normed_grad, axis=0),
            jnp.sum(cot_wide, axis=0),
        ]
    )
    is_col = (jnp.arange(2) == col).astype(F32)
    by_col = by_col[:, None, :] * is_col[None, :, None]
    is_core = (jnp.arange(2 * row_count) == 2 * row + col).astype(F32)
    by_core = expand_bias_part * is_core[:, None]
    triple_sum = jnp.sum(triple_all.astype(F32), axis=1)
    is_row = ((jnp.arange(row_count) == row) & (col == 0)).astype(F32)
    by_row = triple_sum[None, :] * is_row[:, None]
    vector = jnp.concatenate([by_col.reshape(-1), by_core.reshape(-1), by_row.reshape(-1)])
    devices = dp_count * row_count * col_count
    tile = 8 * 128
    size = -(-vector.shape[0] // (devices * tile)) * tile
    vector = jnp.pad(vector, (0, devices * size - vector.shape[0]))
    total = sum_all(
        vector.reshape(devices, size // 128, 128), (row_count, col_count), 8
    ).reshape(-1)
    col_totals = total[: 6 * width].reshape(6, width)
    expand_bias_grad = total[6 * width : 6 * width + 2 * row_count * hidden]
    rest = total[6 * width + 2 * row_count * hidden :]
    return (
        block_out,
        input_grad,
        col_totals[0],
        col_totals[1],
        triple_owned[None],
        rest[:width],
        rest[2 * width : 3 * width],
        proj_owned[None],
        col_totals[2],
        col_totals[3],
        col_totals[4],
        expand_owned[None],
        expand_bias_grad,
        shrink_owned[None],
        col_totals[5],
    )


def solution(mesh):
    assert mesh.shape["row"] == 4 and mesh.shape["col"] == 2
    sizes = tuple(mesh.shape[name] for name in AXES)
    tok, mat, mat_t = P(("dp", "row"), "col"), P("row", "col"), P("col", "row")
    in_specs = (
        tok, P("dp", None), P(), P(), mat_t, P(), P(), mat, P(), P(), P(), mat_t, P(), mat, P(), tok,
    )
    grad, grad_t = P("row", "dp", "col"), P("col", "dp", "row")
    out_specs = (
        tok, tok, P(), P(), grad_t, P(), P(), grad, P(), P(), P(), grad_t, P(), grad, P(),
    )
    return jax.shard_map(
        functools.partial(shards, axis_sizes=sizes),
        mesh=mesh, in_specs=in_specs, out_specs=out_specs, check_vma=False,
    )
```

```python
import functools

import jax
import jax.numpy as jnp
from jax import lax
from jax.experimental import pallas as pl
from jax.experimental.pallas import tpu as pltpu
from jax.sharding import PartitionSpec as P

HEADS = 25
HEAD_DIM = 64
EPS = 1e-05
NEG = -1e30
GRAIN = 16
AXES = ("dp", "row", "col")
MESH = pl.DeviceIdType.MESH
F32 = jnp.float32
BF16 = jnp.bfloat16
VMEM_BYTES = 60 * 1024 * 1024

NN = (((1,), (0,)), ((), ()))
NT = (((1,), (1,)), ((), ()))
TN = (((0,), (0,)), ((), ()))


def dot(left, right, dims):
    return lax.dot_general(left, right, dims, preferred_element_type=F32)


class Place:
    def __init__(self):
        self.d = lax.axis_index("dp")
        self.r = lax.axis_index("row")
        self.c = lax.axis_index("col")
        one = self.r + 1 - 2 * lax.rem(self.r, 2)
        two = lax.rem(self.r + 2, 4)
        self.a = 1 + self.c
        self.b = 2 - self.c
        self.ra = (1 - self.c) * one + self.c * two
        self.rb = self.c * one + (1 - self.c) * two
        self.r3 = 3 - self.r

    def dev(self, row, col=None):
        return (self.d, row, self.c if col is None else col)

    def mate(self):
        return (self.d, self.r, 1 - self.c)

    def barrier(self, devices):
        semaphore = pltpu.get_barrier_semaphore()
        for device in devices:
            pl.semaphore_signal(semaphore, inc=1, device_id=device, device_id_type=MESH)
        pl.semaphore_wait(semaphore, len(devices))

    def group(self):
        flat = 2 * self.r + self.c
        found = []
        for step in range(1, 8):
            other = lax.rem(flat + step, 8)
            found.append((self.d, other // 2, lax.rem(other, 2)))
        return found

    def square(self):
        return [self.mate(), self.dev(self.ra), self.dev(self.rb)]


def rcopy(src, dst, send, recv, device):
    return pltpu.make_async_remote_copy(
        src_ref=src, dst_ref=dst, send_sem=send, recv_sem=recv, device_id=device,
        device_id_type=MESH,
    )


def lanes(index, size):
    return pl.ds(pl.multiple_of(index * size, size), size)


def call(kernel, out_shapes, out_specs, in_specs, scratch, cid, flops=0, bytes_accessed=0):
    return pl.pallas_call(
        kernel,
        out_shape=out_shapes,
        in_specs=in_specs,
        out_specs=out_specs,
        scratch_shapes=scratch,
        compiler_params=pltpu.CompilerParams(
            collective_id=cid, has_side_effects=True, vmem_limit_bytes=VMEM_BYTES
        ),
    )


VM = pl.BlockSpec(memory_space=pltpu.VMEM)
ANY = pl.BlockSpec(memory_space=pl.ANY)
DMA = pltpu.SemaphoreType.DMA


def struct(shape, dtype):
    return jax.ShapeDtypeStruct(shape, dtype)


def chunks(size):
    count = next(n for n in (5, 4, 2, 1) if size % (n * GRAIN) == 0)
    return [pl.ds(k * (size // count), size // count) for k in range(count)]


def col_sums(matrix):
    ones = jnp.ones((8, matrix.shape[1]), matrix.dtype)
    exact = lax.Precision.HIGHEST if matrix.dtype == F32 else None
    return lax.dot_general(ones, matrix, NT, precision=exact, preferred_element_type=F32)[0:1]


class Totals:
    scratch = [pltpu.VMEM((2, 8, 256), F32), DMA((2,))]

    def __init__(self, place, buf, sems):
        self.place, self.buf, self.sems = place, buf, sems

    def __call__(self, first, second):
        self.buf[0, 0:1] = jnp.sum(first, axis=0, keepdims=True)
        self.buf[0, 1:2] = jnp.sum(second, axis=0, keepdims=True)
        copy = rcopy(
            self.buf.at[0], self.buf.at[1], self.sems.at[0], self.sems.at[1], self.place.mate()
        )
        copy.start()
        copy.wait()
        return (
            self.buf[0, 0:1] + self.buf[1, 0:1],
            self.buf[0, 1:2] + self.buf[1, 1:2],
        )


def moments(totals, matrix, width):
    total, square = totals(matrix, matrix * matrix)
    average = total / width
    return average, lax.rsqrt(square / width - average * average + EPS)


def keep_moments(ref, average, rstd):
    ref[0:1] = average
    ref[1:2] = rstd


def norm_back(totals, grad_in, hat, rstd, gain, width):
    scaled = grad_in * gain
    total, mixed = totals(scaled, scaled * hat)
    return rstd * (scaled - total / width - hat * mixed / width)


def gather_scratch(rows, cols, feats, turned):
    count = len(chunks(rows))
    return [
        pltpu.VMEM((2, 4, rows, cols), BF16), DMA((7, count)), DMA((2, 4, count)), DMA((4,)),
        pltpu.VMEM((rows, turned), BF16), pltpu.VMEM((turned, rows), BF16),
        pltpu.VMEM((feats, rows), BF16), DMA((3,)),
    ]


class Gather:
    def __init__(self, place, all_ref, w_ref, w_step, refs):
        self.place, self.all_ref = place, all_ref
        self.got, self.send, self.recv, self.out_sem = refs[:4]
        self.w_flat, self.turned, self.w_oth, w_sem = refs[4:]
        self.w_load = pltpu.make_async_copy(w_ref, self.w_flat, w_sem.at[2])
        self.w_load.start()
        feats = self.w_oth.shape[0]
        start = w_step[0] + w_step[1] * place.c
        other = w_step[0] + w_step[1] * (1 - place.c)
        self.w_own = self.turned.at[pl.ds(pl.multiple_of(start, GRAIN), feats)]
        theirs = self.turned.at[pl.ds(pl.multiple_of(other, GRAIN), feats)]
        self.w_copy = rcopy(theirs, self.w_oth, w_sem.at[0], w_sem.at[1], place.mate())

    def product(self, slot):
        return dot(self.w_own[...], self.got[0, slot], NN) + dot(
            self.w_oth[...], self.got[1, slot], NN
        )

    def run(self, work, idle=None):
        place, got, send, recv = self.place, self.got, self.send, self.recv
        mate, size = place.mate(), got.shape[3]
        parts = list(enumerate(chunks(got.shape[2])))
        dev_a, dev_b = place.dev(place.ra), place.dev(place.rb)

        def move(number, source, target, device):
            return [
                rcopy(
                    got.at[source[0], source[1], part], got.at[target[0], target[1], part],
                    send.at[number, k], recv.at[target[0], target[1], k], device,
                )
                for k, part in parts
            ]

        def keep(slot, row, number):
            copy = pltpu.make_async_copy(
                got.at[0, slot], self.all_ref.at[:, lanes(row, size)], self.out_sem.at[number]
            )
            copy.start()
            return copy

        to_a = move(0, (0, 0), (0, place.a), dev_a)
        to_b = move(1, (0, 0), (0, place.b), dev_b)
        to_mate = move(2, (0, 0), (1, 0), mate)
        relay = move(3, (0, place.a), (0, 3), dev_b)
        fwd_a = move(4, (0, place.a), (1, place.a), mate)
        fwd_b = move(5, (0, place.b), (1, place.b), mate)
        fwd_3 = move(6, (0, 3), (1, 3), mate)
        for copies in (to_a, to_b, to_mate):
            for copy in copies:
                copy.start()
        kept = [keep(0, place.r, 0)]
        self.w_load.wait()
        self.turned[...] = self.w_flat[...].T
        self.w_copy.start()
        if idle is not None:
            idle()
        self.w_copy.wait()
        for copy in to_mate:
            copy.wait_recv()
        work(0, place.r)
        for k, copy in enumerate(to_a):
            copy.wait_recv()
            relay[k].start()
            fwd_a[k].start()
        kept.append(keep(place.a, place.ra, 1))
        for k, copy in enumerate(to_b):
            copy.wait_recv()
            fwd_b[k].start()
        kept.append(keep(place.b, place.rb, 2))
        for copy in fwd_b:
            copy.wait_recv()
        work(place.b, place.rb)
        for copy in fwd_a:
            copy.wait_recv()
        work(place.a, place.ra)
        for k, copy in enumerate(relay):
            copy.wait_recv()
            fwd_3[k].start()
        kept.append(keep(3, place.r3, 3))
        for copy in fwd_3:
            copy.wait_recv()
        work(3, place.r3)
        for copies in (to_mate, to_a, to_b, relay, fwd_a, fwd_b, fwd_3):
            for copy in copies:
                copy.wait_send()
        for copy in kept:
            copy.wait()


def gather_triple(tokens, cols, bias, weight, width, feats, cid):
    rows, size = tokens.shape
    triple_width = weight.shape[1]
    grains = feats // GRAIN
    shift = triple_width - feats
    per = 3 * HEAD_DIM

    def kernel(x_ref, c_ref, b_ref, w_ref, all_ref, h_ref, st_ref, tt, tb, ts, gs, gr, *refs):
        place = Place()
        place.barrier(place.group())
        me = 2 * place.r + place.c
        gather = Gather(place, all_ref, w_ref, (0, shift), refs)
        wide = x_ref[...].astype(F32)
        average, rstd = moments(Totals(place, tb, ts), wide, width)
        keep_moments(st_ref, average, rstd)
        gather.got[0, 0] = ((wide - average) * rstd * c_ref[:, 0:1] + c_ref[:, 1:2]).astype(BF16)

        def target(j):
            feature = triple_width * place.r + shift * place.c + GRAIN * j
            part = feature // width
            inner = feature - part * width
            head = inner // HEAD_DIM
            owner = jnp.minimum(head // 3, 7)
            row = (head - 3 * owner) * per + part * HEAD_DIM + (inner - head * HEAD_DIM)
            return owner, pl.ds(pl.multiple_of(row, GRAIN), GRAIN)

        def work(slot, row):
            tt[:, lanes(row, size)] = (gather.product(slot) + b_ref[...]).astype(BF16)

            def send_grain(j, carry):
                owner, place_rows = target(j)
                src = tt.at[pl.ds(pl.multiple_of(GRAIN * j, GRAIN), GRAIN), lanes(row, size)]
                dst = h_ref.at[place_rows, lanes(row, size)]

                @pl.when(owner == me)
                def _():
                    pltpu.make_async_copy(src, dst, gr).start()

                @pl.when(owner != me)
                def _():
                    rcopy(src, dst, gs, gr, (place.d, owner // 2, lax.rem(owner, 2))).start()

                return carry

            lax.fori_loop(place.c, grains, send_grain, 0)

        gather.run(work)

        def drain(j, carry):
            @pl.when(target(j)[0] != me)
            def _():
                src = tt.at[pl.ds(0, GRAIN)]
                pltpu.make_async_copy(src, src, gs).wait()

            return carry

        lax.fori_loop(place.c, grains, drain, 0)

        @pl.when(me == 7)
        def _():
            pltpu.make_async_copy(h_ref, h_ref, gr).wait()

        @pl.when(me != 7)
        def _():
            part = h_ref.at[pl.ds(0, 3 * per)]
            pltpu.make_async_copy(part, part, gr).wait()

    return call(
        kernel,
        (struct((rows, 4 * size), BF16), struct((4 * per, 4 * size), BF16), struct((8, size), F32)),
        (ANY, ANY, VM), [VM] * 3 + [ANY],
        [pltpu.VMEM((feats, 4 * size), BF16)] + Totals.scratch + [DMA, DMA]
        + gather_scratch(rows, size, feats, triple_width), cid,
    )(tokens, cols, bias, weight)


def gather_cotangent(cot, weight, cid):
    rows, size = cot.shape
    feats = weight.shape[1] // 2

    def kernel(x_ref, w_ref, all_ref, y_ref, y, y_sem, *refs):
        place = Place()
        place.barrier(place.square())
        gather = Gather(place, all_ref, w_ref, (0, feats), refs)
        gather.got[0, 0] = x_ref[...]
        pending = []

        def work(slot, row):
            number = len(pending)
            y[number] = gather.product(slot)
            copy = pltpu.make_async_copy(
                y.at[number], y_ref.at[:, lanes(row, size)], y_sem.at[number]
            )
            copy.start()
            pending.append(copy)

        gather.run(work)
        for copy in pending:
            copy.wait()

    return call(
        kernel, (struct((rows, 4 * size), BF16), struct((feats, 4 * size), F32)),
        (ANY, ANY), [VM, ANY],
        [pltpu.VMEM((4, feats, size), F32), DMA((4,))]
        + gather_scratch(rows, size, feats, 2 * feats), cid,
    )(cot, weight)


def gather_hidden(tokens, proj_out, cols, bias, act_grad, weight, width, cid):
    rows, size = tokens.shape
    feats = weight.shape[1] // 2

    def kernel(
        t_ref, p_ref, c_ref, b_ref, g_ref, w_ref,
        all_ref, act_ref, hid_ref, mid_ref, st_ref, sum_ref,
        act, hid, swap_send, swap_recv, swap_out, grads, g_sem, grad_sum, tb, ts, *refs,
    ):
        place = Place()
        place.barrier(place.square())
        mate = place.mate()
        g_load = pltpu.make_async_copy(g_ref, grads, g_sem)
        g_load.start()
        gather = Gather(place, all_ref, w_ref, (0, feats), refs)
        middle = t_ref[...].astype(F32) + p_ref[...] + c_ref[:, 2:3]
        mid_ref[...] = middle
        average, rstd = moments(Totals(place, tb, ts), middle, width)
        keep_moments(st_ref, average, rstd)
        gather.got[0, 0] = ((middle - average) * rstd * c_ref[:, 3:4] + c_ref[:, 4:5]).astype(BF16)
        pending = []
        mine = pl.ds(pl.multiple_of(place.c * feats, GRAIN), feats)

        def work(slot, row):
            number = len(pending)
            if number == 0:
                g_load.wait()
            p = gather.product(slot) + b_ref[...]
            square = p * p
            t = jnp.tanh(0.7978845608028654 * (p + 0.044715 * (square * p)))
            act[number] = (0.5 * p * (1.0 + t)).astype(BF16)
            slope = 0.5 * (1.0 + t) + 0.5 * p * (1.0 - t * t) * (
                0.7978845608028654 * (1.0 + 3.0 * 0.044715 * square)
            )
            grad = grads[:, lanes(row, size)] * slope
            hid[number] = grad.astype(BF16)
            copies = []
            for k, (buf, out) in enumerate(((act, act_ref), (hid, hid_ref))):
                there = out.at[mine, lanes(row, size)]
                out_copy = pltpu.make_async_copy(buf.at[number], there, swap_out.at[k, number])
                swap = rcopy(
                    buf.at[number], there, swap_send.at[k, number], swap_recv.at[k, number], mate
                )
                out_copy.start()
                swap.start()
                copies += [out_copy, swap]
            grad_sum[...] = grad if number == 0 else grad_sum[...] + grad
            pending.append(copies)

        gather.run(work)
        sum_ref[0:1] = col_sums(grad_sum[...])
        for copies in pending:
            for copy in copies:
                copy.wait()

    full = struct((2 * feats, 4 * size), BF16)
    return call(
        kernel,
        (
            struct((rows, 4 * size), BF16), full, full, struct((rows, size), F32),
            struct((8, size), F32), struct((8, feats), F32),
        ),
        (ANY, ANY, ANY, VM, VM, VM), [VM] * 4 + [ANY, ANY],
        [pltpu.VMEM((4, feats, size), BF16)] * 2 + [DMA((2, 4))] * 3
        + [pltpu.VMEM((feats, 4 * size), F32), DMA, pltpu.VMEM((feats, size), F32)]
        + Totals.scratch + gather_scratch(rows, size, feats, 2 * feats), cid,
    )(tokens, proj_out, cols, bias, act_grad, weight)


def gather_middle(grad_in, middle, stats, cot, cols, weight, start, step, width, cid):
    rows, size = cot.shape
    feats = 4 * HEAD_DIM

    def kernel(
        s_ref, m_ref, st_ref, x_ref, c_ref, w_ref, all_ref, y_ref, mg_ref, sum_ref, tb, ts, *refs
    ):
        place = Place()
        place.barrier(place.square())
        gather = Gather(place, all_ref, w_ref, (start[0] + start[1] * place.r, step), refs)
        rstd = st_ref[1:2]
        hat = (m_ref[...] - st_ref[0:1]) * rstd
        back = norm_back(Totals(place, tb, ts), s_ref[...], hat, rstd, c_ref[:, 3:4], width)
        mg_ref[...] = x_ref[...].astype(F32) + back
        gather.got[0, 0] = mg_ref[...].astype(BF16)

        def idle():
            hat = (m_ref[...] - st_ref[0:1]) * st_ref[1:2]
            sum_ref[0:1] = col_sums(s_ref[...] * hat)
            sum_ref[1:2] = col_sums(s_ref[...])
            sum_ref[2:3] = col_sums(mg_ref[...])
            sum_ref[3:4] = col_sums(x_ref[...])

        def work(slot, row):
            y_ref[:, lanes(row, size)] = gather.product(slot).astype(BF16)

        gather.run(work, idle)

    return call(
        kernel,
        (
            struct((rows, 4 * size), BF16), struct((feats, 4 * size), BF16),
            struct((rows, size), F32), struct((8, rows), F32),
        ),
        (ANY, VM, VM, VM), [VM] * 5 + [ANY],
        Totals.scratch + gather_scratch(rows, size, feats, weight.shape[1]), cid,
    )(grad_in, middle, stats, cot, cols, weight)


def scatter_scratch(rows, cols):
    count = len(chunks(rows))
    return [
        pltpu.VMEM((3, rows, cols), BF16), pltpu.VMEM((3, rows, cols), BF16),
        DMA((3, count)), DMA((3, count)), pltpu.VMEM((rows, cols), F32),
    ]


def run_scatter(place, block, refs):
    outbox, inbox, send, recv, passed = refs
    parts = list(enumerate(chunks(outbox.shape[1])))

    def move(number, device):
        return [
            rcopy(
                outbox.at[number, part], inbox.at[number, part],
                send.at[number, k], recv.at[number, k], device,
            )
            for k, part in parts
        ]

    first = move(0, place.dev(place.ra))
    second = move(1, place.dev(place.ra))
    third = move(2, place.dev(place.rb))
    outbox[0] = block(place.r3).astype(BF16)
    for copy in first:
        copy.start()
    passed[...] = block(place.rb)
    outbox[1] = block(place.ra).astype(BF16)
    for copy in second:
        copy.start()
    for k, part in parts:
        first[k].wait_recv()
        outbox[2, part] = (passed[part] + inbox[0, part].astype(F32)).astype(BF16)
        third[k].start()
    passed[...] = block(place.r)
    for copy in second:
        copy.wait_recv()
    passed[...] += inbox[1].astype(F32)
    for copy in third:
        copy.wait_recv()
    total = passed[...] + inbox[2].astype(F32)
    for copies in (first, second, third):
        for copy in copies:
            copy.wait_send()
    return total


def load_scratch(weight, left):
    return [pltpu.VMEM(weight.shape, BF16), pltpu.VMEM(left.shape, BF16), DMA((5,))]


def loaded_block(place, l_ref, w_ref, weight, left, sems, size):
    w_load = pltpu.make_async_copy(w_ref, weight, sems.at[4])
    w_load.start()
    loads = []
    for k, row in enumerate((place.r3, place.rb, place.ra, place.r)):
        span = lanes(row, size)
        loads.append(pltpu.make_async_copy(l_ref.at[:, span], left.at[:, span], sems.at[k]))
        loads[-1].start()

    def block(row):
        if len(loads) == 4:
            w_load.wait()
        loads.pop(0).wait()
        return dot(weight[...], left[:, lanes(row, size)], NN)

    return block


def hidden_scatter(left, weight, cid):
    rows, size = weight.shape[0], left.shape[1] // 4

    def kernel(l_ref, w_ref, out_ref, w, l, l_sem, *refs):
        place = Place()
        block = loaded_block(place, l_ref, w_ref, w, l, l_sem, size)
        place.barrier([place.dev(place.ra), place.dev(place.rb)])
        out_ref[...] = run_scatter(place, block, refs)

    return call(
        kernel, struct((rows, size), F32), VM, [ANY] * 2,
        load_scratch(weight, left) + scatter_scratch(rows, size), cid,
    )(left, weight)


def output_scatter(left, weight, middle, cols, cid):
    rows, size = middle.shape

    def kernel(l_ref, w_ref, m_ref, c_ref, out_ref, w, l, l_sem, *refs):
        place = Place()
        block = loaded_block(place, l_ref, w_ref, w, l, l_sem, size)
        place.barrier([place.dev(place.ra), place.dev(place.rb)])
        total = run_scatter(place, block, refs)
        out_ref[...] = (m_ref[...] + total + c_ref[:, 5:6]).astype(BF16)

    return call(
        kernel, struct((rows, size), BF16), VM, [ANY, ANY, VM, VM],
        load_scratch(weight, left) + scatter_scratch(rows, size), cid,
    )(left, weight, middle, cols)


def attended_scatter(heads, weight, cid):
    feats, rows = weight.shape
    tokens = heads.shape[1]
    size = tokens // 4

    def kernel(h_ref, w_ref, all_ref, out_ref, full, gs, gr, kept_sem, *refs):
        place = Place()
        place.barrier(place.group())
        me = 2 * place.r + place.c
        count = jnp.where(me == 7, 4, 3) * (HEAD_DIM // GRAIN)

        def send_grain(j, carry):
            feature = 3 * HEAD_DIM * me + GRAIN * j
            owner = feature // feats
            src = h_ref.at[pl.ds(pl.multiple_of(GRAIN * j, GRAIN), GRAIN)]
            dst = full.at[pl.ds(pl.multiple_of(feature - owner * feats, GRAIN), GRAIN)]
            rcopy(src, dst, gs, gr, (place.d, owner, 1 - place.c)).start()

            @pl.when(owner == place.r)
            def _():
                pltpu.make_async_copy(src, dst, gr).start()

            @pl.when(owner != place.r)
            def _():
                rcopy(src, dst, gs, gr, (place.d, owner, place.c)).start()

            return carry

        lax.fori_loop(0, count, send_grain, 0)

        def drain(j, carry):
            feature = 3 * HEAD_DIM * me + GRAIN * j
            src = h_ref.at[pl.ds(0, GRAIN)]
            pltpu.make_async_copy(src, src, gs).wait()

            @pl.when(feature // feats != place.r)
            def _():
                pltpu.make_async_copy(src, src, gs).wait()

            return carry

        lax.fori_loop(0, count, drain, 0)
        pltpu.make_async_copy(full, full, gr).wait()
        kept = pltpu.make_async_copy(full, all_ref, kept_sem)
        kept.start()
        out_ref[...] = run_scatter(
            place, lambda row: dot(w_ref[...], full[:, lanes(row, size)], TN), refs
        )
        kept.wait()

    return call(
        kernel, (struct((feats, tokens), BF16), struct((rows, size), F32)),
        (ANY, VM), [ANY, VM],
        [pltpu.VMEM((feats, tokens), BF16), DMA, DMA, DMA] + scatter_scratch(rows, size), cid,
    )(heads, weight)


def triple_scatter(heads, weight, tokens, stats, middle_grad, cols, width, cid):
    rows, feats = weight.shape
    count_tokens = heads.shape[1]
    size = count_tokens // 4
    per = 3 * HEAD_DIM
    low = (feats // GRAIN + 1) // 2 * GRAIN

    def kernel(
        h_ref, w_ref, t_ref, st_ref, mg_ref, c_ref, all_ref, out_ref, sum_ref, bias_ref,
        full, w, w_sem, tb, ts, gs, gr, ms, mr, kept_sem, *refs,
    ):
        place = Place()
        w_load = pltpu.make_async_copy(w_ref, w, w_sem)
        w_load.start()
        place.barrier(place.group())
        me = 2 * place.r + place.c
        count = jnp.where(me == 7, 4, 3) * (per // GRAIN)

        def target(j):
            row = GRAIN * j
            head = row // per
            rest = row - head * per
            part = rest // HEAD_DIM
            feature = part * width + (3 * me + head) * HEAD_DIM + rest - part * HEAD_DIM
            owner = feature // feats
            inner = feature - owner * feats
            return 2 * owner + inner // low, inner

        def send_grain(j, carry):
            owner, inner = target(j)
            src = h_ref.at[pl.ds(pl.multiple_of(GRAIN * j, GRAIN), GRAIN)]
            dst = full.at[pl.ds(pl.multiple_of(inner, GRAIN), GRAIN)]

            @pl.when(owner == me)
            def _():
                pltpu.make_async_copy(src, dst, gr).start()

            @pl.when(owner != me)
            def _():
                rcopy(src, dst, gs, gr, (place.d, owner // 2, lax.rem(owner, 2))).start()

            return carry

        lax.fori_loop(0, count, send_grain, 0)

        def drain(j, carry):
            @pl.when(target(j)[0] != me)
            def _():
                src = h_ref.at[pl.ds(0, GRAIN)]
                pltpu.make_async_copy(src, src, gs).wait()

            return carry

        lax.fori_loop(0, count, drain, 0)
        lower, upper = full.at[pl.ds(0, low)], full.at[pl.ds(low, feats - low)]

        def swap(mine, theirs):
            pltpu.make_async_copy(mine, mine, gr).wait()
            copy = rcopy(mine, mine, ms, mr, place.mate())
            copy.start()
            copy.wait_send()
            pltpu.make_async_copy(theirs, theirs, mr).wait()

        @pl.when(place.c == 0)
        def _():
            swap(lower, upper)

        @pl.when(place.c == 1)
        def _():
            swap(upper, lower)

        kept = pltpu.make_async_copy(full, all_ref, kept_sem)
        kept.start()
        w_load.wait()
        grad = run_scatter(place, lambda row: dot(w[...], full[:, lanes(row, size)], NN), refs)
        rstd = st_ref[1:2]
        hat = (t_ref[...].astype(F32) - st_ref[0:1]) * rstd
        back = norm_back(Totals(place, tb, ts), grad, hat, rstd, c_ref[:, 0:1], width)
        out_ref[...] = mg_ref[...] + back
        sum_ref[0:1] = col_sums(grad * hat)
        sum_ref[1:2] = col_sums(grad)
        bias_ref[0:1] = col_sums(full[...])
        kept.wait()

    return call(
        kernel,
        (
            struct((feats, count_tokens), BF16), struct((rows, size), F32),
            struct((8, rows), F32), struct((8, feats), F32),
        ),
        (ANY, VM, VM, VM), [ANY, ANY] + [VM] * 4,
        [pltpu.VMEM((feats, count_tokens), BF16), pltpu.VMEM(weight.shape, BF16), DMA]
        + Totals.scratch + [DMA] * 5
        + scatter_scratch(rows, size), cid,
    )(heads, weight, tokens, stats, middle_grad, cols)


def attention_bias(seg_col, seg_row, bias_ref):
    tokens = seg_row.shape[1]
    key = lax.broadcasted_iota(jnp.int32, (tokens, tokens), 0)
    query = lax.broadcasted_iota(jnp.int32, (tokens, tokens), 1)
    allowed = (seg_col[...] == seg_row[...]) & (key <= query)
    bias_ref[...] = jnp.where(allowed, 0.0, NEG)


def holds(head):
    return (head < 3) | ((lax.axis_index("row") == 3) & (lax.axis_index("col") == 1))


def attention_forward(triple, seg_col, seg_row):
    per = 3 * HEAD_DIM
    tokens = triple.shape[1]
    span = tokens // 4

    def kernel(sc_ref, sr_ref, t_ref, o_ref, l_ref, bias_ref):
        @pl.when(pl.program_id(0) == 0)
        def _():
            attention_bias(sc_ref, sr_ref, bias_ref)

        @pl.when(holds(pl.program_id(0)))
        def _():
            for j in range(4):
                reach, here = (j + 1) * span, slice(j * span, (j + 1) * span)
                query = t_ref[0:HEAD_DIM, here] * BF16(HEAD_DIM ** (-0.5))
                score = dot(t_ref[HEAD_DIM : 2 * HEAD_DIM, 0:reach], query, TN)
                score = score + bias_ref[0:reach, here]
                top = jnp.max(score, axis=0, keepdims=True)
                weight = jnp.exp(score - top)
                total = jnp.sum(weight, axis=0, keepdims=True)
                mixed = dot(t_ref[2 * HEAD_DIM : per, 0:reach], weight.astype(BF16), NN)
                o_ref[:, here] = (mixed / total).astype(BF16)
                l_ref[0, :, here] = top + jnp.log(total)

    return pl.pallas_call(
        kernel,
        grid=(4,),
        out_shape=(
            jax.ShapeDtypeStruct((4 * HEAD_DIM, tokens), BF16),
            jax.ShapeDtypeStruct((4, 1, tokens), F32),
        ),
        in_specs=[
            pl.BlockSpec((tokens, 1), lambda h: (0, 0)),
            pl.BlockSpec((1, tokens), lambda h: (0, 0)),
            pl.BlockSpec((per, tokens), lambda h: (h, 0)),
        ],
        out_specs=(
            pl.BlockSpec((HEAD_DIM, tokens), lambda h: (h, 0)),
            pl.BlockSpec((1, 1, tokens), lambda h: (h, 0, 0)),
        ),
        scratch_shapes=[pltpu.VMEM((tokens, tokens), F32)],
        compiler_params=pltpu.CompilerParams(vmem_limit_bytes=VMEM_BYTES),
    )(seg_col, seg_row, triple)


def attention_backward(triple, seg_col, seg_row, attended, attended_grad, lse):
    per = 3 * HEAD_DIM
    tokens = triple.shape[1]
    span = tokens // 4

    def kernel(sc_ref, sr_ref, t_ref, o_ref, g_ref, l_ref, d_ref, bias_ref, kg_ref, vg_ref):
        @pl.when(pl.program_id(0) == 0)
        def _():
            attention_bias(sc_ref, sr_ref, bias_ref)

        @pl.when(holds(pl.program_id(0)))
        def _():
            kg_ref[...] = jnp.zeros_like(kg_ref)
            vg_ref[...] = jnp.zeros_like(vg_ref)
            for j in range(4):
                reach, here = (j + 1) * span, slice(j * span, (j + 1) * span)
                query = t_ref[0:HEAD_DIM, here] * BF16(HEAD_DIM ** (-0.5))
                key = t_ref[HEAD_DIM : 2 * HEAD_DIM, 0:reach]
                grad = g_ref[:, here]
                delta = jnp.sum(
                    grad.astype(F32) * o_ref[:, here].astype(F32), axis=0, keepdims=True
                )
                score = dot(key, query, TN) + bias_ref[0:reach, here]
                prob = jnp.exp(score - l_ref[0, :, here])
                vg_ref[:, 0:reach] += dot(grad, prob.astype(BF16), NT)
                back = dot(t_ref[2 * HEAD_DIM : per, 0:reach], grad, TN)
                mix = (prob * (back - delta)).astype(BF16)
                d_ref[0:HEAD_DIM, here] = (dot(key, mix, NN) * HEAD_DIM ** (-0.5)).astype(BF16)
                kg_ref[:, 0:reach] += dot(query, mix, NT)
            d_ref[HEAD_DIM : 2 * HEAD_DIM, :] = kg_ref[...].astype(BF16)
            d_ref[2 * HEAD_DIM : per, :] = vg_ref[...].astype(BF16)

    return pl.pallas_call(
        kernel,
        grid=(4,),
        out_shape=jax.ShapeDtypeStruct((4 * per, tokens), BF16),
        in_specs=[
            pl.BlockSpec((tokens, 1), lambda h: (0, 0)),
            pl.BlockSpec((1, tokens), lambda h: (0, 0)),
            pl.BlockSpec((per, tokens), lambda h: (h, 0)),
            pl.BlockSpec((HEAD_DIM, tokens), lambda h: (h, 0)),
            pl.BlockSpec((HEAD_DIM, tokens), lambda h: (h, 0)),
            pl.BlockSpec((1, 1, tokens), lambda h: (h, 0, 0)),
        ],
        out_specs=pl.BlockSpec((per, tokens), lambda h: (h, 0)),
        scratch_shapes=[
            pltpu.VMEM((tokens, tokens), F32),
            pltpu.VMEM((HEAD_DIM, tokens), F32),
            pltpu.VMEM((HEAD_DIM, tokens), F32),
        ],
        compiler_params=pltpu.CompilerParams(vmem_limit_bytes=VMEM_BYTES),
    )(seg_col, seg_row, triple, attended, attended_grad, lse)


def sum_all(pieces, sizes, cid):
    count = pieces.shape[0]
    rows, cols = sizes

    def kernel(x_ref, out_ref, inbox, piece, sems):
        me = (lax.axis_index("dp") * rows + lax.axis_index("row")) * cols + lax.axis_index("col")

        def dev(step):
            flat = lax.rem(me + step, count)
            return flat, (flat // (rows * cols), lax.rem(flat // cols, rows), lax.rem(flat, cols))

        semaphore = pltpu.get_barrier_semaphore()

        def greet(step, carry):
            pl.semaphore_signal(semaphore, inc=1, device_id=dev(step)[1], device_id_type=MESH)
            return carry

        lax.fori_loop(1, count, greet, 0)
        pl.semaphore_wait(semaphore, count - 1)

        def spread(step, carry):
            flat, device = dev(step)
            rcopy(x_ref.at[flat], inbox.at[me], sems.at[0], sems.at[1], device).start()
            return carry

        lax.fori_loop(1, count, spread, 0)
        inbox[me] = x_ref[me]
        rest = inbox.at[pl.ds(0, count - 1)]
        pltpu.make_async_copy(rest, rest, sems.at[1]).wait()
        pltpu.make_async_copy(rest, rest, sems.at[0]).wait()
        piece[...] = jnp.sum(inbox[...], axis=0)

        def share(step, carry):
            rcopy(piece, out_ref.at[me], sems.at[2], sems.at[3], dev(step)[1]).start()
            return carry

        lax.fori_loop(1, count, share, 0)
        out_ref[me] = piece[...]
        rest = out_ref.at[pl.ds(0, count - 1)]
        pltpu.make_async_copy(rest, rest, sems.at[3]).wait()
        pltpu.make_async_copy(rest, rest, sems.at[2]).wait()

    return call(
        kernel, jax.ShapeDtypeStruct(pieces.shape, F32), VM, [VM],
        [pltpu.VMEM(pieces.shape, F32), pltpu.VMEM(pieces.shape[1:], F32), DMA((4,))], cid,
    )(pieces)


def shards(
    tokens, segment_ids, first_gain, first_shift, triple_weight, query_bias, value_bias,
    proj_weight, proj_bias, second_gain, second_shift, expand_weight, expand_bias,
    shrink_weight, shrink_bias, cotangent, *, axis_sizes,
):
    width = HEADS * HEAD_DIM
    dp_count, row_count, col_count = axis_sizes
    row, col = lax.axis_index("row"), lax.axis_index("col")
    col_width = tokens.shape[1]
    triple_width = triple_weight.shape[1]
    proj_rows = proj_weight.shape[0]
    hidden = expand_weight.shape[1] // 2
    core_feats = (triple_width // GRAIN + 1) // 2 * GRAIN

    stacked = jnp.concatenate(
        [first_gain, first_shift, proj_bias, second_gain, second_shift, shrink_bias]
    ).reshape(6, width)
    cols = lax.dynamic_slice_in_dim(stacked, col * col_width, col_width, 1).T
    full_bias = jnp.concatenate([query_bias, jnp.zeros((width,), F32), value_bias])
    core_bias = lax.dynamic_slice_in_dim(
        full_bias, row * triple_width + col * (triple_width - core_feats), core_feats
    )[:, None]
    core_expand_bias = lax.dynamic_slice_in_dim(
        expand_bias, (row * 2 + col) * hidden, hidden
    )[:, None]
    tokens_t, cot_t = tokens.T, cotangent.T
    seg_row = segment_ids
    seg_col = segment_ids.reshape(-1, 1)

    first_all, triple, first_stats = gather_triple(
        tokens_t, cols, core_bias, triple_weight, width, core_feats, 0
    )
    cot_all, act_grad = gather_cotangent(cot_t, shrink_weight.T, 1)
    attended, lse = attention_forward(triple, seg_col, seg_row)
    attended_all, proj_out = attended_scatter(attended, proj_weight, 2)
    second_all, act_all, hid_all, middle, second_stats, expand_bias_part = gather_hidden(
        tokens_t, proj_out, cols, core_expand_bias, act_grad, expand_weight, width, 3
    )

    def product(left, right):
        return lax.dot_general(left, right, NT, preferred_element_type=F32).astype(BF16)

    def owned(grad):
        parts = grad.reshape(dp_count, -1, grad.shape[1])
        summed = lax.psum_scatter(parts, "dp", scatter_dimension=0, tiled=True)
        return summed.reshape(1, -1, grad.shape[1])

    shrink_grad = product(act_all, cot_all)
    hid_all, shrink_grad = lax.optimization_barrier((hid_all, shrink_grad))
    shrink_owned = owned(shrink_grad)

    second_normed_grad = hidden_scatter(hid_all, expand_weight, 4)
    head_rows = 3 * HEAD_DIM
    lag = (row_count - 1) * (proj_rows - 2 * head_rows)
    before = lax.ppermute(
        proj_weight[proj_rows - lag :], "row", [(i, i + 1) for i in range(row_count - 1)]
    )
    padded = jnp.concatenate(
        [before, proj_weight, jnp.zeros((2 * HEAD_DIM, col_width), BF16)], axis=0
    )
    middle_all, attended_grad, middle_grad, second_sums = gather_middle(
        second_normed_grad, middle, second_stats, cot_t, cols, padded.T,
        (lag, 2 * head_rows - proj_rows), head_rows, width, 5,
    )
    proj_grad = product(attended_all, middle_all)
    pieces = [
        product(second_all, hid_all[:hidden]),
        product(second_all, hid_all[hidden:]),
        proj_grad,
    ]
    both_grad = jnp.concatenate(
        [piece.reshape(dp_count, -1, piece.shape[1]) for piece in pieces], axis=1
    )
    attended_grad, shrink_owned, both_grad = lax.optimization_barrier(
        (attended_grad, shrink_owned, both_grad)
    )
    both_owned = owned(both_grad.reshape(-1, col_width))
    triple_head_grad = attention_backward(
        triple, seg_col, seg_row, attended, attended_grad, lse
    )
    triple_all, input_grad, first_sums, bias_sums = triple_scatter(
        triple_head_grad, triple_weight, tokens_t, first_stats, middle_grad, cols, width, 6
    )
    triple_grad = product(first_all, triple_all)
    act_all, triple_grad, both_owned, first_sums = lax.optimization_barrier(
        (act_all, triple_grad, both_owned, first_sums)
    )
    part = col_width // dp_count
    expand_owned = jnp.concatenate([both_owned[:, :part], both_owned[:, part : 2 * part]], axis=2)
    proj_owned = both_owned[:, 2 * part :]
    triple_owned = owned(triple_grad)
    block_out = output_scatter(act_all, shrink_weight.T, middle, cols, 7)

    by_col = jnp.concatenate([first_sums[:2], second_sums[:4]])
    is_col = (jnp.arange(2) == col).astype(F32)
    by_col = by_col[:, None, :] * is_col[None, :, None]
    is_core = (jnp.arange(2 * row_count) == 2 * row + col).astype(F32)
    by_core = expand_bias_part[0] * is_core[:, None]
    is_row = ((jnp.arange(row_count) == row) & (col == 0)).astype(F32)
    by_row = bias_sums[0][None, :] * is_row[:, None]
    vector = jnp.concatenate([by_col.reshape(-1), by_core.reshape(-1), by_row.reshape(-1)])
    devices = dp_count * row_count * col_count
    tile = 8 * 128
    size = -(-vector.shape[0] // (devices * tile)) * tile
    vector = jnp.pad(vector, (0, devices * size - vector.shape[0]))
    total = sum_all(
        vector.reshape(devices, size // 128, 128), (row_count, col_count), 8
    ).reshape(-1)
    col_totals = total[: 6 * width].reshape(6, width)
    expand_bias_grad = total[6 * width : 6 * width + 2 * row_count * hidden]
    rest = total[6 * width + 2 * row_count * hidden :]
    return (
        block_out.T,
        input_grad.T,
        col_totals[0],
        col_totals[1],
        triple_owned.astype(F32),
        rest[:width],
        rest[2 * width : 3 * width],
        proj_owned.astype(F32),
        col_totals[4],
        col_totals[2],
        col_totals[3],
        expand_owned.astype(F32),
        expand_bias_grad,
        shrink_owned.astype(F32),
        col_totals[5],
    )


def solution(mesh):
    assert mesh.shape["row"] == 4 and mesh.shape["col"] == 2
    sizes = tuple(mesh.shape[name] for name in AXES)
    tok, mat, mat_t = P(("dp", "row"), "col"), P("row", "col"), P("col", "row")
    in_specs = (
        tok, P("dp", None), P(), P(), mat_t, P(), P(), mat, P(), P(), P(), mat_t, P(), mat, P(), tok,
    )
    grad, grad_t = P("row", "dp", "col"), P("col", "dp", "row")
    out_specs = (
        tok, tok, P(), P(), grad_t, P(), P(), grad, P(), P(), P(), grad_t, P(), grad, P(),
    )
    return jax.shard_map(
        functools.partial(shards, axis_sizes=sizes),
        mesh=mesh, in_specs=in_specs, out_specs=out_specs, check_vma=False,
    )
```

```python
import functools

import jax
import jax.numpy as jnp
from jax import lax
from jax.experimental import pallas as pl
from jax.experimental.pallas import tpu as pltpu
from jax.sharding import PartitionSpec as P

HEADS = 25
HEAD_DIM = 64
EPS = 1e-05
NEG = -1e30
GRAIN = 16
AXES = ("dp", "row", "col")
MESH = pl.DeviceIdType.MESH
F32 = jnp.float32
BF16 = jnp.bfloat16
VMEM_BYTES = 60 * 1024 * 1024

NN = (((1,), (0,)), ((), ()))
NT = (((1,), (1,)), ((), ()))
TN = (((0,), (0,)), ((), ()))


def dot(left, right, dims):
    return lax.dot_general(left, right, dims, preferred_element_type=F32)


class Place:
    def __init__(self):
        self.d = lax.axis_index("dp")
        self.r = lax.axis_index("row")
        self.c = lax.axis_index("col")
        one = self.r + 1 - 2 * lax.rem(self.r, 2)
        two = lax.rem(self.r + 2, 4)
        self.a = 1 + self.c
        self.b = 2 - self.c
        self.ra = (1 - self.c) * one + self.c * two
        self.rb = self.c * one + (1 - self.c) * two
        self.r3 = 3 - self.r

    def dev(self, row, col=None):
        return (self.d, row, self.c if col is None else col)

    def mate(self):
        return (self.d, self.r, 1 - self.c)

    def barrier(self, devices):
        semaphore = pltpu.get_barrier_semaphore()
        for device in devices:
            pl.semaphore_signal(semaphore, inc=1, device_id=device, device_id_type=MESH)
        pl.semaphore_wait(semaphore, len(devices))

    def group(self):
        flat = 2 * self.r + self.c
        found = []
        for step in range(1, 8):
            other = lax.rem(flat + step, 8)
            found.append((self.d, other // 2, lax.rem(other, 2)))
        return found

    def square(self):
        return [self.mate(), self.dev(self.ra), self.dev(self.rb)]


def rcopy(src, dst, send, recv, device):
    return pltpu.make_async_remote_copy(
        src_ref=src, dst_ref=dst, send_sem=send, recv_sem=recv, device_id=device,
        device_id_type=MESH,
    )


def lanes(index, size):
    return pl.ds(pl.multiple_of(index * size, size), size)


def call(kernel, out_shapes, out_specs, in_specs, scratch, cid, flops=0, bytes_accessed=0):
    return pl.pallas_call(
        kernel,
        out_shape=out_shapes,
        in_specs=in_specs,
        out_specs=out_specs,
        scratch_shapes=scratch,
        compiler_params=pltpu.CompilerParams(
            collective_id=cid, has_side_effects=True, vmem_limit_bytes=VMEM_BYTES
        ),
    )


VM = pl.BlockSpec(memory_space=pltpu.VMEM)
ANY = pl.BlockSpec(memory_space=pl.ANY)
DMA = pltpu.SemaphoreType.DMA


def struct(shape, dtype):
    return jax.ShapeDtypeStruct(shape, dtype)


def chunks(size):
    count = next(n for n in (5, 4, 2, 1) if size % (n * GRAIN) == 0)
    return [pl.ds(k * (size // count), size // count) for k in range(count)]


def col_sums(matrix):
    ones = jnp.ones((8, matrix.shape[1]), matrix.dtype)
    exact = lax.Precision.HIGHEST if matrix.dtype == F32 else None
    return lax.dot_general(ones, matrix, NT, precision=exact, preferred_element_type=F32)[0:1]


class Totals:
    scratch = [pltpu.VMEM((2, 8, 256), F32), DMA((2,))]

    def __init__(self, place, buf, sems):
        self.place, self.buf, self.sems = place, buf, sems

    def __call__(self, first, second):
        self.buf[0, 0:1] = jnp.sum(first, axis=0, keepdims=True)
        self.buf[0, 1:2] = jnp.sum(second, axis=0, keepdims=True)
        copy = rcopy(
            self.buf.at[0], self.buf.at[1], self.sems.at[0], self.sems.at[1], self.place.mate()
        )
        copy.start()
        copy.wait()
        return (
            self.buf[0, 0:1] + self.buf[1, 0:1],
            self.buf[0, 1:2] + self.buf[1, 1:2],
        )


def moments(totals, matrix, width):
    total, square = totals(matrix, matrix * matrix)
    average = total / width
    return average, lax.rsqrt(square / width - average * average + EPS)


def keep_moments(ref, average, rstd):
    ref[0:1] = average
    ref[1:2] = rstd


def norm_back(totals, grad_in, hat, rstd, gain, width):
    scaled = grad_in * gain
    total, mixed = totals(scaled, scaled * hat)
    return rstd * (scaled - total / width - hat * mixed / width)


def weight_scratch(rows, feats, turned):
    return [
        pltpu.VMEM((rows, turned), BF16), pltpu.VMEM((turned, rows), BF16),
        pltpu.VMEM((feats, rows), BF16), DMA((3,)),
    ]


def gather_scratch(rows, cols):
    count = len(chunks(rows))
    return [
        pltpu.VMEM((2, 4, rows, cols), BF16), DMA((7, count)), DMA((2, 4, count)), DMA((4,)),
    ]


class PairWeight:
    def __init__(self, place, w_ref, step, refs):
        self.flat, self.turned, self.other, sems = refs
        self.load = pltpu.make_async_copy(w_ref, self.flat, sems.at[2])
        self.load.start()
        feats = self.other.shape[0]
        self.own = self.turned.at[pl.ds(pl.multiple_of(step * place.c, GRAIN), feats)]
        theirs = self.turned.at[
            pl.ds(pl.multiple_of(step * (1 - place.c), GRAIN), feats)
        ]
        self.copy = rcopy(theirs, self.other, sems.at[0], sems.at[1], place.mate())

    def share(self):
        self.load.wait()
        self.turned[...] = self.flat[...].T
        self.copy.start()

    def product(self, own, other):
        return dot(self.own[...], own, NN) + dot(self.other[...], other, NN)


class Gather:
    def __init__(self, place, all_ref, refs):
        self.place, self.all_ref = place, all_ref
        self.got, self.send, self.recv, self.out_sem = refs

    def run(self, work, idle):
        place, got, send, recv = self.place, self.got, self.send, self.recv
        mate, size = place.mate(), got.shape[3]
        parts = list(enumerate(chunks(got.shape[2])))
        dev_a, dev_b = place.dev(place.ra), place.dev(place.rb)

        def move(number, source, target, device):
            return [
                rcopy(
                    got.at[source[0], source[1], part], got.at[target[0], target[1], part],
                    send.at[number, k], recv.at[target[0], target[1], k], device,
                )
                for k, part in parts
            ]

        def keep(slot, row, number):
            copy = pltpu.make_async_copy(
                got.at[0, slot], self.all_ref.at[:, lanes(row, size)], self.out_sem.at[number]
            )
            copy.start()
            return copy

        to_a = move(0, (0, 0), (0, place.a), dev_a)
        to_b = move(1, (0, 0), (0, place.b), dev_b)
        to_mate = move(2, (0, 0), (1, 0), mate)
        relay = move(3, (0, place.a), (0, 3), dev_b)
        fwd_a = move(4, (0, place.a), (1, place.a), mate)
        fwd_b = move(5, (0, place.b), (1, place.b), mate)
        fwd_3 = move(6, (0, 3), (1, 3), mate)
        for copies in (to_a, to_b, to_mate):
            for copy in copies:
                copy.start()
        kept = [keep(0, place.r, 0)]
        idle()
        for copy in to_mate:
            copy.wait_recv()
        work(0, place.r)
        for k, copy in enumerate(to_a):
            copy.wait_recv()
            relay[k].start()
            fwd_a[k].start()
        kept.append(keep(place.a, place.ra, 1))
        for k, copy in enumerate(to_b):
            copy.wait_recv()
            fwd_b[k].start()
        kept.append(keep(place.b, place.rb, 2))
        for copy in fwd_b:
            copy.wait_recv()
        work(place.b, place.rb)
        for copy in fwd_a:
            copy.wait_recv()
        work(place.a, place.ra)
        for k, copy in enumerate(relay):
            copy.wait_recv()
            fwd_3[k].start()
        kept.append(keep(3, place.r3, 3))
        for copy in fwd_3:
            copy.wait_recv()
        work(3, place.r3)
        for copies in (to_mate, to_a, to_b, relay, fwd_a, fwd_b, fwd_3):
            for copy in copies:
                copy.wait_send()
        for copy in kept:
            copy.wait()


def gather_triple(tokens, cols, bias, weight, width, feats, cid):
    rows, size = tokens.shape
    triple_width = weight.shape[1]
    grains = feats // GRAIN
    shift = triple_width - feats
    per = 3 * HEAD_DIM

    def kernel(x_ref, c_ref, b_ref, w_ref, all_ref, h_ref, st_ref, tt, tb, ts, gs, gr, *refs):
        place = Place()
        place.barrier(place.group())
        me = 2 * place.r + place.c
        weight = PairWeight(place, w_ref, shift, refs[:4])
        gather = Gather(place, all_ref, refs[4:])
        wide = x_ref[...].astype(F32)
        average, rstd = moments(Totals(place, tb, ts), wide, width)
        keep_moments(st_ref, average, rstd)
        gather.got[0, 0] = ((wide - average) * rstd * c_ref[:, 0:1] + c_ref[:, 1:2]).astype(BF16)

        def target(j):
            feature = triple_width * place.r + shift * place.c + GRAIN * j
            part = feature // width
            inner = feature - part * width
            head = inner // HEAD_DIM
            owner = jnp.minimum(head // 3, 7)
            row = (head - 3 * owner) * per + part * HEAD_DIM + (inner - head * HEAD_DIM)
            return owner, pl.ds(pl.multiple_of(row, GRAIN), GRAIN)

        def work(slot, row):
            total = weight.product(gather.got[0, slot], gather.got[1, slot])
            tt[:, lanes(row, size)] = (total + b_ref[...]).astype(BF16)

            def send_grain(j, carry):
                owner, place_rows = target(j)
                src = tt.at[pl.ds(pl.multiple_of(GRAIN * j, GRAIN), GRAIN), lanes(row, size)]
                dst = h_ref.at[place_rows, lanes(row, size)]

                @pl.when(owner == me)
                def _():
                    pltpu.make_async_copy(src, dst, gr).start()

                @pl.when(owner != me)
                def _():
                    rcopy(src, dst, gs, gr, (place.d, owner // 2, lax.rem(owner, 2))).start()

                return carry

            lax.fori_loop(place.c, grains, send_grain, 0)

        def idle():
            weight.share()
            weight.copy.wait()

        gather.run(work, idle)

        def drain(j, carry):
            @pl.when(target(j)[0] != me)
            def _():
                src = tt.at[pl.ds(0, GRAIN)]
                pltpu.make_async_copy(src, src, gs).wait()

            return carry

        lax.fori_loop(place.c, grains, drain, 0)

        @pl.when(me == 7)
        def _():
            pltpu.make_async_copy(h_ref, h_ref, gr).wait()

        @pl.when(me != 7)
        def _():
            part = h_ref.at[pl.ds(0, 3 * per)]
            pltpu.make_async_copy(part, part, gr).wait()

    return call(
        kernel,
        (struct((rows, 4 * size), BF16), struct((4 * per, 4 * size), BF16), struct((8, size), F32)),
        (ANY, ANY, VM), [VM] * 3 + [ANY],
        [pltpu.VMEM((feats, 4 * size), BF16)] + Totals.scratch + [DMA, DMA]
        + weight_scratch(rows, feats, triple_width) + gather_scratch(rows, size), cid,
    )(tokens, cols, bias, weight)


def gather_hidden(tokens, proj_out, cols, bias, cot, weight, back_weight, width, cid):
    rows, size = tokens.shape
    feats = weight.shape[1] // 2
    tokens_all = 4 * size

    def kernel(
        t_ref, p_ref, c_ref, b_ref, x_ref, w_ref, v_ref,
        all_ref, act_ref, hid_ref, mid_ref, st_ref, sum_ref, grad_ref,
        act, hid, swap_send, swap_recv, swap_out, cots, cot_sems, grads, grad_sum,
        tb, ts, *refs,
    ):
        place = Place()
        cot_load = pltpu.make_async_copy(x_ref, cots.at[0], cot_sems.at[2])
        cot_load.start()
        place.barrier(place.square())
        mate = place.mate()
        back = PairWeight(place, v_ref, feats, refs[:4])
        ahead = PairWeight(place, w_ref, feats, refs[4:8])
        gather = Gather(place, all_ref, refs[8:])
        cot_swap = rcopy(x_ref, cots.at[1], cot_sems.at[0], cot_sems.at[1], mate)
        middle = t_ref[...].astype(F32) + p_ref[...] + c_ref[:, 2:3]
        mid_ref[...] = middle
        average, rstd = moments(Totals(place, tb, ts), middle, width)
        keep_moments(st_ref, average, rstd)
        gather.got[0, 0] = ((middle - average) * rstd * c_ref[:, 3:4] + c_ref[:, 4:5]).astype(BF16)
        pending = []
        mine = pl.ds(pl.multiple_of(place.c * feats, GRAIN), feats)

        def idle():
            back.share()
            cot_swap.start()
            ahead.share()
            cot_load.wait()
            back.copy.wait()
            cot_swap.wait()

            def one(row, carry):
                grads[row] = back.product(cots[0, row], cots[1, row])
                return carry

            lax.fori_loop(0, 4, one, 0)
            ahead.copy.wait()

        def work(slot, row):
            number = len(pending)
            p = ahead.product(gather.got[0, slot], gather.got[1, slot]) + b_ref[...]
            square = p * p
            t = jnp.tanh(0.7978845608028654 * (p + 0.044715 * (square * p)))
            span = lanes(row, size)
            act[mine, span] = (0.5 * p * (1.0 + t)).astype(BF16)
            slope = 0.5 * (1.0 + t) + 0.5 * p * (1.0 - t * t) * (
                0.7978845608028654 * (1.0 + 3.0 * 0.044715 * square)
            )
            grad = grads[row] * slope
            hid[number] = grad.astype(BF16)
            there = hid_ref.at[mine, span]
            copies = [
                rcopy(
                    act.at[mine, span], act.at[mine, span],
                    swap_send.at[0, number], swap_recv.at[0, number], mate,
                ),
                rcopy(
                    hid.at[number], there, swap_send.at[1, number], swap_recv.at[1, number], mate
                ),
                pltpu.make_async_copy(hid.at[number], there, swap_out.at[number]),
            ]
            for copy in copies:
                copy.start()
            grad_sum[...] = grad if number == 0 else grad_sum[...] + grad
            pending.append(copies)

        gather.run(work, idle)
        sum_ref[0:1] = col_sums(grad_sum[...])
        for copies in pending:
            copies[0].wait()
        act_out = pltpu.make_async_copy(act, act_ref, swap_out.at[4])
        act_out.start()
        part = feats // 2

        def some(k, carry):
            here = pl.ds(pl.multiple_of(k * part, GRAIN), part)
            total = dot(act[here, 0:size], cots[0, 0], NT)
            for row in range(1, 4):
                total += dot(act[here, row * size : (row + 1) * size], cots[0, row], NT)
            grad_ref[here] = total.astype(BF16)
            return carry

        lax.fori_loop(0, 4, some, 0)
        for copies in pending:
            for copy in copies[1:]:
                copy.wait()
        act_out.wait()

    full = struct((2 * feats, tokens_all), BF16)
    return call(
        kernel,
        (
            struct((rows, tokens_all), BF16), full, full, struct((rows, size), F32),
            struct((8, size), F32), struct((8, feats), F32), struct((2 * feats, rows), BF16),
        ),
        (ANY, ANY, ANY, VM, VM, VM, VM), [VM] * 4 + [ANY] * 3,
        [pltpu.VMEM((2 * feats, tokens_all), BF16), pltpu.VMEM((4, feats, size), BF16)]
        + [DMA((2, 4)), DMA((2, 4)), DMA((5,))]
        + [pltpu.VMEM((2, 4, rows, size), BF16), DMA((3,))]
        + [pltpu.VMEM((4, feats, size), F32), pltpu.VMEM((feats, size), F32)]
        + Totals.scratch + weight_scratch(rows, feats, 2 * feats) * 2
        + gather_scratch(rows, size), cid,
    )(tokens, proj_out, cols, bias, cot, weight, back_weight)


def gather_middle(grad_in, middle, stats, cot, cols, weight, width, cid):
    rows, size = cot.shape
    owned = weight.shape[0]
    feats = 4 * HEAD_DIM
    step = 3 * HEAD_DIM
    lag = 3 * (owned - 2 * step)
    whole = lag + owned + 2 * HEAD_DIM

    def kernel(
        s_ref, m_ref, st_ref, x_ref, c_ref, w_ref, all_ref, y_ref, mg_ref, sum_ref,
        wide, other, w_sems, tb, ts, *refs,
    ):
        place = Place()
        load = pltpu.make_async_copy(w_ref, wide.at[pl.ds(lag, owned)], w_sems.at[0])
        load.start()
        place.barrier(place.group())
        before = rcopy(
            w_ref.at[pl.ds(owned - lag, lag)], wide.at[pl.ds(0, lag)], w_sems.at[1], w_sems.at[2],
            place.dev(lax.rem(place.r + 1, 4)),
        )
        before.start()
        wide[lag + owned : whole] = jnp.zeros((2 * HEAD_DIM, rows), BF16)
        first = lag - (owned - 2 * step) * place.r

        def heads(col):
            return wide.at[pl.ds(pl.multiple_of(first + step * col, GRAIN), feats)]

        swap = rcopy(heads(1 - place.c), other, w_sems.at[3], w_sems.at[4], place.mate())
        gather = Gather(place, all_ref, refs)
        rstd = st_ref[1:2]
        hat = (m_ref[...] - st_ref[0:1]) * rstd
        back = norm_back(Totals(place, tb, ts), s_ref[...], hat, rstd, c_ref[:, 3:4], width)
        mg_ref[...] = x_ref[...].astype(F32) + back
        gather.got[0, 0] = mg_ref[...].astype(BF16)

        def idle():
            load.wait()
            before.wait()
            swap.start()
            hat = (m_ref[...] - st_ref[0:1]) * st_ref[1:2]
            sum_ref[0:1] = col_sums(s_ref[...] * hat)
            sum_ref[1:2] = col_sums(s_ref[...])
            sum_ref[2:3] = col_sums(mg_ref[...])
            sum_ref[3:4] = col_sums(x_ref[...])
            swap.wait()

        def work(slot, row):
            total = dot(heads(place.c)[...], gather.got[0, slot], NN)
            total += dot(other[...], gather.got[1, slot], NN)
            y_ref[:, lanes(row, size)] = total.astype(BF16)

        gather.run(work, idle)

    return call(
        kernel,
        (
            struct((rows, 4 * size), BF16), struct((feats, 4 * size), BF16),
            struct((rows, size), F32), struct((8, rows), F32),
        ),
        (ANY, VM, VM, VM), [VM] * 5 + [ANY],
        [pltpu.VMEM((whole, rows), BF16), pltpu.VMEM((feats, rows), BF16), DMA((5,))]
        + Totals.scratch + gather_scratch(rows, size), cid,
    )(grad_in, middle, stats, cot, cols, weight)


def scatter_scratch(rows, cols):
    count = len(chunks(rows))
    return [
        pltpu.VMEM((3, rows, cols), BF16), pltpu.VMEM((3, rows, cols), BF16),
        DMA((3, count)), DMA((3, count)), pltpu.VMEM((rows, cols), F32),
    ]


def run_scatter(place, block, refs):
    outbox, inbox, send, recv, passed = refs
    parts = list(enumerate(chunks(outbox.shape[1])))

    def move(number, device):
        return [
            rcopy(
                outbox.at[number, part], inbox.at[number, part],
                send.at[number, k], recv.at[number, k], device,
            )
            for k, part in parts
        ]

    first = move(0, place.dev(place.ra))
    second = move(1, place.dev(place.ra))
    third = move(2, place.dev(place.rb))
    outbox[0] = block(place.r3).astype(BF16)
    for copy in first:
        copy.start()
    passed[...] = block(place.rb)
    outbox[1] = block(place.ra).astype(BF16)
    for copy in second:
        copy.start()
    for k, part in parts:
        first[k].wait_recv()
        outbox[2, part] = (passed[part] + inbox[0, part].astype(F32)).astype(BF16)
        third[k].start()
    passed[...] = block(place.r)
    for copy in second:
        copy.wait_recv()
    passed[...] += inbox[1].astype(F32)
    for copy in third:
        copy.wait_recv()
    total = passed[...] + inbox[2].astype(F32)
    for copies in (first, second, third):
        for copy in copies:
            copy.wait_send()
    return total


def load_scratch(weight, left):
    return [pltpu.VMEM(weight.shape, BF16), pltpu.VMEM(left.shape, BF16), DMA((5,))]


def loaded_block(place, l_ref, w_ref, weight, left, sems, size):
    w_load = pltpu.make_async_copy(w_ref, weight, sems.at[4])
    w_load.start()
    loads = []
    for k, row in enumerate((place.r3, place.rb, place.ra, place.r)):
        span = lanes(row, size)
        loads.append(pltpu.make_async_copy(l_ref.at[:, span], left.at[:, span], sems.at[k]))
        loads[-1].start()

    def block(row):
        if len(loads) == 4:
            w_load.wait()
        loads.pop(0).wait()
        return dot(weight[...], left[:, lanes(row, size)], NN)

    return block


def hidden_scatter(left, weight, cid):
    rows, size = weight.shape[0], left.shape[1] // 4

    def kernel(l_ref, w_ref, out_ref, w, l, l_sem, *refs):
        place = Place()
        block = loaded_block(place, l_ref, w_ref, w, l, l_sem, size)
        place.barrier([place.dev(place.ra), place.dev(place.rb)])
        out_ref[...] = run_scatter(place, block, refs)

    return call(
        kernel, struct((rows, size), F32), VM, [ANY] * 2,
        load_scratch(weight, left) + scatter_scratch(rows, size), cid,
    )(left, weight)


def output_scatter(left, weight, middle, cols, cid):
    rows, size = middle.shape

    def kernel(l_ref, w_ref, m_ref, c_ref, out_ref, w, l, l_sem, *refs):
        place = Place()
        block = loaded_block(place, l_ref, w_ref, w, l, l_sem, size)
        place.barrier([place.dev(place.ra), place.dev(place.rb)])
        total = run_scatter(place, block, refs)
        out_ref[...] = (m_ref[...] + total + c_ref[:, 5:6]).astype(BF16)

    return call(
        kernel, struct((rows, size), BF16), VM, [ANY, ANY, VM, VM],
        load_scratch(weight, left) + scatter_scratch(rows, size), cid,
    )(left, weight, middle, cols)


def attended_scatter(heads, weight, cid):
    feats, rows = weight.shape
    tokens = heads.shape[1]
    size = tokens // 4

    def kernel(h_ref, w_ref, all_ref, out_ref, full, gs, gr, kept_sem, *refs):
        place = Place()
        place.barrier(place.group())
        me = 2 * place.r + place.c
        count = jnp.where(me == 7, 4, 3) * (HEAD_DIM // GRAIN)

        def send_grain(j, carry):
            feature = 3 * HEAD_DIM * me + GRAIN * j
            owner = feature // feats
            src = h_ref.at[pl.ds(pl.multiple_of(GRAIN * j, GRAIN), GRAIN)]
            dst = full.at[pl.ds(pl.multiple_of(feature - owner * feats, GRAIN), GRAIN)]
            rcopy(src, dst, gs, gr, (place.d, owner, 1 - place.c)).start()

            @pl.when(owner == place.r)
            def _():
                pltpu.make_async_copy(src, dst, gr).start()

            @pl.when(owner != place.r)
            def _():
                rcopy(src, dst, gs, gr, (place.d, owner, place.c)).start()

            return carry

        lax.fori_loop(0, count, send_grain, 0)

        def drain(j, carry):
            feature = 3 * HEAD_DIM * me + GRAIN * j
            src = h_ref.at[pl.ds(0, GRAIN)]
            pltpu.make_async_copy(src, src, gs).wait()

            @pl.when(feature // feats != place.r)
            def _():
                pltpu.make_async_copy(src, src, gs).wait()

            return carry

        lax.fori_loop(0, count, drain, 0)
        pltpu.make_async_copy(full, full, gr).wait()
        kept = pltpu.make_async_copy(full, all_ref, kept_sem)
        kept.start()
        out_ref[...] = run_scatter(
            place, lambda row: dot(w_ref[...], full[:, lanes(row, size)], TN), refs
        )
        kept.wait()

    return call(
        kernel, (struct((feats, tokens), BF16), struct((rows, size), F32)),
        (ANY, VM), [ANY, VM],
        [pltpu.VMEM((feats, tokens), BF16), DMA, DMA, DMA] + scatter_scratch(rows, size), cid,
    )(heads, weight)


def triple_scatter(heads, weight, tokens, stats, middle_grad, cols, width, cid):
    rows, feats = weight.shape
    count_tokens = heads.shape[1]
    size = count_tokens // 4
    per = 3 * HEAD_DIM
    low = (feats // GRAIN + 1) // 2 * GRAIN

    def kernel(
        h_ref, w_ref, t_ref, st_ref, mg_ref, c_ref, all_ref, out_ref, sum_ref, bias_ref,
        full, w, w_sem, tb, ts, gs, gr, ms, mr, kept_sem, *refs,
    ):
        place = Place()
        w_load = pltpu.make_async_copy(w_ref, w, w_sem)
        w_load.start()
        place.barrier(place.group())
        me = 2 * place.r + place.c
        count = jnp.where(me == 7, 4, 3) * (per // GRAIN)

        def target(j):
            row = GRAIN * j
            head = row // per
            rest = row - head * per
            part = rest // HEAD_DIM
            feature = part * width + (3 * me + head) * HEAD_DIM + rest - part * HEAD_DIM
            owner = feature // feats
            inner = feature - owner * feats
            return 2 * owner + inner // low, inner

        def send_grain(j, carry):
            owner, inner = target(j)
            src = h_ref.at[pl.ds(pl.multiple_of(GRAIN * j, GRAIN), GRAIN)]
            dst = full.at[pl.ds(pl.multiple_of(inner, GRAIN), GRAIN)]

            @pl.when(owner == me)
            def _():
                pltpu.make_async_copy(src, dst, gr).start()

            @pl.when(owner != me)
            def _():
                rcopy(src, dst, gs, gr, (place.d, owner // 2, lax.rem(owner, 2))).start()

            return carry

        lax.fori_loop(0, count, send_grain, 0)

        def drain(j, carry):
            @pl.when(target(j)[0] != me)
            def _():
                src = h_ref.at[pl.ds(0, GRAIN)]
                pltpu.make_async_copy(src, src, gs).wait()

            return carry

        lax.fori_loop(0, count, drain, 0)
        lower, upper = full.at[pl.ds(0, low)], full.at[pl.ds(low, feats - low)]

        def swap(mine, theirs):
            pltpu.make_async_copy(mine, mine, gr).wait()
            copy = rcopy(mine, mine, ms, mr, place.mate())
            copy.start()
            copy.wait_send()
            pltpu.make_async_copy(theirs, theirs, mr).wait()

        @pl.when(place.c == 0)
        def _():
            swap(lower, upper)

        @pl.when(place.c == 1)
        def _():
            swap(upper, lower)

        kept = pltpu.make_async_copy(full, all_ref, kept_sem)
        kept.start()
        w_load.wait()
        grad = run_scatter(place, lambda row: dot(w[...], full[:, lanes(row, size)], NN), refs)
        rstd = st_ref[1:2]
        hat = (t_ref[...].astype(F32) - st_ref[0:1]) * rstd
        back = norm_back(Totals(place, tb, ts), grad, hat, rstd, c_ref[:, 0:1], width)
        out_ref[...] = mg_ref[...] + back
        sum_ref[0:1] = col_sums(grad * hat)
        sum_ref[1:2] = col_sums(grad)
        bias_ref[0:1] = col_sums(full[...])
        kept.wait()

    return call(
        kernel,
        (
            struct((feats, count_tokens), BF16), struct((rows, size), F32),
            struct((8, rows), F32), struct((8, feats), F32),
        ),
        (ANY, VM, VM, VM), [ANY, ANY] + [VM] * 4,
        [pltpu.VMEM((feats, count_tokens), BF16), pltpu.VMEM(weight.shape, BF16), DMA]
        + Totals.scratch + [DMA] * 5
        + scatter_scratch(rows, size), cid,
    )(heads, weight, tokens, stats, middle_grad, cols)


def attention_bias(seg_col, seg_row, bias_ref):
    tokens = seg_row.shape[1]
    key = lax.broadcasted_iota(jnp.int32, (tokens, tokens), 0)
    query = lax.broadcasted_iota(jnp.int32, (tokens, tokens), 1)
    allowed = (seg_col[...] == seg_row[...]) & (key <= query)
    bias_ref[...] = jnp.where(allowed, 0.0, NEG)


def holds(head):
    return (head < 3) | ((lax.axis_index("row") == 3) & (lax.axis_index("col") == 1))


def attention_forward(triple, seg_col, seg_row):
    per = 3 * HEAD_DIM
    tokens = triple.shape[1]
    span = tokens // 4

    def kernel(sc_ref, sr_ref, t_ref, o_ref, l_ref, bias_ref):
        @pl.when(pl.program_id(0) == 0)
        def _():
            attention_bias(sc_ref, sr_ref, bias_ref)

        @pl.when(holds(pl.program_id(0)))
        def _():
            for j in range(4):
                reach, here = (j + 1) * span, slice(j * span, (j + 1) * span)
                query = t_ref[0:HEAD_DIM, here] * BF16(HEAD_DIM ** (-0.5))
                score = dot(t_ref[HEAD_DIM : 2 * HEAD_DIM, 0:reach], query, TN)
                score = score + bias_ref[0:reach, here]
                top = jnp.max(score, axis=0, keepdims=True)
                weight = jnp.exp(score - top)
                total = jnp.sum(weight, axis=0, keepdims=True)
                mixed = dot(t_ref[2 * HEAD_DIM : per, 0:reach], weight.astype(BF16), NN)
                o_ref[:, here] = (mixed / total).astype(BF16)
                l_ref[0, :, here] = top + jnp.log(total)

    return pl.pallas_call(
        kernel,
        grid=(4,),
        out_shape=(
            jax.ShapeDtypeStruct((4 * HEAD_DIM, tokens), BF16),
            jax.ShapeDtypeStruct((4, 1, tokens), F32),
        ),
        in_specs=[
            pl.BlockSpec((tokens, 1), lambda h: (0, 0)),
            pl.BlockSpec((1, tokens), lambda h: (0, 0)),
            pl.BlockSpec((per, tokens), lambda h: (h, 0)),
        ],
        out_specs=(
            pl.BlockSpec((HEAD_DIM, tokens), lambda h: (h, 0)),
            pl.BlockSpec((1, 1, tokens), lambda h: (h, 0, 0)),
        ),
        scratch_shapes=[pltpu.VMEM((tokens, tokens), F32)],
        compiler_params=pltpu.CompilerParams(vmem_limit_bytes=VMEM_BYTES),
    )(seg_col, seg_row, triple)


def attention_backward(triple, seg_col, seg_row, attended, attended_grad, lse):
    per = 3 * HEAD_DIM
    tokens = triple.shape[1]
    span = tokens // 4

    def kernel(sc_ref, sr_ref, t_ref, o_ref, g_ref, l_ref, d_ref, bias_ref, kg_ref, vg_ref):
        @pl.when(pl.program_id(0) == 0)
        def _():
            attention_bias(sc_ref, sr_ref, bias_ref)

        @pl.when(holds(pl.program_id(0)))
        def _():
            kg_ref[...] = jnp.zeros_like(kg_ref)
            vg_ref[...] = jnp.zeros_like(vg_ref)
            for j in range(4):
                reach, here = (j + 1) * span, slice(j * span, (j + 1) * span)
                query = t_ref[0:HEAD_DIM, here] * BF16(HEAD_DIM ** (-0.5))
                key = t_ref[HEAD_DIM : 2 * HEAD_DIM, 0:reach]
                grad = g_ref[:, here]
                delta = jnp.sum(
                    grad.astype(F32) * o_ref[:, here].astype(F32), axis=0, keepdims=True
                )
                score = dot(key, query, TN) + bias_ref[0:reach, here]
                prob = jnp.exp(score - l_ref[0, :, here])
                vg_ref[:, 0:reach] += dot(grad, prob.astype(BF16), NT)
                back = dot(t_ref[2 * HEAD_DIM : per, 0:reach], grad, TN)
                mix = (prob * (back - delta)).astype(BF16)
                d_ref[0:HEAD_DIM, here] = (dot(key, mix, NN) * HEAD_DIM ** (-0.5)).astype(BF16)
                kg_ref[:, 0:reach] += dot(query, mix, NT)
            d_ref[HEAD_DIM : 2 * HEAD_DIM, :] = kg_ref[...].astype(BF16)
            d_ref[2 * HEAD_DIM : per, :] = vg_ref[...].astype(BF16)

    return pl.pallas_call(
        kernel,
        grid=(4,),
        out_shape=jax.ShapeDtypeStruct((4 * per, tokens), BF16),
        in_specs=[
            pl.BlockSpec((tokens, 1), lambda h: (0, 0)),
            pl.BlockSpec((1, tokens), lambda h: (0, 0)),
            pl.BlockSpec((per, tokens), lambda h: (h, 0)),
            pl.BlockSpec((HEAD_DIM, tokens), lambda h: (h, 0)),
            pl.BlockSpec((HEAD_DIM, tokens), lambda h: (h, 0)),
            pl.BlockSpec((1, 1, tokens), lambda h: (h, 0, 0)),
        ],
        out_specs=pl.BlockSpec((per, tokens), lambda h: (h, 0)),
        scratch_shapes=[
            pltpu.VMEM((tokens, tokens), F32),
            pltpu.VMEM((HEAD_DIM, tokens), F32),
            pltpu.VMEM((HEAD_DIM, tokens), F32),
        ],
        compiler_params=pltpu.CompilerParams(vmem_limit_bytes=VMEM_BYTES),
    )(seg_col, seg_row, triple, attended, attended_grad, lse)


def sum_all(pieces, sizes, cid):
    count = pieces.shape[0]
    rows, cols = sizes

    def kernel(x_ref, out_ref, inbox, piece, sems):
        me = (lax.axis_index("dp") * rows + lax.axis_index("row")) * cols + lax.axis_index("col")

        def dev(step):
            flat = lax.rem(me + step, count)
            return flat, (flat // (rows * cols), lax.rem(flat // cols, rows), lax.rem(flat, cols))

        semaphore = pltpu.get_barrier_semaphore()

        def greet(step, carry):
            pl.semaphore_signal(semaphore, inc=1, device_id=dev(step)[1], device_id_type=MESH)
            return carry

        lax.fori_loop(1, count, greet, 0)
        pl.semaphore_wait(semaphore, count - 1)

        def spread(step, carry):
            flat, device = dev(step)
            rcopy(x_ref.at[flat], inbox.at[me], sems.at[0], sems.at[1], device).start()
            return carry

        lax.fori_loop(1, count, spread, 0)
        inbox[me] = x_ref[me]
        rest = inbox.at[pl.ds(0, count - 1)]
        pltpu.make_async_copy(rest, rest, sems.at[1]).wait()
        pltpu.make_async_copy(rest, rest, sems.at[0]).wait()
        piece[...] = jnp.sum(inbox[...], axis=0)

        def share(step, carry):
            rcopy(piece, out_ref.at[me], sems.at[2], sems.at[3], dev(step)[1]).start()
            return carry

        lax.fori_loop(1, count, share, 0)
        out_ref[me] = piece[...]
        rest = out_ref.at[pl.ds(0, count - 1)]
        pltpu.make_async_copy(rest, rest, sems.at[3]).wait()
        pltpu.make_async_copy(rest, rest, sems.at[2]).wait()

    return call(
        kernel, jax.ShapeDtypeStruct(pieces.shape, F32), VM, [VM],
        [pltpu.VMEM(pieces.shape, F32), pltpu.VMEM(pieces.shape[1:], F32), DMA((4,))], cid,
    )(pieces)


def shards(
    tokens, segment_ids, first_gain, first_shift, triple_weight, query_bias, value_bias,
    proj_weight, proj_bias, second_gain, second_shift, expand_weight, expand_bias,
    shrink_weight, shrink_bias, cotangent, *, axis_sizes,
):
    width = HEADS * HEAD_DIM
    dp_count, row_count, col_count = axis_sizes
    row, col = lax.axis_index("row"), lax.axis_index("col")
    col_width = tokens.shape[1]
    triple_width = triple_weight.shape[1]
    hidden = expand_weight.shape[1] // 2
    core_feats = (triple_width // GRAIN + 1) // 2 * GRAIN

    stacked = jnp.concatenate(
        [first_gain, first_shift, proj_bias, second_gain, second_shift, shrink_bias]
    ).reshape(6, width)
    cols = lax.dynamic_slice_in_dim(stacked, col * col_width, col_width, 1).T
    full_bias = jnp.concatenate([query_bias, jnp.zeros((width,), F32), value_bias])
    core_bias = lax.dynamic_slice_in_dim(
        full_bias, row * triple_width + col * (triple_width - core_feats), core_feats
    )[:, None]
    core_expand_bias = lax.dynamic_slice_in_dim(
        expand_bias, (row * 2 + col) * hidden, hidden
    )[:, None]
    tokens_t, cot_t = tokens.T, cotangent.T
    seg_row = segment_ids
    seg_col = segment_ids.reshape(-1, 1)

    first_all, triple, first_stats = gather_triple(
        tokens_t, cols, core_bias, triple_weight, width, core_feats, 0
    )
    triple, cot_later = lax.optimization_barrier((triple, cot_t))
    cot_rows = lax.all_gather(cot_later, "row")
    attended, lse = attention_forward(triple, seg_col, seg_row)
    attended_all, proj_out = attended_scatter(attended, proj_weight, 2)
    (
        second_all, act_all, hid_all, middle, second_stats, expand_bias_part, shrink_grad
    ) = gather_hidden(
        tokens_t, proj_out, cols, core_expand_bias, cot_rows, expand_weight, shrink_weight.T,
        width, 3,
    )

    def product(left, right):
        return lax.dot_general(left, right, NT, preferred_element_type=F32).astype(BF16)

    def owned(grad):
        parts = grad.reshape(dp_count, -1, grad.shape[1])
        summed = lax.psum_scatter(parts, "dp", scatter_dimension=0, tiled=True)
        return summed.reshape(1, -1, grad.shape[1])

    shrink_owned = owned(shrink_grad)

    second_normed_grad = hidden_scatter(hid_all, expand_weight, 4)
    middle_all, attended_grad, middle_grad, second_sums = gather_middle(
        second_normed_grad, middle, second_stats, cot_t, cols, proj_weight, width, 5
    )
    proj_grad = product(attended_all, middle_all)
    pieces = [
        product(second_all, hid_all[:hidden]),
        product(second_all, hid_all[hidden:]),
        proj_grad,
    ]
    pieces = [piece.reshape(dp_count, -1, col_width) for piece in pieces]
    joint = sum(piece.shape[1] for piece in pieces)
    pieces.append(jnp.zeros((dp_count, -joint % 32, col_width), BF16))
    both_grad = jnp.concatenate(pieces, axis=1)
    attended_grad, shrink_owned, both_grad = lax.optimization_barrier(
        (attended_grad, shrink_owned, both_grad)
    )
    both_owned = owned(both_grad.reshape(-1, col_width))
    triple_head_grad = attention_backward(
        triple, seg_col, seg_row, attended, attended_grad, lse
    )
    triple_all, input_grad, first_sums, bias_sums = triple_scatter(
        triple_head_grad, triple_weight, tokens_t, first_stats, middle_grad, cols, width, 6
    )
    triple_grad = product(first_all, triple_all)
    act_all, triple_grad, both_owned, first_sums = lax.optimization_barrier(
        (act_all, triple_grad, both_owned, first_sums)
    )
    part = col_width // dp_count
    expand_owned = jnp.concatenate([both_owned[:, :part], both_owned[:, part : 2 * part]], axis=2)
    proj_owned = both_owned[:, 2 * part : joint]
    triple_owned = owned(triple_grad)
    block_out = output_scatter(act_all, shrink_weight.T, middle, cols, 7)

    by_col = jnp.concatenate([first_sums[:2], second_sums[:4]])
    is_col = (jnp.arange(2) == col).astype(F32)
    by_col = by_col[:, None, :] * is_col[None, :, None]
    is_core = (jnp.arange(2 * row_count) == 2 * row + col).astype(F32)
    by_core = expand_bias_part[0] * is_core[:, None]
    is_row = ((jnp.arange(row_count) == row) & (col == 0)).astype(F32)
    by_row = bias_sums[0][None, :] * is_row[:, None]
    vector = jnp.concatenate([by_col.reshape(-1), by_core.reshape(-1), by_row.reshape(-1)])
    devices = dp_count * row_count * col_count
    tile = 8 * 128
    size = -(-vector.shape[0] // (devices * tile)) * tile
    vector = jnp.pad(vector, (0, devices * size - vector.shape[0]))
    total = sum_all(
        vector.reshape(devices, size // 128, 128), (row_count, col_count), 8
    ).reshape(-1)
    col_totals = total[: 6 * width].reshape(6, width)
    expand_bias_grad = total[6 * width : 6 * width + 2 * row_count * hidden]
    rest = total[6 * width + 2 * row_count * hidden :]
    return (
        block_out.T,
        input_grad.T,
        col_totals[0],
        col_totals[1],
        triple_owned.astype(F32),
        rest[:width],
        rest[2 * width : 3 * width],
        proj_owned.astype(F32),
        col_totals[4],
        col_totals[2],
        col_totals[3],
        expand_owned.astype(F32),
        expand_bias_grad,
        shrink_owned.astype(F32),
        col_totals[5],
    )


def solution(mesh):
    assert mesh.shape["row"] == 4 and mesh.shape["col"] == 2
    sizes = tuple(mesh.shape[name] for name in AXES)
    tok, mat, mat_t = P(("dp", "row"), "col"), P("row", "col"), P("col", "row")
    in_specs = (
        tok, P("dp", None), P(), P(), mat_t, P(), P(), mat, P(), P(), P(), mat_t, P(), mat, P(), tok,
    )
    grad, grad_t = P("row", "dp", "col"), P("col", "dp", "row")
    out_specs = (
        tok, tok, P(), P(), grad_t, P(), P(), grad, P(), P(), P(), grad_t, P(), grad, P(),
    )
    return jax.shard_map(
        functools.partial(shards, axis_sizes=sizes),
        mesh=mesh, in_specs=in_specs, out_specs=out_specs, check_vma=False,
    )
```

```python
import functools

import jax
import jax.numpy as jnp
from jax import lax
from jax.experimental import pallas as pl
from jax.experimental.pallas import tpu as pltpu
from jax.sharding import PartitionSpec as P

HEADS = 25
HEAD_DIM = 64
EPS = 1e-05
NEG = -1e30
GRAIN = 16
AXES = ("dp", "row", "col")
MESH = pl.DeviceIdType.MESH
F32 = jnp.float32
BF16 = jnp.bfloat16
VMEM_BYTES = 60 * 1024 * 1024

NN = (((1,), (0,)), ((), ()))
NT = (((1,), (1,)), ((), ()))
TN = (((0,), (0,)), ((), ()))


def dot(left, right, dims):
    return lax.dot_general(left, right, dims, preferred_element_type=F32)


class Place:
    def __init__(self):
        self.d = lax.axis_index("dp")
        self.r = lax.axis_index("row")
        self.c = lax.axis_index("col")
        one = self.r + 1 - 2 * lax.rem(self.r, 2)
        two = lax.rem(self.r + 2, 4)
        self.a = 1 + self.c
        self.b = 2 - self.c
        self.ra = (1 - self.c) * one + self.c * two
        self.rb = self.c * one + (1 - self.c) * two
        self.r3 = 3 - self.r

    def dev(self, row, col=None):
        return (self.d, row, self.c if col is None else col)

    def mate(self):
        return (self.d, self.r, 1 - self.c)

    def barrier(self, devices):
        semaphore = pltpu.get_barrier_semaphore()
        for device in devices:
            pl.semaphore_signal(semaphore, inc=1, device_id=device, device_id_type=MESH)
        pl.semaphore_wait(semaphore, len(devices))

    def group(self):
        flat = 2 * self.r + self.c
        found = []
        for step in range(1, 8):
            other = lax.rem(flat + step, 8)
            found.append((self.d, other // 2, lax.rem(other, 2)))
        return found

    def square(self):
        return [self.mate(), self.dev(self.ra), self.dev(self.rb)]


def rcopy(src, dst, send, recv, device):
    return pltpu.make_async_remote_copy(
        src_ref=src, dst_ref=dst, send_sem=send, recv_sem=recv, device_id=device,
        device_id_type=MESH,
    )


def pick(k, zero, one, two, three):
    return jnp.where(k == 0, zero, jnp.where(k == 1, one, jnp.where(k == 2, two, three)))


def lanes(index, size):
    return pl.ds(pl.multiple_of(index * size, size), size)


def call(kernel, out_shapes, out_specs, in_specs, scratch, cid, flops=0, bytes_accessed=0):
    return pl.pallas_call(
        kernel,
        out_shape=out_shapes,
        in_specs=in_specs,
        out_specs=out_specs,
        scratch_shapes=scratch,
        compiler_params=pltpu.CompilerParams(
            collective_id=cid, has_side_effects=True, vmem_limit_bytes=VMEM_BYTES
        ),
    )


VM = pl.BlockSpec(memory_space=pltpu.VMEM)
ANY = pl.BlockSpec(memory_space=pl.ANY)
DMA = pltpu.SemaphoreType.DMA


def struct(shape, dtype):
    return jax.ShapeDtypeStruct(shape, dtype)


def chunks(size):
    count = next(n for n in (5, 4, 2, 1) if size % (n * GRAIN) == 0)
    return [pl.ds(k * (size // count), size // count) for k in range(count)]


def col_sums(matrix):
    ones = jnp.ones((8, matrix.shape[1]), matrix.dtype)
    exact = lax.Precision.HIGHEST if matrix.dtype == F32 else None
    return lax.dot_general(ones, matrix, NT, precision=exact, preferred_element_type=F32)[0:1]


class Totals:
    scratch = [pltpu.VMEM((2, 8, 256), F32), DMA((2,))]

    def __init__(self, place, buf, sems):
        self.place, self.buf, self.sems = place, buf, sems

    def __call__(self, first, second):
        self.buf[0, 0:1] = jnp.sum(first, axis=0, keepdims=True)
        self.buf[0, 1:2] = jnp.sum(second, axis=0, keepdims=True)
        copy = rcopy(
            self.buf.at[0], self.buf.at[1], self.sems.at[0], self.sems.at[1], self.place.mate()
        )
        copy.start()
        copy.wait()
        return (
            self.buf[0, 0:1] + self.buf[1, 0:1],
            self.buf[0, 1:2] + self.buf[1, 1:2],
        )


def moments(totals, matrix, width):
    total, square = totals(matrix, matrix * matrix)
    average = total / width
    return average, lax.rsqrt(square / width - average * average + EPS)


def keep_moments(ref, average, rstd):
    ref[0:1] = average
    ref[1:2] = rstd


def norm_back(totals, grad_in, hat, rstd, gain, width):
    scaled = grad_in * gain
    total, mixed = totals(scaled, scaled * hat)
    return rstd * (scaled - total / width - hat * mixed / width)


def weight_scratch(rows, feats, turned):
    return [
        pltpu.VMEM((rows, turned), BF16), pltpu.VMEM((turned, rows), BF16),
        pltpu.VMEM((feats, rows), BF16), DMA((3,)),
    ]


def gather_scratch(rows, cols):
    count = len(chunks(rows))
    return [
        pltpu.VMEM((2, 4, rows, cols), BF16), DMA((7, count)), DMA((2, 4, count)), DMA((4,)),
    ]


class PairWeight:
    def __init__(self, place, w_ref, step, refs):
        self.flat, self.turned, self.other, sems = refs
        self.load = pltpu.make_async_copy(w_ref, self.flat, sems.at[2])
        self.load.start()
        feats = self.other.shape[0]
        self.own = self.turned.at[pl.ds(pl.multiple_of(step * place.c, GRAIN), feats)]
        theirs = self.turned.at[
            pl.ds(pl.multiple_of(step * (1 - place.c), GRAIN), feats)
        ]
        self.copy = rcopy(theirs, self.other, sems.at[0], sems.at[1], place.mate())

    def share(self):
        self.load.wait()
        self.turned[...] = self.flat[...].T
        self.copy.start()

    def product(self, own, other):
        return dot(self.own[...], own, NN) + dot(self.other[...], other, NN)


class Gather:
    def __init__(self, place, all_ref, refs):
        self.place, self.all_ref = place, all_ref
        self.got, self.send, self.recv, self.out_sem = refs

    def run(self, work, idle):
        place, got, send, recv = self.place, self.got, self.send, self.recv
        mate, size = place.mate(), got.shape[3]
        parts = list(enumerate(chunks(got.shape[2])))
        dev_a, dev_b = place.dev(place.ra), place.dev(place.rb)

        def move(number, source, target, device):
            return [
                rcopy(
                    got.at[source[0], source[1], part], got.at[target[0], target[1], part],
                    send.at[number, k], recv.at[target[0], target[1], k], device,
                )
                for k, part in parts
            ]

        def keep(slot, row, number):
            return pltpu.make_async_copy(
                got.at[0, slot], self.all_ref.at[:, lanes(row, size)], self.out_sem.at[number]
            )

        to_a = move(0, (0, 0), (0, place.a), dev_a)
        to_b = move(1, (0, 0), (0, place.b), dev_b)
        to_mate = move(2, (0, 0), (1, 0), mate)
        relay = move(3, (0, place.a), (0, 3), dev_b)
        fwd_a = move(4, (0, place.a), (1, place.a), mate)
        fwd_b = move(5, (0, place.b), (1, place.b), mate)
        fwd_3 = move(6, (0, 3), (1, 3), mate)
        for copies in (to_a, to_b, to_mate):
            for copy in copies:
                copy.start()
        keep(0, place.r, 0).start()
        idle()

        def phase(k, carry):
            @pl.when(k == 0)
            def _():
                for copy in to_mate:
                    copy.wait_recv()

            @pl.when(k == 1)
            def _():
                for n, copy in enumerate(to_a):
                    copy.wait_recv()
                    relay[n].start()
                    fwd_a[n].start()
                keep(place.a, place.ra, 1).start()
                for n, copy in enumerate(to_b):
                    copy.wait_recv()
                    fwd_b[n].start()
                keep(place.b, place.rb, 2).start()
                for copy in fwd_b:
                    copy.wait_recv()

            @pl.when(k == 2)
            def _():
                for copy in fwd_a:
                    copy.wait_recv()

            @pl.when(k == 3)
            def _():
                for n, copy in enumerate(relay):
                    copy.wait_recv()
                    fwd_3[n].start()
                keep(3, place.r3, 3).start()
                for copy in fwd_3:
                    copy.wait_recv()

            slot = pick(k, 0, place.b, place.a, 3)
            work(k, slot, pick(k, place.r, place.rb, place.ra, place.r3))
            return carry

        lax.fori_loop(0, 4, phase, 0)
        for copies in (to_mate, to_a, to_b, relay, fwd_a, fwd_b, fwd_3):
            for copy in copies:
                copy.wait_send()
        for slot, row, number in (
            (0, place.r, 0), (place.a, place.ra, 1), (place.b, place.rb, 2), (3, place.r3, 3)
        ):
            keep(slot, row, number).wait()


def gather_triple(tokens, cols, bias, weight, width, feats, cid):
    rows, size = tokens.shape
    triple_width = weight.shape[1]
    grains = feats // GRAIN
    shift = triple_width - feats
    per = 3 * HEAD_DIM

    def kernel(x_ref, c_ref, b_ref, w_ref, all_ref, h_ref, st_ref, tt, tb, ts, gs, gr, *refs):
        place = Place()
        place.barrier(place.group())
        me = 2 * place.r + place.c
        weight = PairWeight(place, w_ref, shift, refs[:4])
        gather = Gather(place, all_ref, refs[4:])
        wide = x_ref[...].astype(F32)
        average, rstd = moments(Totals(place, tb, ts), wide, width)
        keep_moments(st_ref, average, rstd)
        gather.got[0, 0] = ((wide - average) * rstd * c_ref[:, 0:1] + c_ref[:, 1:2]).astype(BF16)

        def target(j):
            feature = triple_width * place.r + shift * place.c + GRAIN * j
            part = feature // width
            inner = feature - part * width
            head = inner // HEAD_DIM
            owner = jnp.minimum(head // 3, 7)
            row = (head - 3 * owner) * per + part * HEAD_DIM + (inner - head * HEAD_DIM)
            return owner, pl.ds(pl.multiple_of(row, GRAIN), GRAIN)

        def work(k, slot, row):
            total = weight.product(gather.got[0, slot], gather.got[1, slot])
            tt[:, lanes(row, size)] = (total + b_ref[...]).astype(BF16)

            def send_grain(j, carry):
                owner, place_rows = target(j)
                src = tt.at[pl.ds(pl.multiple_of(GRAIN * j, GRAIN), GRAIN), lanes(row, size)]
                dst = h_ref.at[place_rows, lanes(row, size)]

                @pl.when(owner == me)
                def _():
                    pltpu.make_async_copy(src, dst, gr).start()

                @pl.when(owner != me)
                def _():
                    rcopy(src, dst, gs, gr, (place.d, owner // 2, lax.rem(owner, 2))).start()

                return carry

            lax.fori_loop(place.c, grains, send_grain, 0)

        def idle():
            weight.share()
            weight.copy.wait()

        gather.run(work, idle)

        def drain(j, carry):
            @pl.when(target(j)[0] != me)
            def _():
                src = tt.at[pl.ds(0, GRAIN)]
                pltpu.make_async_copy(src, src, gs).wait()

            return carry

        lax.fori_loop(place.c, grains, drain, 0)

        @pl.when(me == 7)
        def _():
            pltpu.make_async_copy(h_ref, h_ref, gr).wait()

        @pl.when(me != 7)
        def _():
            part = h_ref.at[pl.ds(0, 3 * per)]
            pltpu.make_async_copy(part, part, gr).wait()

    return call(
        kernel,
        (struct((rows, 4 * size), BF16), struct((4 * per, 4 * size), BF16), struct((8, size), F32)),
        (ANY, ANY, VM), [VM] * 3 + [ANY],
        [pltpu.VMEM((feats, 4 * size), BF16)] + Totals.scratch + [DMA, DMA]
        + weight_scratch(rows, feats, triple_width) + gather_scratch(rows, size), cid,
    )(tokens, cols, bias, weight)


def gather_hidden(tokens, proj_out, cols, bias, cot, weight, back_weight, width, cid):
    rows, size = tokens.shape
    feats = weight.shape[1] // 2
    tokens_all = 4 * size

    def kernel(
        t_ref, p_ref, c_ref, b_ref, x_ref, w_ref, v_ref,
        all_ref, act_ref, hid_ref, mid_ref, st_ref, sum_ref, grad_ref,
        act, hid, swap_send, swap_recv, swap_out, cots, cot_sems, grads, grad_sum,
        tb, ts, *refs,
    ):
        place = Place()
        cot_load = pltpu.make_async_copy(x_ref, cots.at[0], cot_sems.at[2])
        cot_load.start()
        place.barrier(place.square())
        mate = place.mate()
        back = PairWeight(place, v_ref, feats, refs[:4])
        ahead = PairWeight(place, w_ref, feats, refs[4:8])
        gather = Gather(place, all_ref, refs[8:])
        cot_swap = rcopy(x_ref, cots.at[1], cot_sems.at[0], cot_sems.at[1], mate)
        middle = t_ref[...].astype(F32) + p_ref[...] + c_ref[:, 2:3]
        mid_ref[...] = middle
        average, rstd = moments(Totals(place, tb, ts), middle, width)
        keep_moments(st_ref, average, rstd)
        gather.got[0, 0] = ((middle - average) * rstd * c_ref[:, 3:4] + c_ref[:, 4:5]).astype(BF16)
        mine = pl.ds(pl.multiple_of(place.c * feats, GRAIN), feats)
        grad_sum[...] = jnp.zeros_like(grad_sum)

        def moves(k, row):
            span = lanes(row, size)
            index = row
            there = hid_ref.at[mine, span]
            return (
                rcopy(
                    act.at[mine, span], act.at[mine, span],
                    swap_send.at[0, k], swap_recv.at[0, index], mate,
                ),
                rcopy(hid.at[k], there, swap_send.at[1, k], swap_recv.at[1, index], mate),
                pltpu.make_async_copy(hid.at[k], there, swap_out.at[k]),
            )

        def idle():
            back.share()
            cot_swap.start()
            ahead.share()
            cot_load.wait()
            back.copy.wait()
            cot_swap.wait()

            def one(row, carry):
                grads[row] = back.product(cots[0, row], cots[1, row])
                return carry

            lax.fori_loop(0, 4, one, 0)
            ahead.copy.wait()

        def work(k, slot, row):
            p = ahead.product(gather.got[0, slot], gather.got[1, slot]) + b_ref[...]
            square = p * p
            t = jnp.tanh(0.7978845608028654 * (p + 0.044715 * (square * p)))
            act[mine, lanes(row, size)] = (0.5 * p * (1.0 + t)).astype(BF16)
            slope = 0.5 * (1.0 + t) + 0.5 * p * (1.0 - t * t) * (
                0.7978845608028654 * (1.0 + 3.0 * 0.044715 * square)
            )
            grad = grads[row] * slope
            hid[k] = grad.astype(BF16)
            for copy in moves(k, row):
                copy.start()
            grad_sum[...] += grad

        gather.run(work, idle)
        sum_ref[0:1] = col_sums(grad_sum[...])
        order = [place.r, place.rb, place.ra, place.r3]
        for k, row in enumerate(order):
            moves(k, row)[0].wait()
        act_out = pltpu.make_async_copy(act, act_ref, swap_out.at[4])
        act_out.start()
        part = feats // 2

        def some(k, carry):
            here = pl.ds(pl.multiple_of(k * part, GRAIN), part)
            total = dot(act[here, 0:size], cots[0, 0], NT)
            for row in range(1, 4):
                total += dot(act[here, row * size : (row + 1) * size], cots[0, row], NT)
            grad_ref[here] = total.astype(BF16)
            return carry

        lax.fori_loop(0, 4, some, 0)
        for k, row in enumerate(order):
            for copy in moves(k, row)[1:]:
                copy.wait()
        act_out.wait()

    full = struct((2 * feats, tokens_all), BF16)
    return call(
        kernel,
        (
            struct((rows, tokens_all), BF16), full, full, struct((rows, size), F32),
            struct((8, size), F32), struct((8, feats), F32), struct((2 * feats, rows), BF16),
        ),
        (ANY, ANY, ANY, VM, VM, VM, VM), [VM] * 4 + [ANY] * 3,
        [pltpu.VMEM((2 * feats, tokens_all), BF16), pltpu.VMEM((4, feats, size), BF16)]
        + [DMA((2, 4)), DMA((2, 4)), DMA((5,))]
        + [pltpu.VMEM((2, 4, rows, size), BF16), DMA((3,))]
        + [pltpu.VMEM((4, feats, size), F32), pltpu.VMEM((feats, size), F32)]
        + Totals.scratch + weight_scratch(rows, feats, 2 * feats) * 2
        + gather_scratch(rows, size), cid,
    )(tokens, proj_out, cols, bias, cot, weight, back_weight)


def gather_middle(grad_in, middle, stats, cot, cols, weight, width, cid):
    rows, size = cot.shape
    owned = weight.shape[0]
    feats = 4 * HEAD_DIM
    step = 3 * HEAD_DIM
    lag = 3 * (owned - 2 * step)
    whole = lag + owned + 2 * HEAD_DIM

    def kernel(
        s_ref, m_ref, st_ref, x_ref, c_ref, w_ref, all_ref, y_ref, mg_ref, sum_ref,
        wide, other, w_sems, tb, ts, *refs,
    ):
        place = Place()
        load = pltpu.make_async_copy(w_ref, wide.at[pl.ds(lag, owned)], w_sems.at[0])
        load.start()
        place.barrier(place.group())
        before = rcopy(
            w_ref.at[pl.ds(owned - lag, lag)], wide.at[pl.ds(0, lag)], w_sems.at[1], w_sems.at[2],
            place.dev(lax.rem(place.r + 1, 4)),
        )
        before.start()
        wide[lag + owned : whole] = jnp.zeros((2 * HEAD_DIM, rows), BF16)
        first = lag - (owned - 2 * step) * place.r

        def heads(col):
            return wide.at[pl.ds(pl.multiple_of(first + step * col, GRAIN), feats)]

        swap = rcopy(heads(1 - place.c), other, w_sems.at[3], w_sems.at[4], place.mate())
        gather = Gather(place, all_ref, refs)
        rstd = st_ref[1:2]
        hat = (m_ref[...] - st_ref[0:1]) * rstd
        back = norm_back(Totals(place, tb, ts), s_ref[...], hat, rstd, c_ref[:, 3:4], width)
        mg_ref[...] = x_ref[...].astype(F32) + back
        gather.got[0, 0] = mg_ref[...].astype(BF16)

        def idle():
            load.wait()
            before.wait()
            swap.start()
            hat = (m_ref[...] - st_ref[0:1]) * st_ref[1:2]
            sum_ref[0:1] = col_sums(s_ref[...] * hat)
            sum_ref[1:2] = col_sums(s_ref[...])
            sum_ref[2:3] = col_sums(mg_ref[...])
            sum_ref[3:4] = col_sums(x_ref[...])
            swap.wait()

        def work(k, slot, row):
            total = dot(heads(place.c)[...], gather.got[0, slot], NN)
            total += dot(other[...], gather.got[1, slot], NN)
            y_ref[:, lanes(row, size)] = total.astype(BF16)

        gather.run(work, idle)

    return call(
        kernel,
        (
            struct((rows, 4 * size), BF16), struct((feats, 4 * size), BF16),
            struct((rows, size), F32), struct((8, rows), F32),
        ),
        (ANY, VM, VM, VM), [VM] * 5 + [ANY],
        [pltpu.VMEM((whole, rows), BF16), pltpu.VMEM((feats, rows), BF16), DMA((5,))]
        + Totals.scratch + gather_scratch(rows, size), cid,
    )(grad_in, middle, stats, cot, cols, weight)


def scatter_scratch(rows, cols):
    count = len(chunks(rows))
    return [
        pltpu.VMEM((3, rows, cols), BF16), pltpu.VMEM((3, rows, cols), BF16),
        DMA((3, count)), DMA((3, count)), pltpu.VMEM((rows, cols), F32),
    ]


def run_scatter(place, block, refs):
    outbox, inbox, send, recv, passed = refs
    parts = list(enumerate(chunks(outbox.shape[1])))

    def move(number, device):
        return [
            rcopy(
                outbox.at[number, part], inbox.at[number, part],
                send.at[number, k], recv.at[number, k], device,
            )
            for k, part in parts
        ]

    first = move(0, place.dev(place.ra))
    second = move(1, place.dev(place.ra))
    third = move(2, place.dev(place.rb))

    def phase(k, carry):
        @pl.when(k == 3)
        def _():
            for n, part in parts:
                first[n].wait_recv()
                outbox[2, part] = (passed[part] + inbox[0, part].astype(F32)).astype(BF16)
                third[n].start()

        total = block(k, pick(k, place.r3, place.rb, place.ra, place.r))

        @pl.when((k == 1) | (k == 3))
        def _():
            passed[...] = total

        @pl.when(k == 0)
        def _():
            outbox[0] = total.astype(BF16)
            for copy in first:
                copy.start()

        @pl.when(k == 2)
        def _():
            outbox[1] = total.astype(BF16)
            for copy in second:
                copy.start()

        return carry

    lax.fori_loop(0, 4, phase, 0)
    for copy in second:
        copy.wait_recv()
    passed[...] += inbox[1].astype(F32)
    for copy in third:
        copy.wait_recv()
    total = passed[...] + inbox[2].astype(F32)
    for copies in (first, second, third):
        for copy in copies:
            copy.wait_send()
    return total


def load_scratch(weight, left):
    return [pltpu.VMEM(weight.shape, BF16), pltpu.VMEM(left.shape, BF16), DMA((5,))]


def loaded_block(place, l_ref, w_ref, weight, left, sems, size):
    w_load = pltpu.make_async_copy(w_ref, weight, sems.at[4])
    w_load.start()

    def load(k, row):
        span = lanes(row, size)
        return pltpu.make_async_copy(l_ref.at[:, span], left.at[:, span], sems.at[k])

    for k, row in enumerate((place.r3, place.rb, place.ra, place.r)):
        load(k, row).start()

    def block(k, row):
        @pl.when(k == 0)
        def _():
            w_load.wait()

        load(k, row).wait()
        return dot(weight[...], left[:, lanes(row, size)], NN)

    return block


def hidden_scatter(left, weight, cid):
    rows, size = weight.shape[0], left.shape[1] // 4

    def kernel(l_ref, w_ref, out_ref, w, l, l_sem, *refs):
        place = Place()
        block = loaded_block(place, l_ref, w_ref, w, l, l_sem, size)
        place.barrier([place.dev(place.ra), place.dev(place.rb)])
        out_ref[...] = run_scatter(place, block, refs)

    return call(
        kernel, struct((rows, size), F32), VM, [ANY] * 2,
        load_scratch(weight, left) + scatter_scratch(rows, size), cid,
    )(left, weight)


def output_scatter(left, weight, middle, cols, cid):
    rows, size = middle.shape

    def kernel(l_ref, w_ref, m_ref, c_ref, out_ref, w, l, l_sem, *refs):
        place = Place()
        block = loaded_block(place, l_ref, w_ref, w, l, l_sem, size)
        place.barrier([place.dev(place.ra), place.dev(place.rb)])
        total = run_scatter(place, block, refs)
        out_ref[...] = (m_ref[...] + total + c_ref[:, 5:6]).astype(BF16)

    return call(
        kernel, struct((rows, size), BF16), VM, [ANY, ANY, VM, VM],
        load_scratch(weight, left) + scatter_scratch(rows, size), cid,
    )(left, weight, middle, cols)


def attended_scatter(heads, weight, cid):
    feats, rows = weight.shape
    tokens = heads.shape[1]
    size = tokens // 4

    def kernel(h_ref, w_ref, all_ref, out_ref, full, gs, gr, kept_sem, *refs):
        place = Place()
        place.barrier(place.group())
        me = 2 * place.r + place.c
        count = jnp.where(me == 7, 4, 3) * (HEAD_DIM // GRAIN)

        def send_grain(j, carry):
            feature = 3 * HEAD_DIM * me + GRAIN * j
            owner = feature // feats
            src = h_ref.at[pl.ds(pl.multiple_of(GRAIN * j, GRAIN), GRAIN)]
            dst = full.at[pl.ds(pl.multiple_of(feature - owner * feats, GRAIN), GRAIN)]
            rcopy(src, dst, gs, gr, (place.d, owner, 1 - place.c)).start()

            @pl.when(owner == place.r)
            def _():
                pltpu.make_async_copy(src, dst, gr).start()

            @pl.when(owner != place.r)
            def _():
                rcopy(src, dst, gs, gr, (place.d, owner, place.c)).start()

            return carry

        lax.fori_loop(0, count, send_grain, 0)

        def drain(j, carry):
            feature = 3 * HEAD_DIM * me + GRAIN * j
            src = h_ref.at[pl.ds(0, GRAIN)]
            pltpu.make_async_copy(src, src, gs).wait()

            @pl.when(feature // feats != place.r)
            def _():
                pltpu.make_async_copy(src, src, gs).wait()

            return carry

        lax.fori_loop(0, count, drain, 0)
        pltpu.make_async_copy(full, full, gr).wait()
        kept = pltpu.make_async_copy(full, all_ref, kept_sem)
        kept.start()
        out_ref[...] = run_scatter(
            place, lambda k, row: dot(w_ref[...], full[:, lanes(row, size)], TN), refs
        )
        kept.wait()

    return call(
        kernel, (struct((feats, tokens), BF16), struct((rows, size), F32)),
        (ANY, VM), [ANY, VM],
        [pltpu.VMEM((feats, tokens), BF16), DMA, DMA, DMA] + scatter_scratch(rows, size), cid,
    )(heads, weight)


def triple_scatter(heads, weight, tokens, stats, middle_grad, cols, pieces, width, cid):
    groups = pieces.shape[0]
    rows, feats = weight.shape
    count_tokens = heads.shape[1]
    size = count_tokens // 4
    per = 3 * HEAD_DIM
    low = (feats // GRAIN + 1) // 2 * GRAIN

    def kernel(
        h_ref, w_ref, p_ref, t_ref, st_ref, mg_ref, c_ref,
        all_ref, got_ref, out_ref, sum_ref, bias_ref, full, w, w_sem, p_sems, tb, ts, gs, gr, ms, mr, kept_sem, *refs,
    ):
        place = Place()
        w_load = pltpu.make_async_copy(w_ref, w, w_sem)
        w_load.start()
        peers = [
            (lax.rem(place.d + step, groups), place.r, place.c) for step in range(1, groups)
        ]
        place.barrier(place.group() + peers)
        me = 2 * place.r + place.c
        count = jnp.where(me == 7, 4, 3) * (per // GRAIN)

        def target(j):
            row = GRAIN * j
            head = row // per
            rest = row - head * per
            part = rest // HEAD_DIM
            feature = part * width + (3 * me + head) * HEAD_DIM + rest - part * HEAD_DIM
            owner = feature // feats
            inner = feature - owner * feats
            return 2 * owner + inner // low, inner

        def send_grain(j, carry):
            owner, inner = target(j)
            src = h_ref.at[pl.ds(pl.multiple_of(GRAIN * j, GRAIN), GRAIN)]
            dst = full.at[pl.ds(pl.multiple_of(inner, GRAIN), GRAIN)]

            @pl.when(owner == me)
            def _():
                pltpu.make_async_copy(src, dst, gr).start()

            @pl.when(owner != me)
            def _():
                rcopy(src, dst, gs, gr, (place.d, owner // 2, lax.rem(owner, 2))).start()

            return carry

        lax.fori_loop(0, count, send_grain, 0)
        traded = [
            rcopy(
                p_ref.at[peer[0]], got_ref.at[place.d],
                p_sems.at[0, k], p_sems.at[1, k], peer,
            )
            for k, peer in enumerate(peers)
        ]
        for copy in traded:
            copy.start()
        own_piece = pltpu.make_async_copy(
            p_ref.at[place.d], got_ref.at[place.d], p_sems.at[0, groups - 1]
        )
        own_piece.start()

        def drain(j, carry):
            @pl.when(target(j)[0] != me)
            def _():
                src = h_ref.at[pl.ds(0, GRAIN)]
                pltpu.make_async_copy(src, src, gs).wait()

            return carry

        lax.fori_loop(0, count, drain, 0)
        lower, upper = full.at[pl.ds(0, low)], full.at[pl.ds(low, feats - low)]

        def swap(mine, theirs):
            pltpu.make_async_copy(mine, mine, gr).wait()
            copy = rcopy(mine, mine, ms, mr, place.mate())
            copy.start()
            copy.wait_send()
            pltpu.make_async_copy(theirs, theirs, mr).wait()

        @pl.when(place.c == 0)
        def _():
            swap(lower, upper)

        @pl.when(place.c == 1)
        def _():
            swap(upper, lower)

        kept = pltpu.make_async_copy(full, all_ref, kept_sem)
        kept.start()
        w_load.wait()
        grad = run_scatter(place, lambda k, row: dot(w[...], full[:, lanes(row, size)], NN), refs)
        rstd = st_ref[1:2]
        hat = (t_ref[...].astype(F32) - st_ref[0:1]) * rstd
        back = norm_back(Totals(place, tb, ts), grad, hat, rstd, c_ref[:, 0:1], width)
        out_ref[...] = mg_ref[...] + back
        sum_ref[0:1] = col_sums(grad * hat)
        sum_ref[1:2] = col_sums(grad)
        bias_ref[0:1] = col_sums(full[...])
        kept.wait()
        own_piece.wait()
        for copy in traded:
            copy.wait()

    return call(
        kernel,
        (
            struct((feats, count_tokens), BF16), struct(pieces.shape, BF16),
            struct((rows, size), F32), struct((8, rows), F32), struct((8, feats), F32),
        ),
        (ANY, ANY, VM, VM, VM), [ANY] * 3 + [VM] * 4,
        [pltpu.VMEM((feats, count_tokens), BF16), pltpu.VMEM(weight.shape, BF16), DMA]
        + [DMA((2, groups))]
        + Totals.scratch + [DMA] * 5
        + scatter_scratch(rows, size), cid,
    )(heads, weight, pieces, tokens, stats, middle_grad, cols)


def attention_bias(seg_col, seg_row, bias_ref):
    tokens = seg_row.shape[1]
    key = lax.broadcasted_iota(jnp.int32, (tokens, tokens), 0)
    query = lax.broadcasted_iota(jnp.int32, (tokens, tokens), 1)
    allowed = (seg_col[...] == seg_row[...]) & (key <= query)
    bias_ref[...] = jnp.where(allowed, 0.0, NEG)


def holds(head):
    return (head < 3) | ((lax.axis_index("row") == 3) & (lax.axis_index("col") == 1))


def attention_forward(triple, seg_col, seg_row):
    per = 3 * HEAD_DIM
    tokens = triple.shape[1]
    span = tokens // 4

    def kernel(sc_ref, sr_ref, t_ref, o_ref, l_ref, bias_ref):
        @pl.when(pl.program_id(0) == 0)
        def _():
            attention_bias(sc_ref, sr_ref, bias_ref)

        @pl.when(holds(pl.program_id(0)))
        def _():
            for j in range(4):
                reach, here = (j + 1) * span, slice(j * span, (j + 1) * span)
                query = t_ref[0:HEAD_DIM, here] * BF16(HEAD_DIM ** (-0.5))
                score = dot(t_ref[HEAD_DIM : 2 * HEAD_DIM, 0:reach], query, TN)
                score = score + bias_ref[0:reach, here]
                top = jnp.max(score, axis=0, keepdims=True)
                weight = jnp.exp(score - top)
                total = jnp.sum(weight, axis=0, keepdims=True)
                mixed = dot(t_ref[2 * HEAD_DIM : per, 0:reach], weight.astype(BF16), NN)
                o_ref[:, here] = (mixed / total).astype(BF16)
                l_ref[0, :, here] = top + jnp.log(total)

    return pl.pallas_call(
        kernel,
        grid=(4,),
        out_shape=(
            jax.ShapeDtypeStruct((4 * HEAD_DIM, tokens), BF16),
            jax.ShapeDtypeStruct((4, 1, tokens), F32),
        ),
        in_specs=[
            pl.BlockSpec((tokens, 1), lambda h: (0, 0)),
            pl.BlockSpec((1, tokens), lambda h: (0, 0)),
            pl.BlockSpec((per, tokens), lambda h: (h, 0)),
        ],
        out_specs=(
            pl.BlockSpec((HEAD_DIM, tokens), lambda h: (h, 0)),
            pl.BlockSpec((1, 1, tokens), lambda h: (h, 0, 0)),
        ),
        scratch_shapes=[pltpu.VMEM((tokens, tokens), F32)],
        compiler_params=pltpu.CompilerParams(vmem_limit_bytes=VMEM_BYTES),
    )(seg_col, seg_row, triple)


def attention_backward(triple, seg_col, seg_row, attended, attended_grad, lse):
    per = 3 * HEAD_DIM
    tokens = triple.shape[1]
    span = tokens // 4

    def kernel(sc_ref, sr_ref, t_ref, o_ref, g_ref, l_ref, d_ref, bias_ref, kg_ref, vg_ref):
        @pl.when(pl.program_id(0) == 0)
        def _():
            attention_bias(sc_ref, sr_ref, bias_ref)

        @pl.when(holds(pl.program_id(0)))
        def _():
            kg_ref[...] = jnp.zeros_like(kg_ref)
            vg_ref[...] = jnp.zeros_like(vg_ref)
            for j in range(4):
                reach, here = (j + 1) * span, slice(j * span, (j + 1) * span)
                query = t_ref[0:HEAD_DIM, here] * BF16(HEAD_DIM ** (-0.5))
                key = t_ref[HEAD_DIM : 2 * HEAD_DIM, 0:reach]
                grad = g_ref[:, here]
                delta = jnp.sum(
                    grad.astype(F32) * o_ref[:, here].astype(F32), axis=0, keepdims=True
                )
                score = dot(key, query, TN) + bias_ref[0:reach, here]
                prob = jnp.exp(score - l_ref[0, :, here])
                vg_ref[:, 0:reach] += dot(grad, prob.astype(BF16), NT)
                back = dot(t_ref[2 * HEAD_DIM : per, 0:reach], grad, TN)
                mix = (prob * (back - delta)).astype(BF16)
                d_ref[0:HEAD_DIM, here] = (dot(key, mix, NN) * HEAD_DIM ** (-0.5)).astype(BF16)
                kg_ref[:, 0:reach] += dot(query, mix, NT)
            d_ref[HEAD_DIM : 2 * HEAD_DIM, :] = kg_ref[...].astype(BF16)
            d_ref[2 * HEAD_DIM : per, :] = vg_ref[...].astype(BF16)

    return pl.pallas_call(
        kernel,
        grid=(4,),
        out_shape=jax.ShapeDtypeStruct((4 * per, tokens), BF16),
        in_specs=[
            pl.BlockSpec((tokens, 1), lambda h: (0, 0)),
            pl.BlockSpec((1, tokens), lambda h: (0, 0)),
            pl.BlockSpec((per, tokens), lambda h: (h, 0)),
            pl.BlockSpec((HEAD_DIM, tokens), lambda h: (h, 0)),
            pl.BlockSpec((HEAD_DIM, tokens), lambda h: (h, 0)),
            pl.BlockSpec((1, 1, tokens), lambda h: (h, 0, 0)),
        ],
        out_specs=pl.BlockSpec((per, tokens), lambda h: (h, 0)),
        scratch_shapes=[
            pltpu.VMEM((tokens, tokens), F32),
            pltpu.VMEM((HEAD_DIM, tokens), F32),
            pltpu.VMEM((HEAD_DIM, tokens), F32),
        ],
        compiler_params=pltpu.CompilerParams(vmem_limit_bytes=VMEM_BYTES),
    )(seg_col, seg_row, triple, attended, attended_grad, lse)


def sum_all(pieces, sizes, cid):
    count = pieces.shape[0]
    rows, cols = sizes

    def kernel(x_ref, out_ref, inbox, piece, sems):
        me = (lax.axis_index("dp") * rows + lax.axis_index("row")) * cols + lax.axis_index("col")

        def dev(step):
            flat = lax.rem(me + step, count)
            return flat, (flat // (rows * cols), lax.rem(flat // cols, rows), lax.rem(flat, cols))

        semaphore = pltpu.get_barrier_semaphore()

        def greet(step, carry):
            pl.semaphore_signal(semaphore, inc=1, device_id=dev(step)[1], device_id_type=MESH)
            return carry

        lax.fori_loop(1, count, greet, 0)
        pl.semaphore_wait(semaphore, count - 1)

        def spread(step, carry):
            flat, device = dev(step)
            rcopy(x_ref.at[flat], inbox.at[me], sems.at[0], sems.at[1], device).start()
            return carry

        lax.fori_loop(1, count, spread, 0)
        inbox[me] = x_ref[me]
        rest = inbox.at[pl.ds(0, count - 1)]
        pltpu.make_async_copy(rest, rest, sems.at[1]).wait()
        pltpu.make_async_copy(rest, rest, sems.at[0]).wait()
        piece[...] = jnp.sum(inbox[...], axis=0)

        def share(step, carry):
            rcopy(piece, out_ref.at[me], sems.at[2], sems.at[3], dev(step)[1]).start()
            return carry

        lax.fori_loop(1, count, share, 0)
        out_ref[me] = piece[...]
        rest = out_ref.at[pl.ds(0, count - 1)]
        pltpu.make_async_copy(rest, rest, sems.at[3]).wait()
        pltpu.make_async_copy(rest, rest, sems.at[2]).wait()

    return call(
        kernel, jax.ShapeDtypeStruct(pieces.shape, F32), VM, [VM],
        [pltpu.VMEM(pieces.shape, F32), pltpu.VMEM(pieces.shape[1:], F32), DMA((4,))], cid,
    )(pieces)


def shards(
    tokens, segment_ids, first_gain, first_shift, triple_weight, query_bias, value_bias,
    proj_weight, proj_bias, second_gain, second_shift, expand_weight, expand_bias,
    shrink_weight, shrink_bias, cotangent, *, axis_sizes,
):
    width = HEADS * HEAD_DIM
    dp_count, row_count, col_count = axis_sizes
    row, col = lax.axis_index("row"), lax.axis_index("col")
    col_width = tokens.shape[1]
    triple_width = triple_weight.shape[1]
    hidden = expand_weight.shape[1] // 2
    core_feats = (triple_width // GRAIN + 1) // 2 * GRAIN

    stacked = jnp.concatenate(
        [first_gain, first_shift, proj_bias, second_gain, second_shift, shrink_bias]
    ).reshape(6, width)
    cols = lax.dynamic_slice_in_dim(stacked, col * col_width, col_width, 1).T
    full_bias = jnp.concatenate([query_bias, jnp.zeros((width,), F32), value_bias])
    core_bias = lax.dynamic_slice_in_dim(
        full_bias, row * triple_width + col * (triple_width - core_feats), core_feats
    )[:, None]
    core_expand_bias = lax.dynamic_slice_in_dim(
        expand_bias, (row * 2 + col) * hidden, hidden
    )[:, None]
    tokens_t, cot_t = tokens.T, cotangent.T
    seg_row = segment_ids
    seg_col = segment_ids.reshape(-1, 1)

    first_all, triple, first_stats = gather_triple(
        tokens_t, cols, core_bias, triple_weight, width, core_feats, 0
    )
    triple, cot_later = lax.optimization_barrier((triple, cot_t))
    cot_rows = lax.all_gather(cot_later, "row")
    attended, lse = attention_forward(triple, seg_col, seg_row)
    attended_all, proj_out = attended_scatter(attended, proj_weight, 2)
    (
        second_all, act_all, hid_all, middle, second_stats, expand_bias_part, shrink_grad
    ) = gather_hidden(
        tokens_t, proj_out, cols, core_expand_bias, cot_rows, expand_weight, shrink_weight.T,
        width, 3,
    )

    def product(left, right):
        return lax.dot_general(left, right, NT, preferred_element_type=F32).astype(BF16)

    def owned(grad):
        parts = grad.reshape(dp_count, -1, grad.shape[1])
        summed = lax.psum_scatter(parts, "dp", scatter_dimension=0, tiled=True)
        return summed.reshape(1, -1, grad.shape[1])

    shrink_owned = owned(shrink_grad)

    second_normed_grad = hidden_scatter(hid_all, expand_weight, 4)
    middle_all, attended_grad, middle_grad, second_sums = gather_middle(
        second_normed_grad, middle, second_stats, cot_t, cols, proj_weight, width, 5
    )
    proj_grad = product(attended_all, middle_all)
    expand_grad = product(second_all, hid_all)
    attended_grad, shrink_owned, expand_grad = lax.optimization_barrier(
        (attended_grad, shrink_owned, expand_grad)
    )
    expand_owned = owned(expand_grad)
    triple_head_grad = attention_backward(
        triple, seg_col, seg_row, attended, attended_grad, lse
    )
    triple_all, proj_parts, input_grad, first_sums, bias_sums = triple_scatter(
        triple_head_grad, triple_weight, tokens_t, first_stats, middle_grad, cols,
        proj_grad.reshape(dp_count, -1, col_width), width, 6,
    )
    triple_grad = product(first_all, triple_all)
    act_all, triple_grad, expand_owned, first_sums, proj_parts = lax.optimization_barrier(
        (act_all, triple_grad, expand_owned, first_sums, proj_parts)
    )
    proj_owned = jnp.sum(proj_parts.astype(F32), axis=0, keepdims=True)
    triple_owned = owned(triple_grad)
    block_out = output_scatter(act_all, shrink_weight.T, middle, cols, 7)

    by_col = jnp.concatenate([first_sums[:2], second_sums[:4]])
    is_col = (jnp.arange(2) == col).astype(F32)
    by_col = by_col[:, None, :] * is_col[None, :, None]
    is_core = (jnp.arange(2 * row_count) == 2 * row + col).astype(F32)
    by_core = expand_bias_part[0] * is_core[:, None]
    is_row = ((jnp.arange(row_count) == row) & (col == 0)).astype(F32)
    by_row = bias_sums[0][None, :] * is_row[:, None]
    vector = jnp.concatenate([by_col.reshape(-1), by_core.reshape(-1), by_row.reshape(-1)])
    devices = dp_count * row_count * col_count
    tile = 8 * 128
    size = -(-vector.shape[0] // (devices * tile)) * tile
    vector = jnp.pad(vector, (0, devices * size - vector.shape[0]))
    total = sum_all(
        vector.reshape(devices, size // 128, 128), (row_count, col_count), 8
    ).reshape(-1)
    col_totals = total[: 6 * width].reshape(6, width)
    expand_bias_grad = total[6 * width : 6 * width + 2 * row_count * hidden]
    rest = total[6 * width + 2 * row_count * hidden :]
    return (
        block_out.T,
        input_grad.T,
        col_totals[0],
        col_totals[1],
        triple_owned.astype(F32),
        rest[:width],
        rest[2 * width : 3 * width],
        proj_owned.astype(F32),
        col_totals[4],
        col_totals[2],
        col_totals[3],
        expand_owned.astype(F32),
        expand_bias_grad,
        shrink_owned.astype(F32),
        col_totals[5],
    )


def solution(mesh):
    assert mesh.shape["row"] == 4 and mesh.shape["col"] == 2
    sizes = tuple(mesh.shape[name] for name in AXES)
    tok, mat, mat_t = P(("dp", "row"), "col"), P("row", "col"), P("col", "row")
    in_specs = (
        tok, P("dp", None), P(), P(), mat_t, P(), P(), mat, P(), P(), P(), mat_t, P(), mat, P(), tok,
    )
    grad, grad_t = P("row", "dp", "col"), P("col", "dp", "row")
    out_specs = (
        tok, tok, P(), P(), grad_t, P(), P(), grad, P(), P(), P(), grad_t, P(), grad, P(),
    )
    return jax.shard_map(
        functools.partial(shards, axis_sizes=sizes),
        mesh=mesh, in_specs=in_specs, out_specs=out_specs, check_vma=False,
    )
```

```python
import functools

import jax
import jax.numpy as jnp
from jax import lax
from jax.experimental import pallas as pl
from jax.experimental.pallas import tpu as pltpu
from jax.sharding import PartitionSpec as P

HEADS = 25
HEAD_DIM = 64
EPS = 1e-05
NEG = -1e30
GRAIN = 16
AXES = ("dp", "row", "col")
MESH = pl.DeviceIdType.MESH
F32 = jnp.float32
BF16 = jnp.bfloat16
VMEM_BYTES = 60 * 1024 * 1024

NN = (((1,), (0,)), ((), ()))
NT = (((1,), (1,)), ((), ()))
TN = (((0,), (0,)), ((), ()))


def dot(left, right, dims):
    return lax.dot_general(left, right, dims, preferred_element_type=F32)


class Place:
    def __init__(self):
        self.d = lax.axis_index("dp")
        self.r = lax.axis_index("row")
        self.c = lax.axis_index("col")
        one = self.r + 1 - 2 * lax.rem(self.r, 2)
        two = lax.rem(self.r + 2, 4)
        self.a = 1 + self.c
        self.b = 2 - self.c
        self.ra = (1 - self.c) * one + self.c * two
        self.rb = self.c * one + (1 - self.c) * two
        self.r3 = 3 - self.r

    def dev(self, row, col=None):
        return (self.d, row, self.c if col is None else col)

    def mate(self):
        return (self.d, self.r, 1 - self.c)

    def barrier(self, devices):
        semaphore = pltpu.get_barrier_semaphore()
        for device in devices:
            pl.semaphore_signal(semaphore, inc=1, device_id=device, device_id_type=MESH)
        pl.semaphore_wait(semaphore, len(devices))

    def group(self):
        flat = 2 * self.r + self.c
        found = []
        for step in range(1, 8):
            other = lax.rem(flat + step, 8)
            found.append((self.d, other // 2, lax.rem(other, 2)))
        return found

    def square(self):
        return [self.mate(), self.dev(self.ra), self.dev(self.rb)]


def rcopy(src, dst, send, recv, device):
    return pltpu.make_async_remote_copy(
        src_ref=src, dst_ref=dst, send_sem=send, recv_sem=recv, device_id=device,
        device_id_type=MESH,
    )


def pick(k, zero, one, two, three):
    return jnp.where(k == 0, zero, jnp.where(k == 1, one, jnp.where(k == 2, two, three)))


def lanes(index, size):
    return pl.ds(pl.multiple_of(index * size, size), size)


def call(kernel, out_shapes, out_specs, in_specs, scratch, cid, flops=0, bytes_accessed=0):
    return pl.pallas_call(
        kernel,
        out_shape=out_shapes,
        in_specs=in_specs,
        out_specs=out_specs,
        scratch_shapes=scratch,
        compiler_params=pltpu.CompilerParams(
            collective_id=cid, has_side_effects=True, vmem_limit_bytes=VMEM_BYTES
        ),
    )


VM = pl.BlockSpec(memory_space=pltpu.VMEM)
ANY = pl.BlockSpec(memory_space=pl.ANY)
DMA = pltpu.SemaphoreType.DMA


def struct(shape, dtype):
    return jax.ShapeDtypeStruct(shape, dtype)


def chunks(size):
    count = next(n for n in (2, 1) if size % (n * GRAIN) == 0)
    return [pl.ds(k * (size // count), size // count) for k in range(count)]


def col_sums(matrix):
    ones = jnp.ones((8, matrix.shape[1]), matrix.dtype)
    exact = lax.Precision.HIGHEST if matrix.dtype == F32 else None
    return lax.dot_general(ones, matrix, NT, precision=exact, preferred_element_type=F32)[0:1]


class Totals:
    scratch = [pltpu.VMEM((2, 8, 256), F32), DMA((2,))]

    def __init__(self, place, buf, sems):
        self.place, self.buf, self.sems = place, buf, sems

    def __call__(self, first, second):
        self.buf[0, 0:1] = jnp.sum(first, axis=0, keepdims=True)
        self.buf[0, 1:2] = jnp.sum(second, axis=0, keepdims=True)
        copy = rcopy(
            self.buf.at[0], self.buf.at[1], self.sems.at[0], self.sems.at[1], self.place.mate()
        )
        copy.start()
        copy.wait()
        return (
            self.buf[0, 0:1] + self.buf[1, 0:1],
            self.buf[0, 1:2] + self.buf[1, 1:2],
        )


def moments(totals, matrix, width):
    total, square = totals(matrix, matrix * matrix)
    average = total / width
    return average, lax.rsqrt(square / width - average * average + EPS)


def keep_moments(ref, average, rstd):
    ref[0:1] = average
    ref[1:2] = rstd


def norm_back(totals, grad_in, hat, rstd, gain, width):
    scaled = grad_in * gain
    total, mixed = totals(scaled, scaled * hat)
    return rstd * (scaled - total / width - hat * mixed / width)


def weight_scratch(rows, feats, turned):
    return [
        pltpu.VMEM((rows, turned), BF16), pltpu.VMEM((turned, rows), BF16),
        pltpu.VMEM((feats, rows), BF16), DMA((3,)),
    ]


def gather_scratch(rows, cols):
    count = len(chunks(rows))
    return [
        pltpu.VMEM((2, 4, rows, cols), BF16), DMA((7, count)), DMA((2, 4, count)), DMA((4,)),
    ]


class PairWeight:
    def __init__(self, place, w_ref, step, refs):
        self.flat, self.turned, self.other, sems = refs
        self.load = pltpu.make_async_copy(w_ref, self.flat, sems.at[2])
        self.load.start()
        feats = self.other.shape[0]
        self.own = self.turned.at[pl.ds(pl.multiple_of(step * place.c, GRAIN), feats)]
        theirs = self.turned.at[
            pl.ds(pl.multiple_of(step * (1 - place.c), GRAIN), feats)
        ]
        self.copy = rcopy(theirs, self.other, sems.at[0], sems.at[1], place.mate())

    def share(self):
        self.load.wait()
        self.turned[...] = self.flat[...].T
        self.copy.start()

    def product(self, own, other):
        return dot(self.own[...], own, NN) + dot(self.other[...], other, NN)


class Gather:
    def __init__(self, place, all_ref, refs):
        self.place, self.all_ref = place, all_ref
        self.got, self.send, self.recv, self.out_sem = refs

    def run(self, work, idle):
        place, got, send, recv = self.place, self.got, self.send, self.recv
        mate, size = place.mate(), got.shape[3]
        parts = list(enumerate(chunks(got.shape[2])))
        dev_a, dev_b = place.dev(place.ra), place.dev(place.rb)

        def move(number, source, target, device):
            return [
                rcopy(
                    got.at[source[0], source[1], part], got.at[target[0], target[1], part],
                    send.at[number, k], recv.at[target[0], target[1], k], device,
                )
                for k, part in parts
            ]

        def keep(slot, row, number):
            return pltpu.make_async_copy(
                got.at[0, slot], self.all_ref.at[:, lanes(row, size)], self.out_sem.at[number]
            )

        to_a = move(0, (0, 0), (0, place.a), dev_a)
        to_b = move(1, (0, 0), (0, place.b), dev_b)
        to_mate = move(2, (0, 0), (1, 0), mate)
        relay = move(3, (0, place.a), (0, 3), dev_b)
        fwd_a = move(4, (0, place.a), (1, place.a), mate)
        fwd_b = move(5, (0, place.b), (1, place.b), mate)
        fwd_3 = move(6, (0, 3), (1, 3), mate)
        for copies in (to_a, to_b, to_mate):
            for copy in copies:
                copy.start()
        keep(0, place.r, 0).start()
        idle()

        def phase(k, carry):
            @pl.when(k == 0)
            def _():
                for copy in to_mate:
                    copy.wait_recv()

            @pl.when(k == 1)
            def _():
                for n, copy in enumerate(to_a):
                    copy.wait_recv()
                    relay[n].start()
                    fwd_a[n].start()
                keep(place.a, place.ra, 1).start()
                for n, copy in enumerate(to_b):
                    copy.wait_recv()
                    fwd_b[n].start()
                keep(place.b, place.rb, 2).start()
                for copy in fwd_b:
                    copy.wait_recv()

            @pl.when(k == 2)
            def _():
                for copy in fwd_a:
                    copy.wait_recv()

            @pl.when(k == 3)
            def _():
                for n, copy in enumerate(relay):
                    copy.wait_recv()
                    fwd_3[n].start()
                keep(3, place.r3, 3).start()
                for copy in fwd_3:
                    copy.wait_recv()

            slot = pick(k, 0, place.b, place.a, 3)
            work(k, slot, pick(k, place.r, place.rb, place.ra, place.r3))
            return carry

        lax.fori_loop(0, 4, phase, 0)
        for copies in (to_mate, to_a, to_b, relay, fwd_a, fwd_b, fwd_3):
            for copy in copies:
                copy.wait_send()
        for slot, row, number in (
            (0, place.r, 0), (place.a, place.ra, 1), (place.b, place.rb, 2), (3, place.r3, 3)
        ):
            keep(slot, row, number).wait()


def gather_triple(tokens, cols, bias, weight, width, feats, cid):
    rows, size = tokens.shape
    triple_width = weight.shape[1]
    grains = feats // GRAIN
    shift = triple_width - feats
    per = 3 * HEAD_DIM

    def kernel(x_ref, c_ref, b_ref, w_ref, all_ref, h_ref, st_ref, tt, tb, ts, gs, gr, *refs):
        place = Place()
        place.barrier(place.group())
        me = 2 * place.r + place.c
        weight = PairWeight(place, w_ref, shift, refs[:4])
        gather = Gather(place, all_ref, refs[4:])
        wide = x_ref[...].astype(F32)
        average, rstd = moments(Totals(place, tb, ts), wide, width)
        keep_moments(st_ref, average, rstd)
        gather.got[0, 0] = ((wide - average) * rstd * c_ref[:, 0:1] + c_ref[:, 1:2]).astype(BF16)

        def target(j):
            feature = triple_width * place.r + shift * place.c + GRAIN * j
            part = feature // width
            inner = feature - part * width
            head = inner // HEAD_DIM
            owner = jnp.minimum(head // 3, 7)
            row = (head - 3 * owner) * per + part * HEAD_DIM + (inner - head * HEAD_DIM)
            return owner, pl.ds(pl.multiple_of(row, GRAIN), GRAIN)

        def work(k, slot, row):
            total = weight.product(gather.got[0, slot], gather.got[1, slot])
            tt[:, lanes(row, size)] = (total + b_ref[...]).astype(BF16)

            def send_grain(j, carry):
                owner, place_rows = target(j)
                src = tt.at[pl.ds(pl.multiple_of(GRAIN * j, GRAIN), GRAIN), lanes(row, size)]
                dst = h_ref.at[place_rows, lanes(row, size)]

                @pl.when(owner == me)
                def _():
                    pltpu.make_async_copy(src, dst, gr).start()

                @pl.when(owner != me)
                def _():
                    rcopy(src, dst, gs, gr, (place.d, owner // 2, lax.rem(owner, 2))).start()

                return carry

            lax.fori_loop(place.c, grains, send_grain, 0)

        def idle():
            weight.share()
            weight.copy.wait()

        gather.run(work, idle)

        def drain(j, carry):
            @pl.when(target(j)[0] != me)
            def _():
                src = tt.at[pl.ds(0, GRAIN)]
                pltpu.make_async_copy(src, src, gs).wait()

            return carry

        lax.fori_loop(place.c, grains, drain, 0)

        @pl.when(me == 7)
        def _():
            pltpu.make_async_copy(h_ref, h_ref, gr).wait()

        @pl.when(me != 7)
        def _():
            part = h_ref.at[pl.ds(0, 3 * per)]
            pltpu.make_async_copy(part, part, gr).wait()

    return call(
        kernel,
        (struct((rows, 4 * size), BF16), struct((4 * per, 4 * size), BF16), struct((8, size), F32)),
        (ANY, ANY, VM), [VM] * 3 + [ANY],
        [pltpu.VMEM((feats, 4 * size), BF16)] + Totals.scratch + [DMA, DMA]
        + weight_scratch(rows, feats, triple_width) + gather_scratch(rows, size), cid,
    )(tokens, cols, bias, weight)


def gather_hidden(tokens, proj_out, cols, bias, cot, weight, back_weight, width, cid):
    rows, size = tokens.shape
    feats = weight.shape[1] // 2
    tokens_all = 4 * size

    def kernel(
        t_ref, p_ref, c_ref, b_ref, x_ref, w_ref, v_ref,
        all_ref, act_ref, hid_ref, mid_ref, st_ref, sum_ref, grad_ref,
        act, hid, swap_send, swap_recv, swap_out, cots, cot_sems, grads, grad_sum,
        tb, ts, *refs,
    ):
        place = Place()
        cot_load = pltpu.make_async_copy(x_ref, cots.at[0], cot_sems.at[2])
        cot_load.start()
        place.barrier(place.square())
        mate = place.mate()
        back = PairWeight(place, v_ref, feats, refs[:4])
        ahead = PairWeight(place, w_ref, feats, refs[4:8])
        gather = Gather(place, all_ref, refs[8:])
        cot_swap = rcopy(x_ref, cots.at[1], cot_sems.at[0], cot_sems.at[1], mate)
        middle = t_ref[...].astype(F32) + p_ref[...] + c_ref[:, 2:3]
        mid_ref[...] = middle
        average, rstd = moments(Totals(place, tb, ts), middle, width)
        keep_moments(st_ref, average, rstd)
        gather.got[0, 0] = ((middle - average) * rstd * c_ref[:, 3:4] + c_ref[:, 4:5]).astype(BF16)
        mine = pl.ds(pl.multiple_of(place.c * feats, GRAIN), feats)
        grad_sum[...] = jnp.zeros_like(grad_sum)

        def moves(k, row):
            span = lanes(row, size)
            index = row
            there = hid_ref.at[mine, span]
            return (
                rcopy(
                    act.at[mine, span], act.at[mine, span],
                    swap_send.at[0, k], swap_recv.at[0, index], mate,
                ),
                rcopy(hid.at[k], there, swap_send.at[1, k], swap_recv.at[1, index], mate),
                pltpu.make_async_copy(hid.at[k], there, swap_out.at[k]),
            )

        def idle():
            back.share()
            cot_swap.start()
            ahead.share()
            cot_load.wait()
            back.copy.wait()
            cot_swap.wait()

            def one(row, carry):
                grads[row] = back.product(cots[0, row], cots[1, row])
                return carry

            lax.fori_loop(0, 4, one, 0)
            ahead.copy.wait()

        def work(k, slot, row):
            p = ahead.product(gather.got[0, slot], gather.got[1, slot]) + b_ref[...]
            square = p * p
            t = jnp.tanh(0.7978845608028654 * (p + 0.044715 * (square * p)))
            act[mine, lanes(row, size)] = (0.5 * p * (1.0 + t)).astype(BF16)
            slope = 0.5 * (1.0 + t) + 0.5 * p * (1.0 - t * t) * (
                0.7978845608028654 * (1.0 + 3.0 * 0.044715 * square)
            )
            grad = grads[row] * slope
            hid[k] = grad.astype(BF16)
            for copy in moves(k, row):
                copy.start()
            grad_sum[...] += grad

        gather.run(work, idle)
        sum_ref[0:1] = col_sums(grad_sum[...])
        order = [place.r, place.rb, place.ra, place.r3]
        for k, row in enumerate(order):
            moves(k, row)[0].wait()
        act_out = pltpu.make_async_copy(act, act_ref, swap_out.at[4])
        act_out.start()
        part = feats // 2

        def some(k, carry):
            here = pl.ds(pl.multiple_of(k * part, GRAIN), part)
            total = dot(act[here, 0:size], cots[0, 0], NT)
            for row in range(1, 4):
                total += dot(act[here, row * size : (row + 1) * size], cots[0, row], NT)
            grad_ref[here] = total.astype(BF16)
            return carry

        lax.fori_loop(0, 4, some, 0)
        for k, row in enumerate(order):
            for copy in moves(k, row)[1:]:
                copy.wait()
        act_out.wait()

    full = struct((2 * feats, tokens_all), BF16)
    return call(
        kernel,
        (
            struct((rows, tokens_all), BF16), full, full, struct((rows, size), F32),
            struct((8, size), F32), struct((8, feats), F32), struct((2 * feats, rows), BF16),
        ),
        (ANY, ANY, ANY, VM, VM, VM, VM), [VM] * 4 + [ANY] * 3,
        [pltpu.VMEM((2 * feats, tokens_all), BF16), pltpu.VMEM((4, feats, size), BF16)]
        + [DMA((2, 4)), DMA((2, 4)), DMA((5,))]
        + [pltpu.VMEM((2, 4, rows, size), BF16), DMA((3,))]
        + [pltpu.VMEM((4, feats, size), F32), pltpu.VMEM((feats, size), F32)]
        + Totals.scratch + weight_scratch(rows, feats, 2 * feats) * 2
        + gather_scratch(rows, size), cid,
    )(tokens, proj_out, cols, bias, cot, weight, back_weight)


def gather_middle(grad_in, middle, stats, cot, cols, weight, width, cid):
    rows, size = cot.shape
    owned = weight.shape[0]
    feats = 4 * HEAD_DIM
    step = 3 * HEAD_DIM
    lag = 3 * (owned - 2 * step)
    whole = lag + owned + 2 * HEAD_DIM

    def kernel(
        s_ref, m_ref, st_ref, x_ref, c_ref, w_ref, all_ref, y_ref, mg_ref, sum_ref,
        wide, other, w_sems, tb, ts, *refs,
    ):
        place = Place()
        load = pltpu.make_async_copy(w_ref, wide.at[pl.ds(lag, owned)], w_sems.at[0])
        load.start()
        place.barrier(place.group())
        before = rcopy(
            w_ref.at[pl.ds(owned - lag, lag)], wide.at[pl.ds(0, lag)], w_sems.at[1], w_sems.at[2],
            place.dev(lax.rem(place.r + 1, 4)),
        )
        before.start()
        wide[lag + owned : whole] = jnp.zeros((2 * HEAD_DIM, rows), BF16)
        first = lag - (owned - 2 * step) * place.r

        def heads(col):
            return wide.at[pl.ds(pl.multiple_of(first + step * col, GRAIN), feats)]

        swap = rcopy(heads(1 - place.c), other, w_sems.at[3], w_sems.at[4], place.mate())
        gather = Gather(place, all_ref, refs)
        rstd = st_ref[1:2]
        hat = (m_ref[...] - st_ref[0:1]) * rstd
        back = norm_back(Totals(place, tb, ts), s_ref[...], hat, rstd, c_ref[:, 3:4], width)
        mg_ref[...] = x_ref[...].astype(F32) + back
        gather.got[0, 0] = mg_ref[...].astype(BF16)

        def idle():
            load.wait()
            before.wait()
            swap.start()
            hat = (m_ref[...] - st_ref[0:1]) * st_ref[1:2]
            sum_ref[0:1] = col_sums(s_ref[...] * hat)
            sum_ref[1:2] = col_sums(s_ref[...])
            sum_ref[2:3] = col_sums(mg_ref[...])
            sum_ref[3:4] = col_sums(x_ref[...])
            swap.wait()

        def work(k, slot, row):
            total = dot(heads(place.c)[...], gather.got[0, slot], NN)
            total += dot(other[...], gather.got[1, slot], NN)
            y_ref[:, lanes(row, size)] = total.astype(BF16)

        gather.run(work, idle)

    return call(
        kernel,
        (
            struct((rows, 4 * size), BF16), struct((feats, 4 * size), BF16),
            struct((rows, size), F32), struct((8, rows), F32),
        ),
        (ANY, VM, VM, VM), [VM] * 5 + [ANY],
        [pltpu.VMEM((whole, rows), BF16), pltpu.VMEM((feats, rows), BF16), DMA((5,))]
        + Totals.scratch + gather_scratch(rows, size), cid,
    )(grad_in, middle, stats, cot, cols, weight)


def scatter_scratch(rows, cols):
    count = len(chunks(rows))
    return [
        pltpu.VMEM((3, rows, cols), BF16), pltpu.VMEM((3, rows, cols), BF16),
        DMA((3, count)), DMA((3, count)), pltpu.VMEM((rows, cols), F32),
    ]


def run_scatter(place, block, refs):
    outbox, inbox, send, recv, passed = refs
    parts = list(enumerate(chunks(outbox.shape[1])))

    def move(number, device):
        return [
            rcopy(
                outbox.at[number, part], inbox.at[number, part],
                send.at[number, k], recv.at[number, k], device,
            )
            for k, part in parts
        ]

    first = move(0, place.dev(place.ra))
    second = move(1, place.dev(place.ra))
    third = move(2, place.dev(place.rb))

    def phase(k, carry):
        @pl.when(k == 3)
        def _():
            for n, part in parts:
                first[n].wait_recv()
                outbox[2, part] = (passed[part] + inbox[0, part].astype(F32)).astype(BF16)
                third[n].start()

        total = block(k, pick(k, place.r3, place.rb, place.ra, place.r))

        @pl.when((k == 1) | (k == 3))
        def _():
            passed[...] = total

        @pl.when(k == 0)
        def _():
            outbox[0] = total.astype(BF16)
            for copy in first:
                copy.start()

        @pl.when(k == 2)
        def _():
            outbox[1] = total.astype(BF16)
            for copy in second:
                copy.start()

        return carry

    lax.fori_loop(0, 4, phase, 0)
    for copy in second:
        copy.wait_recv()
    passed[...] += inbox[1].astype(F32)
    for copy in third:
        copy.wait_recv()
    total = passed[...] + inbox[2].astype(F32)
    for copies in (first, second, third):
        for copy in copies:
            copy.wait_send()
    return total


def load_scratch(weight, left):
    return [pltpu.VMEM(weight.shape, BF16), pltpu.VMEM(left.shape, BF16), DMA((5,))]


def loaded_block(place, l_ref, w_ref, weight, left, sems, size):
    w_load = pltpu.make_async_copy(w_ref, weight, sems.at[4])
    w_load.start()

    def load(k, row):
        span = lanes(row, size)
        return pltpu.make_async_copy(l_ref.at[:, span], left.at[:, span], sems.at[k])

    for k, row in enumerate((place.r3, place.rb, place.ra, place.r)):
        load(k, row).start()

    def block(k, row):
        @pl.when(k == 0)
        def _():
            w_load.wait()

        load(k, row).wait()
        return dot(weight[...], left[:, lanes(row, size)], NN)

    return block


def hidden_scatter(left, weight, cid):
    rows, size = weight.shape[0], left.shape[1] // 4

    def kernel(l_ref, w_ref, out_ref, w, l, l_sem, *refs):
        place = Place()
        block = loaded_block(place, l_ref, w_ref, w, l, l_sem, size)
        place.barrier([place.dev(place.ra), place.dev(place.rb)])
        out_ref[...] = run_scatter(place, block, refs)

    return call(
        kernel, struct((rows, size), F32), VM, [ANY] * 2,
        load_scratch(weight, left) + scatter_scratch(rows, size), cid,
    )(left, weight)


def output_scatter(left, weight, middle, cols, cid):
    rows, size = middle.shape

    def kernel(l_ref, w_ref, m_ref, c_ref, out_ref, w, l, l_sem, *refs):
        place = Place()
        block = loaded_block(place, l_ref, w_ref, w, l, l_sem, size)
        place.barrier([place.dev(place.ra), place.dev(place.rb)])
        total = run_scatter(place, block, refs)
        out_ref[...] = (m_ref[...] + total + c_ref[:, 5:6]).astype(BF16)

    return call(
        kernel, struct((rows, size), BF16), VM, [ANY, ANY, VM, VM],
        load_scratch(weight, left) + scatter_scratch(rows, size), cid,
    )(left, weight, middle, cols)


def attention_scatter(triple, seg_col, seg_row, weight, cid):
    feats, rows = weight.shape
    tokens = triple.shape[1]
    size = tokens // 4
    per = 3 * HEAD_DIM

    def kernel(
        t_ref, sc_ref, sr_ref, w_ref, o_ref, l_ref, all_ref, out_ref,
        bias_ref, full, gs, gr, kept_sem, *refs,
    ):
        place = Place()
        place.barrier(place.group())
        me = 2 * place.r + place.c
        heads = jnp.where(me == 7, 4, 3)
        grains = HEAD_DIM // GRAIN
        attention_bias(sc_ref, sr_ref, bias_ref)

        def send_grain(j, carry):
            feature = 3 * HEAD_DIM * me + GRAIN * j
            owner = feature // feats
            src = o_ref.at[pl.ds(pl.multiple_of(GRAIN * j, GRAIN), GRAIN)]
            dst = full.at[pl.ds(pl.multiple_of(feature - owner * feats, GRAIN), GRAIN)]
            rcopy(src, dst, gs, gr, (place.d, owner, 1 - place.c)).start()

            @pl.when(owner == place.r)
            def _():
                pltpu.make_async_copy(src, dst, gr).start()

            @pl.when(owner != place.r)
            def _():
                rcopy(src, dst, gs, gr, (place.d, owner, place.c)).start()

            return carry

        def one_head(h, carry):
            def rows_of(part):
                return pl.ds(pl.multiple_of(per * h + HEAD_DIM * part, GRAIN), HEAD_DIM)

            for j in range(4):
                reach, here = (j + 1) * size, slice(j * size, (j + 1) * size)
                query = t_ref[rows_of(0), here] * BF16(HEAD_DIM ** (-0.5))
                score = dot(t_ref[rows_of(1), 0:reach], query, TN) + bias_ref[0:reach, here]
                top = jnp.max(score, axis=0, keepdims=True)
                each = jnp.exp(score - top)
                total = jnp.sum(each, axis=0, keepdims=True)
                mixed = dot(t_ref[rows_of(2), 0:reach], each.astype(BF16), NN)
                out_rows = pl.ds(pl.multiple_of(HEAD_DIM * h, GRAIN), HEAD_DIM)
                o_ref[out_rows, here] = (mixed / total).astype(BF16)
                l_ref[h, :, here] = top + jnp.log(total)
            lax.fori_loop(grains * h, grains * (h + 1), send_grain, 0)
            return carry

        lax.fori_loop(0, heads, one_head, 0)

        def drain(j, carry):
            feature = 3 * HEAD_DIM * me + GRAIN * j
            src = o_ref.at[pl.ds(0, GRAIN)]
            pltpu.make_async_copy(src, src, gs).wait()

            @pl.when(feature // feats != place.r)
            def _():
                pltpu.make_async_copy(src, src, gs).wait()

            return carry

        lax.fori_loop(0, heads * grains, drain, 0)
        pltpu.make_async_copy(full, full, gr).wait()
        kept = pltpu.make_async_copy(full, all_ref, kept_sem)
        kept.start()
        out_ref[...] = run_scatter(
            place, lambda k, row: dot(w_ref[...], full[:, lanes(row, size)], TN), refs
        )
        kept.wait()

    return call(
        kernel,
        (
            struct((4 * HEAD_DIM, tokens), BF16), struct((4, 1, tokens), F32),
            struct((feats, tokens), BF16), struct((rows, size), F32),
        ),
        (VM, VM, ANY, VM), [VM] * 4,
        [pltpu.VMEM((tokens, tokens), F32), pltpu.VMEM((feats, tokens), BF16), DMA, DMA, DMA]
        + scatter_scratch(rows, size), cid,
    )(triple, seg_col, seg_row, weight)


def triple_scatter(heads, weight, tokens, stats, middle_grad, cols, pieces, width, cid):
    groups = pieces.shape[0]
    rows, feats = weight.shape
    count_tokens = heads.shape[1]
    size = count_tokens // 4
    per = 3 * HEAD_DIM
    low = (feats // GRAIN + 1) // 2 * GRAIN

    def kernel(
        h_ref, w_ref, p_ref, t_ref, st_ref, mg_ref, c_ref,
        all_ref, got_ref, out_ref, sum_ref, bias_ref, full, w, w_sem, p_sems, tb, ts, gs, gr, ms, mr, kept_sem, *refs,
    ):
        place = Place()
        w_load = pltpu.make_async_copy(w_ref, w, w_sem)
        w_load.start()
        peers = [
            (lax.rem(place.d + step, groups), place.r, place.c) for step in range(1, groups)
        ]
        place.barrier(place.group() + peers)
        me = 2 * place.r + place.c
        count = jnp.where(me == 7, 4, 3) * (per // GRAIN)

        def target(j):
            row = GRAIN * j
            head = row // per
            rest = row - head * per
            part = rest // HEAD_DIM
            feature = part * width + (3 * me + head) * HEAD_DIM + rest - part * HEAD_DIM
            owner = feature // feats
            inner = feature - owner * feats
            return 2 * owner + inner // low, inner

        def send_grain(j, carry):
            owner, inner = target(j)
            src = h_ref.at[pl.ds(pl.multiple_of(GRAIN * j, GRAIN), GRAIN)]
            dst = full.at[pl.ds(pl.multiple_of(inner, GRAIN), GRAIN)]

            @pl.when(owner == me)
            def _():
                pltpu.make_async_copy(src, dst, gr).start()

            @pl.when(owner != me)
            def _():
                rcopy(src, dst, gs, gr, (place.d, owner // 2, lax.rem(owner, 2))).start()

            return carry

        lax.fori_loop(0, count, send_grain, 0)
        traded = [
            rcopy(
                p_ref.at[peer[0]], got_ref.at[place.d],
                p_sems.at[0, k], p_sems.at[1, k], peer,
            )
            for k, peer in enumerate(peers)
        ]
        for copy in traded:
            copy.start()
        own_piece = pltpu.make_async_copy(
            p_ref.at[place.d], got_ref.at[place.d], p_sems.at[0, groups - 1]
        )
        own_piece.start()

        def drain(j, carry):
            @pl.when(target(j)[0] != me)
            def _():
                src = h_ref.at[pl.ds(0, GRAIN)]
                pltpu.make_async_copy(src, src, gs).wait()

            return carry

        lax.fori_loop(0, count, drain, 0)
        lower, upper = full.at[pl.ds(0, low)], full.at[pl.ds(low, feats - low)]

        def swap(mine, theirs):
            pltpu.make_async_copy(mine, mine, gr).wait()
            copy = rcopy(mine, mine, ms, mr, place.mate())
            copy.start()
            copy.wait_send()
            pltpu.make_async_copy(theirs, theirs, mr).wait()

        @pl.when(place.c == 0)
        def _():
            swap(lower, upper)

        @pl.when(place.c == 1)
        def _():
            swap(upper, lower)

        kept = pltpu.make_async_copy(full, all_ref, kept_sem)
        kept.start()
        w_load.wait()
        grad = run_scatter(place, lambda k, row: dot(w[...], full[:, lanes(row, size)], NN), refs)
        rstd = st_ref[1:2]
        hat = (t_ref[...].astype(F32) - st_ref[0:1]) * rstd
        back = norm_back(Totals(place, tb, ts), grad, hat, rstd, c_ref[:, 0:1], width)
        out_ref[...] = mg_ref[...] + back
        sum_ref[0:1] = col_sums(grad * hat)
        sum_ref[1:2] = col_sums(grad)
        bias_ref[0:1] = col_sums(full[...])
        kept.wait()
        own_piece.wait()
        for copy in traded:
            copy.wait()

    return call(
        kernel,
        (
            struct((feats, count_tokens), BF16), struct(pieces.shape, BF16),
            struct((rows, size), F32), struct((8, rows), F32), struct((8, feats), F32),
        ),
        (ANY, ANY, VM, VM, VM), [ANY] * 3 + [VM] * 4,
        [pltpu.VMEM((feats, count_tokens), BF16), pltpu.VMEM(weight.shape, BF16), DMA]
        + [DMA((2, groups))]
        + Totals.scratch + [DMA] * 5
        + scatter_scratch(rows, size), cid,
    )(heads, weight, pieces, tokens, stats, middle_grad, cols)


def attention_bias(seg_col, seg_row, bias_ref):
    tokens = seg_row.shape[1]
    key = lax.broadcasted_iota(jnp.int32, (tokens, tokens), 0)
    query = lax.broadcasted_iota(jnp.int32, (tokens, tokens), 1)
    allowed = (seg_col[...] == seg_row[...]) & (key <= query)
    bias_ref[...] = jnp.where(allowed, 0.0, NEG)


def holds(head):
    return (head < 3) | ((lax.axis_index("row") == 3) & (lax.axis_index("col") == 1))


def attention_backward(triple, seg_col, seg_row, attended, attended_grad, lse):
    per = 3 * HEAD_DIM
    tokens = triple.shape[1]
    span = tokens // 4

    def kernel(sc_ref, sr_ref, t_ref, o_ref, g_ref, l_ref, d_ref, bias_ref, kg_ref, vg_ref):
        @pl.when(pl.program_id(0) == 0)
        def _():
            attention_bias(sc_ref, sr_ref, bias_ref)

        @pl.when(holds(pl.program_id(0)))
        def _():
            kg_ref[...] = jnp.zeros_like(kg_ref)
            vg_ref[...] = jnp.zeros_like(vg_ref)
            for j in range(4):
                reach, here = (j + 1) * span, slice(j * span, (j + 1) * span)
                query = t_ref[0:HEAD_DIM, here] * BF16(HEAD_DIM ** (-0.5))
                key = t_ref[HEAD_DIM : 2 * HEAD_DIM, 0:reach]
                grad = g_ref[:, here]
                delta = jnp.sum(
                    grad.astype(F32) * o_ref[:, here].astype(F32), axis=0, keepdims=True
                )
                score = dot(key, query, TN) + bias_ref[0:reach, here]
                prob = jnp.exp(score - l_ref[0, :, here])
                vg_ref[:, 0:reach] += dot(grad, prob.astype(BF16), NT)
                back = dot(t_ref[2 * HEAD_DIM : per, 0:reach], grad, TN)
                mix = (prob * (back - delta)).astype(BF16)
                d_ref[0:HEAD_DIM, here] = (dot(key, mix, NN) * HEAD_DIM ** (-0.5)).astype(BF16)
                kg_ref[:, 0:reach] += dot(query, mix, NT)
            d_ref[HEAD_DIM : 2 * HEAD_DIM, :] = kg_ref[...].astype(BF16)
            d_ref[2 * HEAD_DIM : per, :] = vg_ref[...].astype(BF16)

    return pl.pallas_call(
        kernel,
        grid=(4,),
        out_shape=jax.ShapeDtypeStruct((4 * per, tokens), BF16),
        in_specs=[
            pl.BlockSpec((tokens, 1), lambda h: (0, 0)),
            pl.BlockSpec((1, tokens), lambda h: (0, 0)),
            pl.BlockSpec((per, tokens), lambda h: (h, 0)),
            pl.BlockSpec((HEAD_DIM, tokens), lambda h: (h, 0)),
            pl.BlockSpec((HEAD_DIM, tokens), lambda h: (h, 0)),
            pl.BlockSpec((1, 1, tokens), lambda h: (h, 0, 0)),
        ],
        out_specs=pl.BlockSpec((per, tokens), lambda h: (h, 0)),
        scratch_shapes=[
            pltpu.VMEM((tokens, tokens), F32),
            pltpu.VMEM((HEAD_DIM, tokens), F32),
            pltpu.VMEM((HEAD_DIM, tokens), F32),
        ],
        compiler_params=pltpu.CompilerParams(vmem_limit_bytes=VMEM_BYTES),
    )(seg_col, seg_row, triple, attended, attended_grad, lse)


def sum_all(pieces, sizes, cid):
    count = pieces.shape[0]
    rows, cols = sizes

    def kernel(x_ref, out_ref, inbox, piece, sems):
        me = (lax.axis_index("dp") * rows + lax.axis_index("row")) * cols + lax.axis_index("col")

        def dev(step):
            flat = lax.rem(me + step, count)
            return flat, (flat // (rows * cols), lax.rem(flat // cols, rows), lax.rem(flat, cols))

        semaphore = pltpu.get_barrier_semaphore()

        def greet(step, carry):
            pl.semaphore_signal(semaphore, inc=1, device_id=dev(step)[1], device_id_type=MESH)
            return carry

        lax.fori_loop(1, count, greet, 0)
        pl.semaphore_wait(semaphore, count - 1)

        def spread(step, carry):
            flat, device = dev(step)
            rcopy(x_ref.at[flat], inbox.at[me], sems.at[0], sems.at[1], device).start()
            return carry

        lax.fori_loop(1, count, spread, 0)
        inbox[me] = x_ref[me]
        rest = inbox.at[pl.ds(0, count - 1)]
        pltpu.make_async_copy(rest, rest, sems.at[1]).wait()
        pltpu.make_async_copy(rest, rest, sems.at[0]).wait()
        piece[...] = jnp.sum(inbox[...], axis=0)

        def share(step, carry):
            rcopy(piece, out_ref.at[me], sems.at[2], sems.at[3], dev(step)[1]).start()
            return carry

        lax.fori_loop(1, count, share, 0)
        out_ref[me] = piece[...]
        rest = out_ref.at[pl.ds(0, count - 1)]
        pltpu.make_async_copy(rest, rest, sems.at[3]).wait()
        pltpu.make_async_copy(rest, rest, sems.at[2]).wait()

    return call(
        kernel, jax.ShapeDtypeStruct(pieces.shape, F32), VM, [VM],
        [pltpu.VMEM(pieces.shape, F32), pltpu.VMEM(pieces.shape[1:], F32), DMA((4,))], cid,
    )(pieces)


def shards(
    tokens, segment_ids, first_gain, first_shift, triple_weight, query_bias, value_bias,
    proj_weight, proj_bias, second_gain, second_shift, expand_weight, expand_bias,
    shrink_weight, shrink_bias, cotangent, *, axis_sizes,
):
    width = HEADS * HEAD_DIM
    dp_count, row_count, col_count = axis_sizes
    row, col = lax.axis_index("row"), lax.axis_index("col")
    col_width = tokens.shape[1]
    triple_width = triple_weight.shape[1]
    hidden = expand_weight.shape[1] // 2
    core_feats = (triple_width // GRAIN + 1) // 2 * GRAIN

    stacked = jnp.concatenate(
        [first_gain, first_shift, proj_bias, second_gain, second_shift, shrink_bias]
    ).reshape(6, width)
    cols = lax.dynamic_slice_in_dim(stacked, col * col_width, col_width, 1).T
    full_bias = jnp.concatenate([query_bias, jnp.zeros((width,), F32), value_bias])
    core_bias = lax.dynamic_slice_in_dim(
        full_bias, row * triple_width + col * (triple_width - core_feats), core_feats
    )[:, None]
    core_expand_bias = lax.dynamic_slice_in_dim(
        expand_bias, (row * 2 + col) * hidden, hidden
    )[:, None]
    tokens_t, cot_t = tokens.T, cotangent.T
    seg_row = segment_ids
    seg_col = segment_ids.reshape(-1, 1)

    first_all, triple, first_stats = gather_triple(
        tokens_t, cols, core_bias, triple_weight, width, core_feats, 0
    )
    triple, cot_later = lax.optimization_barrier((triple, cot_t))
    cot_rows = lax.all_gather(cot_later, "row")
    attended, lse, attended_all, proj_out = attention_scatter(
        triple, seg_col, seg_row, proj_weight, 2
    )
    (
        second_all, act_all, hid_all, middle, second_stats, expand_bias_part, shrink_grad
    ) = gather_hidden(
        tokens_t, proj_out, cols, core_expand_bias, cot_rows, expand_weight, shrink_weight.T,
        width, 3,
    )

    def product(left, right):
        return lax.dot_general(left, right, NT, preferred_element_type=F32).astype(BF16)

    def owned(grad):
        parts = grad.reshape(dp_count, -1, grad.shape[1])
        summed = lax.psum_scatter(parts, "dp", scatter_dimension=0, tiled=True)
        return summed.reshape(1, -1, grad.shape[1])

    shrink_owned = owned(shrink_grad)

    second_normed_grad = hidden_scatter(hid_all, expand_weight, 4)
    middle_all, attended_grad, middle_grad, second_sums = gather_middle(
        second_normed_grad, middle, second_stats, cot_t, cols, proj_weight, width, 5
    )
    proj_grad = product(attended_all, middle_all)
    expand_grad = product(second_all, hid_all)
    attended_grad, shrink_owned, expand_grad = lax.optimization_barrier(
        (attended_grad, shrink_owned, expand_grad)
    )
    expand_owned = owned(expand_grad)
    triple_head_grad = attention_backward(
        triple, seg_col, seg_row, attended, attended_grad, lse
    )
    triple_all, proj_parts, input_grad, first_sums, bias_sums = triple_scatter(
        triple_head_grad, triple_weight, tokens_t, first_stats, middle_grad, cols,
        proj_grad.reshape(dp_count, -1, col_width), width, 6,
    )
    triple_grad = product(first_all, triple_all)
    act_all, triple_grad, expand_owned, first_sums, proj_parts = lax.optimization_barrier(
        (act_all, triple_grad, expand_owned, first_sums, proj_parts)
    )
    proj_owned = jnp.sum(proj_parts.astype(F32), axis=0, keepdims=True)
    triple_owned = owned(triple_grad)
    block_out = output_scatter(act_all, shrink_weight.T, middle, cols, 7)

    by_col = jnp.concatenate([first_sums[:2], second_sums[:4]])
    is_col = (jnp.arange(2) == col).astype(F32)
    by_col = by_col[:, None, :] * is_col[None, :, None]
    is_core = (jnp.arange(2 * row_count) == 2 * row + col).astype(F32)
    by_core = expand_bias_part[0] * is_core[:, None]
    is_row = ((jnp.arange(row_count) == row) & (col == 0)).astype(F32)
    by_row = bias_sums[0][None, :] * is_row[:, None]
    vector = jnp.concatenate([by_col.reshape(-1), by_core.reshape(-1), by_row.reshape(-1)])
    devices = dp_count * row_count * col_count
    tile = 8 * 128
    size = -(-vector.shape[0] // (devices * tile)) * tile
    vector = jnp.pad(vector, (0, devices * size - vector.shape[0]))
    total = sum_all(
        vector.reshape(devices, size // 128, 128), (row_count, col_count), 8
    ).reshape(-1)
    col_totals = total[: 6 * width].reshape(6, width)
    expand_bias_grad = total[6 * width : 6 * width + 2 * row_count * hidden]
    rest = total[6 * width + 2 * row_count * hidden :]
    return (
        block_out.T,
        input_grad.T,
        col_totals[0],
        col_totals[1],
        triple_owned.astype(F32),
        rest[:width],
        rest[2 * width : 3 * width],
        proj_owned.astype(F32),
        col_totals[4],
        col_totals[2],
        col_totals[3],
        expand_owned.astype(F32),
        expand_bias_grad,
        shrink_owned.astype(F32),
        col_totals[5],
    )


def solution(mesh):
    assert mesh.shape["row"] == 4 and mesh.shape["col"] == 2
    sizes = tuple(mesh.shape[name] for name in AXES)
    tok, mat, mat_t = P(("dp", "row"), "col"), P("row", "col"), P("col", "row")
    in_specs = (
        tok, P("dp", None), P(), P(), mat_t, P(), P(), mat, P(), P(), P(), mat_t, P(), mat, P(), tok,
    )
    grad, grad_t = P("row", "dp", "col"), P("col", "dp", "row")
    out_specs = (
        tok, tok, P(), P(), grad_t, P(), P(), grad, P(), P(), P(), grad_t, P(), grad, P(),
    )
    return jax.shard_map(
        functools.partial(shards, axis_sizes=sizes),
        mesh=mesh, in_specs=in_specs, out_specs=out_specs, check_vma=False,
    )
```
